32 devices in a mesh: band: 4 (over y, core), tile: 8 (over z, x).
Axes of the slice: x: 2, y: 2, z: 4, core: 2. Of those that a mesh axis runs over, the one named last changes fastest.
Arguments:
- patches: bfloat16 [262144, 128], P(('band', 'tile')), may hold values from -6 to 6
- pair_patch: int32 [4096], P(('band', 'tile')), may hold values from 0 to 63
- pair_atm: int32 [4096], P(('band', 'tile')), may hold values from 0 to 4095, as said below
- numerators: int32 [4096, 128, 32], P(('band', 'tile')), may hold values from 0 to 16777215
- counts: int32 [32], P(('band', 'tile')), may hold values from 32 to 128, as said below
Outputs:
- atmosphere: float32 [131072, 128], P(('band', 'tile'))
The draws below stay inside these ranges and needn't reach their ends.
Inputs may be any that keep to these rules, and one draw needn't show every extreme that they name: Block pair_atm[g] is owned by device pair_atm[g] // 128 (band-major device order). Every live pair of device (b, t) targets an owner in band b (any tile) or one of (b - 1, t), (b + 1, t). Among one device's live pairs at most 32 target one owner and at most 16 distinct blocks of one owner; both are reached on some device in every draw. Slots that are not live hold arbitrary blocks in range. `counts`: the value 128 occurs on some device in every draw.
All inputs are finite; a program needn't handle non-finite values.
Results may differ from the reference program's by a relative error of at most 0.0026.
Values sent between devices are 32-bit elements; how exact they have to be, the bound alone decides.
A program may use at most 64 MiB of HBM per device.

```python
import jax
import jax.numpy as jnp
from jax import lax

FLUX = 128
PATCH_BLK = 128
CELL_BLK = 32
PBLK_DEV = 64
CELLS_DEV = 4096
PATCHES = 262144
ALL_PAIRS = 4096
N_BAND = 4
N_TILE = 8


def shuffle_one(subkey):
    return jax.random.permutation(subkey, 2 * PBLK_DEV)


def routing(key):
    base_key = jax.random.fold_in(key, 7)
    subkeys = jax.random.split(base_key, 7)
    devices_all = N_BAND * N_TILE
    pairs_here = 2 * PBLK_DEV
    capacity = PBLK_DEV // 2
    distinct = capacity // 2
    blocks_owned = CELLS_DEV // CELL_BLK
    window = blocks_owned // distinct
    device_ids = jnp.arange(devices_all)
    band_of = (device_ids // N_TILE)[:, None]
    tile_of = (device_ids % N_TILE)[:, None]
    fullest_band = jax.random.randint(subkeys[4], (), 1, N_BAND - 1)
    fullest_tile = jax.random.randint(subkeys[5], (), 0, N_TILE)
    fullest = fullest_band * N_TILE + fullest_tile
    offset_far = jax.random.randint(subkeys[6], (devices_all, 1), 1, N_TILE)
    offset_far = jnp.where(device_ids[:, None] == fullest, N_TILE // 2, offset_far)
    offset_edge = jnp.where(offset_far == N_TILE - 1, 1, offset_far + 1)
    position = jnp.arange(pairs_here)[None, :]
    group = jnp.broadcast_to(position // capacity, (devices_all, pairs_here))
    candidate = jnp.broadcast_to(position % distinct, (devices_all, pairs_here))
    target_band = band_of + jnp.where(group == 1, -1, jnp.where(group == 2, 1, 0))
    target_tile = tile_of + jnp.where(group == 0, offset_far, 0)
    low_edge = (group == 1) & (band_of == 0)
    high_edge = (group == 2) & (band_of == N_BAND - 1)
    at_edge = low_edge | high_edge
    target_band = jnp.where(at_edge, band_of, target_band)
    target_tile = jnp.where(at_edge, tile_of + offset_edge, target_tile) % N_TILE
    owner = target_band * N_TILE + target_tile
    anchor = jax.random.randint(subkeys[0], (devices_all, 4), 0, blocks_owned)
    offsets = jax.random.randint(subkeys[1], (devices_all, 4 * distinct), 0, window)
    anchor_pick = jnp.take_along_axis(anchor, group, axis=1)
    offset_pick = jnp.take_along_axis(offsets, group * distinct + candidate, axis=1)
    local_block = (anchor_pick + candidate * window + offset_pick) % blocks_owned
    global_block = owner * blocks_owned + local_block
    shuffles = jax.vmap(shuffle_one)(jax.random.split(subkeys[2], devices_all))
    global_block = jnp.take_along_axis(global_block, shuffles, axis=1)
    live_counts = jax.random.randint(subkeys[3], (devices_all,), pairs_here // 4, pairs_here + 1)
    live_counts = jnp.where(device_ids == fullest, pairs_here, live_counts)
    return (global_block.reshape(-1).astype(jnp.int32), live_counts.astype(jnp.int32))


def draw_pair_atm(key, part):
    return routing(key)[0]


def draw_counts(key, part):
    return routing(key)[1]


def touch_ends(values, stream_key, least, high):
    extent = values.shape
    index_at = [jax.random.randint(jax.random.fold_in(stream_key, axis), (), 0, extent[axis]) for axis in range(len(extent))]
    values = values.at[tuple(index_at)].set(least)
    longest = extent.index(max(extent))
    index_at[longest] = (index_at[longest] + 1) % extent[longest]
    return values.at[tuple(index_at)].set(high)


def steps_of(stream_key, dims, cuts, smallest, top_value):
    level, own = 1.0, jax.random.fold_in(stream_key, 6)
    for dim, blocks in cuts:
        steps = jnp.exp(jax.random.uniform(jax.random.fold_in(own, dim), (blocks,), jnp.float32, smallest / len(cuts), top_value / len(cuts)))
        level = level * jnp.repeat(steps, dims[dim] // blocks).reshape([-1 if axis == dim else 1 for axis in range(len(dims))])
    return level


def noise(own_key, shape, width, most, shards=(), held_as=jnp.bfloat16):
    loudness = steps_of(own_key, shape, shards, -0.22, 0.18) if shards else 1.0
    result = jax.random.normal(own_key, shape, jnp.float32) * width * loudness
    return jnp.minimum(jnp.maximum(result, -most), most).astype(held_as)


def setup_inputs(seed: int = 0) -> dict:
    key_list = jax.random.split(jax.random.key(seed), 6)
    return {
        "patches": noise(key_list[0], (PATCHES, FLUX), 1.0, 6.0, ((0, 32),)),
        "pair_patch": touch_ends(jax.random.randint(key_list[1], (ALL_PAIRS,), 0, PBLK_DEV), jax.random.fold_in(key_list[1], 1), 0, PBLK_DEV - 1).astype(jnp.int32),
        "pair_atm": draw_pair_atm(jax.random.fold_in(key_list[5], 71), 0),
        "numerators": touch_ends(jax.random.randint(key_list[3], (ALL_PAIRS, PATCH_BLK, CELL_BLK), 0, 16777216), jax.random.fold_in(key_list[3], 1), 0, 16777215).astype(jnp.int32),
        "counts": draw_counts(jax.random.fold_in(key_list[5], 71), 0),
    }


SCALE = 2.0 ** -27


def reference(patches, pair_patch, pair_atm, numerators, counts):
    devices_all = N_BAND * N_TILE
    pairs_here = 2 * PBLK_DEV
    blocks_owned = CELLS_DEV // CELL_BLK
    grouped = patches.reshape(devices_all, PBLK_DEV, PATCH_BLK, FLUX)
    patch_table = pair_patch.reshape(devices_all, pairs_here)
    atm_table = pair_atm.reshape(devices_all, pairs_here)
    numer_table = numerators.reshape(devices_all, pairs_here, PATCH_BLK, CELL_BLK)

    def add_device(accumulated, inputs):
        dev_blocks, patch_index, atm_index, numerator, live_count = inputs
        live_mask = (jnp.arange(pairs_here) < live_count).astype(jnp.float32)
        weight = (numerator.astype(jnp.float32) * SCALE).astype(jnp.bfloat16)
        weight = lax.optimization_barrier(weight).astype(jnp.float32)
        chosen = dev_blocks[patch_index.astype(jnp.int32)].astype(jnp.float32)
        partial_value = jnp.einsum("jpa,jpf->jaf", weight, chosen, precision=lax.Precision.HIGHEST)
        partial_value = partial_value * live_mask[:, None, None]
        return accumulated.at[atm_index.astype(jnp.int32)].add(partial_value), None

    initial = jnp.zeros((devices_all * blocks_owned, CELL_BLK, FLUX), jnp.float32)
    accumulated, unused = lax.scan(add_device, initial, (grouped, patch_table, atm_table, numer_table, counts))
    return accumulated.reshape(devices_all * blocks_owned * CELL_BLK, FLUX)
```

```python
import functools

import jax
import jax.numpy as jnp
from jax import lax
from jax.experimental import pallas as pl
from jax.experimental.pallas import tpu as pltpu
from jax.sharding import PartitionSpec as P

CELLS_DEV = 4096
SCALE = 2.0 ** (-27)
MESH = pl.DeviceIdType.MESH
LANES = 128


def partners(count):
    if count & (count - 1) == 0:
        return [lambda me, k=k: me ^ k for k in range(count - 1, 0, -1)]
    return [lambda me, k=k: lax.rem(me + k, count) for k in range(1, count)]


def pack_kernel(tiles, bucket, blocks_owned, chunk,
                patch_ref, atm_ref, counts_ref, patches_hbm, numer_hbm,
                send_ref, labels_ref,
                patches_v, numer_v, table, used, patch_sem, numer_sems):
    pairs = numer_v.shape[0]
    patch_rows = numer_v.shape[2]
    chunks = pairs // chunk
    buckets = tiles + 2
    patch_copy = pltpu.make_async_copy(patches_hbm, patches_v, patch_sem)
    patch_copy.start()
    copies = []
    for c in range(chunks):
        part = pl.ds(c * chunk, chunk)
        copy = pltpu.make_async_copy(numer_hbm.at[part], numer_v.at[part], numer_sems.at[c])
        copy.start()
        copies.append(copy)
    band = lax.axis_index("band")
    live = counts_ref[0]

    for b in range(buckets):
        used[b] = 0

        @pl.loop(0, blocks_owned, unroll=16)
        def _(i):
            table[b * blocks_owned + i] = -1

        for s in range(bucket):
            labels_ref[b, 0, s] = -1
    patch_copy.wait()
    for c in range(chunks):
        copies[c].wait()

        @pl.when(c * chunk < live)
        def _():
            for j in range(chunk):
                g = c * chunk + j
                is_live = g < live
                atm = atm_ref[g]
                owner = lax.div(atm, blocks_owned)
                block = lax.rem(atm, blocks_owned)
                owner_band = lax.div(owner, tiles)
                owner_tile = lax.rem(owner, tiles)
                b = jnp.where(owner_band == band, owner_tile,
                              jnp.where(owner_band > band, tiles, tiles + 1))
                entry = b * blocks_owned + block
                known = table[entry]
                fresh = known < 0
                new = used[b]
                rank = jnp.where(fresh, new, known)

                @pl.when(is_live)
                def _():
                    table[entry] = rank
                    used[b] = jnp.where(fresh, new + 1, new)
                    labels_ref[b, 0, rank] = block

                slot = jnp.where(is_live, b * bucket + rank, buckets * bucket)
                rows = pl.multiple_of(patch_ref[g] * patch_rows, patch_rows)
                weight = (numer_v[g].astype(jnp.float32) * SCALE).astype(jnp.bfloat16)
                part = jnp.dot(weight, patches_v[pl.ds(rows, patch_rows), :],
                               preferred_element_type=jnp.float32)
                before = send_ref[slot]
                send_ref[slot] = jnp.where(fresh, part, before + part)


def send_kernel(tiles, bands, bucket, send_ref, labels_ref, recv_ref, recv_labels_ref,
                data_send, data_recv, label_send, label_recv):
    band, tile = lax.axis_index("band"), lax.axis_index("tile")
    barrier = pltpu.get_barrier_semaphore()
    steps = partners(tiles)
    for step in steps:
        pl.semaphore_signal(barrier, inc=1, device_id=(band, step(tile)), device_id_type=MESH)

    @pl.when(band < bands - 1)
    def _():
        pl.semaphore_signal(barrier, inc=1, device_id=(band + 1, tile), device_id_type=MESH)

    @pl.when(band > 0)
    def _():
        pl.semaphore_signal(barrier, inc=1, device_id=(band - 1, tile), device_id_type=MESH)

    neighbours = jnp.where(band < bands - 1, 1, 0) + jnp.where(band > 0, 1, 0)
    pl.semaphore_wait(barrier, tiles - 1 + neighbours)

    def pair(source, place, device, sem):
        rows = pl.ds(source * bucket, bucket)
        landing = pl.ds(place * bucket, bucket)
        return (
            pltpu.make_async_remote_copy(
                src_ref=labels_ref.at[source], dst_ref=recv_labels_ref.at[place],
                send_sem=label_send.at[sem], recv_sem=label_recv.at[sem],
                device_id=device, device_id_type=MESH),
            pltpu.make_async_remote_copy(
                src_ref=send_ref.at[rows], dst_ref=recv_ref.at[landing],
                send_sem=data_send.at[sem], recv_sem=data_recv.at[sem],
                device_id=device, device_id_type=MESH),
        )

    inside = [pair(step(tile), tile, (band, step(tile)), k) for k, step in enumerate(steps)]
    upward = pair(tiles, tiles, (band + 1, tile), tiles - 1)
    downward = pair(tiles + 1, tiles + 1, (band - 1, tile), tiles)
    for copies in inside[:2]:
        for copy in copies:
            copy.start()

    @pl.when(band < bands - 1)
    def _():
        for copy in upward:
            copy.start()

    @pl.when(band > 0)
    def _():
        for copy in downward:
            copy.start()

    for copies in inside[2:]:
        for copy in copies:
            copy.start()
    for copies in inside:
        for copy in copies:
            copy.wait()

    @pl.when(band < bands - 1)
    def _():
        for up, down in zip(upward, downward):
            up.wait_send()
            down.wait_recv()

    @pl.when(band > 0)
    def _():
        for up, down in zip(upward, downward):
            down.wait_send()
            up.wait_recv()


def add_kernel(tiles, bands, bucket, labels_ref, recv_labels_ref, send_hbm, recv_hbm, out_ref,
               landed, sems):
    band, tile = lax.axis_index("band"), lax.axis_index("tile")
    buckets = tiles + 2

    def copy_of(b, ref):
        rows = pl.ds(b * bucket, bucket)
        return pltpu.make_async_copy(ref.at[rows], landed.at[rows], sems.at[b])

    for b in range(buckets):
        if b < tiles:
            @pl.when(tile == b)
            def _():
                copy_of(b, send_hbm).start()

            @pl.when(tile != b)
            def _():
                copy_of(b, recv_hbm).start()
        else:
            copy_of(b, recv_hbm).start()
    out_ref[...] = jnp.zeros_like(out_ref)
    for b in range(buckets):
        copy_of(b, recv_hbm).wait()
        if b == tiles:
            valid = band > 0
        elif b == tiles + 1:
            valid = band < bands - 1
        else:
            valid = True
        for s in range(bucket):
            label = recv_labels_ref[b, 0, s]
            if b < tiles:
                label = jnp.where(tile == b, labels_ref[b, 0, s], label)

            @pl.when((label >= 0) & valid)
            def _():
                out_ref[label] += landed[b * bucket + s]


def per_device(tiles, bands, patches, pair_patch, pair_atm, numerators, counts):
    pairs, patch_rows, cell_rows = numerators.shape
    flux = patches.shape[1]
    blocks_owned = CELLS_DEV // cell_rows
    bucket = pairs // 8
    buckets = tiles + 2
    chunk = 16
    smem = pl.BlockSpec(memory_space=pltpu.SMEM)
    vmem = pl.BlockSpec(memory_space=pltpu.VMEM)
    anywhere = pl.BlockSpec(memory_space=pl.ANY)
    labels_shape = jax.ShapeDtypeStruct((buckets, 1, LANES), jnp.int32)
    recv_shape = jax.ShapeDtypeStruct((buckets * bucket, cell_rows, flux), jnp.float32)
    send, labels = pl.pallas_call(
        functools.partial(pack_kernel, tiles, bucket, blocks_owned, chunk),
        out_shape=(jax.ShapeDtypeStruct((buckets * bucket + 1, cell_rows, flux), jnp.float32), labels_shape),
        in_specs=[smem, smem, smem, anywhere, anywhere],
        out_specs=(vmem, smem),
        scratch_shapes=[
            pltpu.VMEM(patches.shape, patches.dtype),
            pltpu.VMEM((pairs, cell_rows, patch_rows), jnp.int32),
            pltpu.SMEM((buckets * blocks_owned,), jnp.int32),
            pltpu.SMEM((buckets,), jnp.int32),
            pltpu.SemaphoreType.DMA,
            pltpu.SemaphoreType.DMA((pairs // chunk,)),
        ],
        name="pack",
    )(pair_patch, pair_atm, counts, patches, jnp.transpose(numerators, (0, 2, 1)))
    recv, recv_labels = pl.pallas_call(
        functools.partial(send_kernel, tiles, bands, bucket),
        out_shape=(recv_shape, labels_shape),
        in_specs=[anywhere, anywhere],
        out_specs=(anywhere, anywhere),
        scratch_shapes=[pltpu.SemaphoreType.DMA((tiles + 1,))] * 4,
        compiler_params=pltpu.CompilerParams(collective_id=0, has_side_effects=True),
        name="exchange",
    )(send, labels)
    out = pl.pallas_call(
        functools.partial(add_kernel, tiles, bands, bucket),
        out_shape=jax.ShapeDtypeStruct((blocks_owned, cell_rows, flux), jnp.float32),
        in_specs=[smem, smem, anywhere, anywhere],
        out_specs=vmem,
        scratch_shapes=[
            pltpu.VMEM(recv_shape.shape, jnp.float32),
            pltpu.SemaphoreType.DMA((buckets,)),
        ],
        name="add",
    )(labels, recv_labels, send, recv)
    return out.reshape(blocks_owned * cell_rows, flux)


def ring_order(tiles):
    wide = tiles // 4
    if wide * 4 != tiles or wide % 2:
        return list(range(tiles))
    order = list(range(wide))
    for step, column in enumerate(reversed(range(wide))):
        rows = range(1, 4) if step % 2 == 0 else range(3, 0, -1)
        order += [row * wide + column for row in rows]
    return order


def chosen(values, index):
    picked = values[0]
    for k in range(1, len(values)):
        picked = jnp.where(index == k, values[k], picked)
    return picked


def ring_tile(tiles, tile, steps):
    order = ring_order(tiles)
    position = chosen([order.index(k) for k in range(tiles)], tile)
    return chosen(order, lax.rem(position + steps + tiles, tiles))


def layout(bucket):
    return dict(up=4 * bucket, down=5 * bucket, own=6 * bucket, end=7 * bucket)


def reaching(tiles, bucket, way, read):
    reach = tiles // 2
    base = 7 * bucket - 1
    far = read(base + reach)
    counts = [read(base + (k if way == 0 else tiles - k)) for k in range(1, reach)]
    counts.append((far + 1) >> 1 if way == 0 else far >> 1)
    beyond = [0]
    for count in reversed(counts):
        beyond.append(beyond[-1] + count)
    return [None] + beyond[::-1]


def list_kernel(tiles, bands, bucket, blocks_owned, chunk,
                patch_ref, atm_ref, counts_ref, patches_hbm, numer_hbm,
                send_ref, labels_ref,
                patches_v, numer_v, table, used, base, spot, code, patch_sem, numer_sems):
    pairs = numer_v.shape[0]
    patch_rows = numer_v.shape[2]
    chunks = pairs // chunk
    reach = tiles // 2
    at = layout(bucket)
    patch_copy = pltpu.make_async_copy(patches_hbm, patches_v, patch_sem)
    patch_copy.start()
    copies = []
    for c in range(chunks):
        part = pl.ds(c * chunk, chunk)
        copy = pltpu.make_async_copy(numer_hbm.at[part], numer_v.at[part], numer_sems.at[c])
        copy.start()
        copies.append(copy)
    band, tile = lax.axis_index("band"), lax.axis_index("tile")
    live = counts_ref[0]
    order = ring_order(tiles)
    for k in range(tiles):
        spot[k] = order.index(k)
    here = spot[tile]

    @pl.loop(0, (tiles + 2) * blocks_owned, step=16)
    def _(i):
        for j in range(16):
            table[i + j] = -1

    for b in range(tiles + 2):
        used[b] = 0
    for s in range(LANES):
        labels_ref[0, s] = -1

    @pl.loop(0, live)
    def _(g):
        atm = atm_ref[g]
        owner = lax.div(atm, blocks_owned)
        block = lax.rem(atm, blocks_owned)
        owner_band = lax.div(owner, tiles)
        owner_tile = lax.rem(owner, tiles)
        ahead = lax.rem(spot[owner_tile] - here + tiles, tiles)
        b = jnp.where(owner_band == band, ahead, jnp.where(owner_band > band, tiles, tiles + 1))
        entry = b * blocks_owned + block
        known = table[entry]
        fresh = known < 0
        new = used[b]
        rank = jnp.where(fresh, new, known)
        table[entry] = rank
        used[b] = jnp.where(fresh, new + 1, new)
        code[g] = (b * pairs + rank) * 2 + jnp.where(fresh, 1, 0)

    half = (used[reach] + 1) >> 1
    start = half
    for k in range(reach - 1, 0, -1):
        base[k] = start
        start = start + used[k]
    total = start
    start = used[reach] - half
    for k in range(reach - 1, 0, -1):
        base[tiles - k] = 2 * bucket + start
        start = start + used[tiles - k]
    overflow = (total > 2 * bucket) | (start > 2 * bucket)
    base[0] = at["own"]
    base[reach] = 0
    base[tiles] = at["up"]
    base[tiles + 1] = at["down"]

    patch_copy.wait()
    for c in range(chunks):
        copies[c].wait()

        @pl.when(c * chunk < live)
        def _():
            for j in range(chunk):
                g = c * chunk + j
                is_live = g < live
                value = jnp.where(is_live, code[g], 0)
                fresh = (value & 1) == 1
                rank = lax.rem(value >> 1, pairs)
                b = lax.div(value >> 1, pairs)
                back = (b == reach) & (rank >= half)
                slot = jnp.where(back, 2 * bucket - half, base[b]) + rank
                slot = jnp.where(is_live, jnp.minimum(slot, at["end"]), at["end"])
                labels_ref[0, slot] = lax.rem(atm_ref[g], blocks_owned)
                rows = pl.multiple_of(patch_ref[g] * patch_rows, patch_rows)
                weight = (numer_v[g].astype(jnp.float32) * SCALE).astype(jnp.bfloat16)
                part = jnp.dot(weight, patches_v[pl.ds(rows, patch_rows), :],
                               preferred_element_type=jnp.float32)
                before = send_ref[slot]
                send_ref[slot] = jnp.where(fresh, part, before + part)

    for k in range(1, tiles):
        labels_ref[0, at["end"] - 1 + k] = used[k]
    labels_ref[0, LANES - 1] = jnp.where(overflow, 1, 0)


def starts(reach, lag, reaches):
    first = [None] * (reach + 1)
    for u in range(reach - 1, -1, -1):
        begin = [0]
        for j in range(1, reach - u):
            after = begin[j - 1] + reaches[u + j - 1][j]
            begin.append(jnp.maximum(after, first[u + 1][j - 1] + lag))
        first[u] = begin
    end = first[0][reach - 1] + reaches[reach - 1][reach]
    return first[0], first[1], end


def stream_kernel(tiles, bands, bucket, plans, send_ref, labels_ref,
                  pool_ref, beside_ref, table_ref, plan_ref,
                  stage, recv, landing, marks, mark,
                  ring_send, ring_recv, beside_send, beside_recv, label_send, label_recv, local_sem):
    band, tile = lax.axis_index("band"), lax.axis_index("tile")
    reach = tiles // 2
    own_rows = 2 * bucket
    at = layout(bucket)
    steps = partners(tiles)
    mine = pltpu.make_async_copy(labels_ref, landing.at[tile], local_sem)
    mine.start()
    barrier = pltpu.get_barrier_semaphore()
    for step in steps:
        pl.semaphore_signal(barrier, inc=1, device_id=(band, step(tile)), device_id_type=MESH)
    for j in range(1, bands):
        pl.semaphore_signal(barrier, inc=1, device_id=(lax.rem(band + j, bands), tile), device_id_type=MESH)
    pl.semaphore_wait(barrier, tiles + bands - 2)

    targets = ((band, ring_tile(tiles, tile, 1)), (band, ring_tile(tiles, tile, -1)))
    is_edge = (band == 0) | (band == bands - 1)
    inside = [
        pltpu.make_async_remote_copy(
            src_ref=labels_ref, dst_ref=landing.at[tile],
            send_sem=label_send.at[k], recv_sem=label_recv.at[k],
            device_id=(band, step(tile)), device_id_type=MESH)
        for k, step in enumerate(steps)
    ]
    across = [
        pltpu.make_async_remote_copy(
            src_ref=mark, dst_ref=marks.at[band],
            send_sem=label_send.at[tiles - 2 + j], recv_sem=label_recv.at[tiles - 2 + j],
            device_id=(lax.rem(band + j, bands), tile), device_id_type=MESH)
        for j in range(1, bands)
    ]
    for copy in inside:
        copy.start()

    def hop(way, r, size, source):
        rows = pl.ds(r * size, size)
        return pltpu.make_async_remote_copy(
            src_ref=source, dst_ref=recv.at[way, rows],
            send_sem=ring_send.at[way, r], recv_sem=ring_recv.at[way, r],
            device_id=targets[way], device_id_type=MESH)

    def own_hop(way, r, size):
        return hop(way, r, size, send_ref.at[pl.ds(way * own_rows + r * size, size)])

    def later_hop(way, r, size):
        return hop(way, r, size, stage.at[way, pl.ds(r * size, size)])

    for edge in (True, False):
        size, rounds, lag = plans[0 if edge else 1]

        @pl.when(is_edge if edge else jnp.logical_not(is_edge))
        def _():
            for r in range(lag):
                for way in range(2):
                    own_hop(way, r, size).start()

    def beside(way, target_band):
        return pltpu.make_async_remote_copy(
            src_ref=send_ref.at[pl.ds(at["up"] + way * bucket, bucket)], dst_ref=beside_ref.at[way],
            send_sem=beside_send.at[way], recv_sem=beside_recv.at[way],
            device_id=(target_band, tile), device_id_type=MESH)

    upward, downward = beside(0, band + 1), beside(1, band - 1)

    @pl.when(band < bands - 1)
    def _():
        upward.start()

    @pl.when(band > 0)
    def _():
        downward.start()

    for way in range(2):
        pool_ref[way, 0:own_rows] = send_ref[way * own_rows:(way + 1) * own_rows]
    mine.wait()
    for copy in inside:
        copy.wait()
    rows_in = pltpu.make_async_copy(landing, table_ref.at[pl.ds(0, tiles)], local_sem)
    rows_in.start()
    rows_in.wait()

    upstream = [[ring_tile(tiles, tile, -u if way == 0 else u) for u in range(tiles)] for way in range(2)]
    reaches = [[reaching(tiles, bucket, way, lambda i, t=t: table_ref[t, 0, i]) for t in upstream[way]]
               for way in range(2)]
    lag_slots = jnp.where(is_edge, plans[0][0] * plans[0][2], plans[1][0] * plans[1][2])
    capacity = jnp.where(is_edge, plans[0][0] * plans[0][1], plans[1][0] * plans[1][1])
    worst = jnp.int32(0)
    flag = jnp.int32(0)
    begins = []
    for way in range(2):
        for v in range(tiles):
            ahead, behind, end = starts(reach, lag_slots, [reaches[way][(v + u) % tiles] for u in range(reach)])
            worst = jnp.maximum(worst, end)
            if v == 0:
                begins.append(ahead)
    arrivals = []
    for way in range(2):
        ahead, _, _ = starts(reach, lag_slots, [reaches[way][(1 + u) % tiles] for u in range(reach)])
        arrivals.append(ahead)
    for t in range(tiles):
        flag = jnp.maximum(flag, table_ref[t, 0, LANES - 1])
    flag = jnp.where(worst > capacity, 1, flag)
    lane = lax.broadcasted_iota(jnp.int32, (1, LANES), 1)
    mark[...] = jnp.where(lane == LANES - 1, flag, landing[tile])
    for way in range(2):
        for j in range(reach):
            plan_ref[0, 1 + way * reach + j] = arrivals[way][j]

    for edge in (True, False):
        size, rounds, lag = plans[0 if edge else 1]
        last_row = own_rows + size * rounds - 1

        @pl.when(is_edge if edge else jnp.logical_not(is_edge))
        def _():
            def keep(way, r):
                later_hop(way, r, size).wait_recv()
                pool_ref[way, pl.ds(own_rows + r * size, size)] = recv[way, pl.ds(r * size, size)]

            def gather(way, r):
                begin, arrived = begins[way], arrivals[way]
                for s in range(size):
                    p = r * size + s
                    row = jnp.minimum(p, own_rows - 1)
                    for j in range(1, reach):
                        row = jnp.where(p >= begin[j], p + (own_rows + arrived[j - 1] - begin[j]), row)
                    row = jnp.clip(row, 0, last_row)
                    stage[way, p] = pool_ref[way, row]

            def one_round(r):
                for way in range(2):
                    keep(way, r - lag)
                for way in range(2):
                    gather(way, r)
                for way in range(2):
                    later_hop(way, r, size).start()

            one_round(lag)
            for copy in across:
                copy.start()

            @pl.loop(lag + 1, rounds)
            def _(r):
                one_round(r)

            @pl.loop(rounds - lag, rounds)
            def _(r):
                for way in range(2):
                    keep(way, r)

            @pl.loop(0, rounds)
            def _(r):
                for way in range(2):
                    later_hop(way, r, size).wait_send()

    for copy in across:
        copy.wait()
    rows_over = pltpu.make_async_copy(marks, table_ref.at[pl.ds(tiles, bands)], local_sem)
    rows_over.start()
    rows_over.wait()
    for j in range(1, bands):
        flag = jnp.maximum(flag, table_ref[tiles + lax.rem(band + j, bands), 0, LANES - 1])
    plan_ref[0, 0] = flag

    @pl.when(band < bands - 1)
    def _():
        upward.wait_send()
        downward.wait_recv()

    @pl.when(band > 0)
    def _():
        downward.wait_send()
        upward.wait_recv()


def take_kernel(tiles, bands, bucket, table_ref, plan_ref, send_ref, pool_ref, beside_ref, out_ref):
    band, tile = lax.axis_index("band"), lax.axis_index("tile")
    reach = tiles // 2
    own_rows = 2 * bucket
    at = layout(bucket)
    out_ref[...] = jnp.zeros_like(out_ref)
    for s in range(bucket):
        label = table_ref[tile, 0, at["own"] + s]

        @pl.when(label >= 0)
        def _():
            out_ref[label] += send_ref[at["own"] + s]

    for way in range(2):
        other = tiles + jnp.clip(band - 1 if way == 0 else band + 1, 0, bands - 1)
        valid = (band > 0) if way == 0 else (band < bands - 1)
        for s in range(bucket):
            label = table_ref[other, 0, at["up"] + way * bucket + s]

            @pl.when((label >= 0) & valid)
            def _():
                out_ref[label] += beside_ref[way, s]

    for way in range(2):
        for distance in range(1, reach + 1):
            source = ring_tile(tiles, tile, -distance if way == 0 else distance)
            reaches = reaching(tiles, bucket, way, lambda i: table_ref[source, 0, i])
            start = own_rows + plan_ref[0, 1 + way * reach + distance - 1]

            @pl.loop(reaches[distance + 1], reaches[distance])
            def _(i):
                out_ref[table_ref[source, 0, way * own_rows + i]] += pool_ref[way, start + i]


def adaptive(tiles, bands, patches, pair_patch, pair_atm, numerators, counts):
    pairs, patch_rows, cell_rows = numerators.shape
    flux = patches.shape[1]
    blocks_owned = CELLS_DEV // cell_rows
    bucket = pairs // 8
    reach = tiles // 2
    chunk = 16
    plans = ((5, 4 * reach, 3), (3, 4 * reach, 3))
    slots = max(size * rounds for size, rounds, _ in plans)
    most = max(rounds for _, rounds, _ in plans)
    smem = pl.BlockSpec(memory_space=pltpu.SMEM)
    vmem = pl.BlockSpec(memory_space=pltpu.VMEM)
    anywhere = pl.BlockSpec(memory_space=pl.ANY)
    block = (cell_rows, flux)
    f32 = jnp.float32
    send, labels = pl.pallas_call(
        functools.partial(list_kernel, tiles, bands, bucket, blocks_owned, chunk),
        out_shape=(jax.ShapeDtypeStruct((7 * bucket + 1,) + block, f32),
                   jax.ShapeDtypeStruct((1, LANES), jnp.int32)),
        in_specs=[smem, smem, smem, anywhere, anywhere],
        out_specs=(vmem, smem),
        scratch_shapes=[
            pltpu.VMEM(patches.shape, patches.dtype),
            pltpu.VMEM((pairs, cell_rows, patch_rows), jnp.int32),
            pltpu.SMEM(((tiles + 2) * blocks_owned,), jnp.int32),
            pltpu.SMEM((tiles + 2,), jnp.int32),
            pltpu.SMEM((tiles + 2,), jnp.int32),
            pltpu.SMEM((tiles,), jnp.int32),
            pltpu.SMEM((pairs,), jnp.int32),
            pltpu.SemaphoreType.DMA,
            pltpu.SemaphoreType.DMA((pairs // chunk,)),
        ],
        name="list",
    )(pair_patch, pair_atm, counts, patches, jnp.transpose(numerators, (0, 2, 1)))
    pool, beside, table, plan = pl.pallas_call(
        functools.partial(stream_kernel, tiles, bands, bucket, plans),
        out_shape=(jax.ShapeDtypeStruct((2, 2 * bucket + slots) + block, f32),
                   jax.ShapeDtypeStruct((2, bucket) + block, f32),
                   jax.ShapeDtypeStruct((tiles + bands, 1, LANES), jnp.int32),
                   jax.ShapeDtypeStruct((1, LANES), jnp.int32)),
        in_specs=[vmem, vmem],
        out_specs=(vmem, vmem, smem, smem),
        scratch_shapes=[
            pltpu.VMEM((2, slots) + block, f32),
            pltpu.VMEM((2, slots) + block, f32),
            pltpu.VMEM((tiles, 1, LANES), jnp.int32),
            pltpu.VMEM((bands, 1, LANES), jnp.int32),
            pltpu.VMEM((1, LANES), jnp.int32),
            pltpu.SemaphoreType.DMA((2, most)),
            pltpu.SemaphoreType.DMA((2, most)),
            pltpu.SemaphoreType.DMA((2,)),
            pltpu.SemaphoreType.DMA((2,)),
            pltpu.SemaphoreType.DMA((tiles + bands - 2,)),
            pltpu.SemaphoreType.DMA((tiles + bands - 2,)),
            pltpu.SemaphoreType.DMA,
        ],
        compiler_params=pltpu.CompilerParams(collective_id=1, has_side_effects=True),
        name="stream",
    )(send, labels)

    def take(patches, pair_patch, pair_atm, numerators, counts, table, plan, send, pool, beside):
        out = pl.pallas_call(
            functools.partial(take_kernel, tiles, bands, bucket),
            out_shape=jax.ShapeDtypeStruct((blocks_owned,) + block, f32),
            in_specs=[smem, smem, vmem, vmem, vmem],
            out_specs=vmem,
            name="take",
        )(table, plan, send, pool, beside)
        return out.reshape(blocks_owned * cell_rows, flux)

    def padded(patches, pair_patch, pair_atm, numerators, counts, table, plan, send, pool, beside):
        return per_device(tiles, bands, patches, pair_patch, pair_atm, numerators, counts)

    return lax.cond(plan[0, 0] > 0, padded, take, patches, pair_patch, pair_atm, numerators, counts,
                    table, plan, send, pool, beside)


def solution(mesh):
    spec = P(("band", "tile"))
    placed = (
        P(("band", "tile"), None),
        spec,
        spec,
        P(("band", "tile"), None, None),
        spec,
    )
    body = functools.partial(adaptive, mesh.shape["tile"], mesh.shape["band"])
    return jax.shard_map(body, mesh=mesh, in_specs=placed, out_specs=P(("band", "tile"), None), check_vma=False)
```

```python
import functools

import jax
import jax.numpy as jnp
from jax import lax
from jax.experimental import pallas as pl
from jax.experimental.pallas import tpu as pltpu
from jax.sharding import PartitionSpec as P

CELLS_DEV = 4096
SCALE = 2.0 ** (-27)
MESH = pl.DeviceIdType.MESH
LANES = 128
VMEM_LIMIT = 20 * 2 ** 20


def partners(count):
    if count & (count - 1) == 0:
        return [lambda me, k=k: me ^ k for k in range(count - 1, 0, -1)]
    return [lambda me, k=k: lax.rem(me + k, count) for k in range(1, count)]


def pack_kernel(tiles, bucket, blocks_owned, chunk,
                patch_ref, atm_ref, counts_ref, patches_hbm, numer_hbm,
                send_ref, labels_ref,
                patches_v, numer_v, table, used, patch_sem, numer_sems):
    pairs = numer_v.shape[0]
    patch_rows = numer_v.shape[2]
    chunks = pairs // chunk
    buckets = tiles + 2
    patch_copy = pltpu.make_async_copy(patches_hbm, patches_v, patch_sem)
    patch_copy.start()
    copies = []
    for c in range(chunks):
        part = pl.ds(c * chunk, chunk)
        copy = pltpu.make_async_copy(numer_hbm.at[part], numer_v.at[part], numer_sems.at[c])
        copy.start()
        copies.append(copy)
    band = lax.axis_index("band")
    live = counts_ref[0]

    for b in range(buckets):
        used[b] = 0

        @pl.loop(0, blocks_owned, unroll=16)
        def _(i):
            table[b * blocks_owned + i] = -1

        for s in range(bucket):
            labels_ref[b, 0, s] = -1
    patch_copy.wait()
    for c in range(chunks):
        copies[c].wait()

        @pl.when(c * chunk < live)
        def _():
            for j in range(chunk):
                g = c * chunk + j
                is_live = g < live
                atm = atm_ref[g]
                owner = lax.div(atm, blocks_owned)
                block = lax.rem(atm, blocks_owned)
                owner_band = lax.div(owner, tiles)
                owner_tile = lax.rem(owner, tiles)
                b = jnp.where(owner_band == band, owner_tile,
                              jnp.where(owner_band > band, tiles, tiles + 1))
                entry = b * blocks_owned + block
                known = table[entry]
                fresh = known < 0
                new = used[b]
                rank = jnp.where(fresh, new, known)

                @pl.when(is_live)
                def _():
                    table[entry] = rank
                    used[b] = jnp.where(fresh, new + 1, new)
                    labels_ref[b, 0, rank] = block

                slot = jnp.where(is_live, b * bucket + rank, buckets * bucket)
                rows = pl.multiple_of(patch_ref[g] * patch_rows, patch_rows)
                weight = (numer_v[g].astype(jnp.float32) * SCALE).astype(jnp.bfloat16)
                part = jnp.dot(weight, patches_v[pl.ds(rows, patch_rows), :],
                               preferred_element_type=jnp.float32)
                before = send_ref[slot]
                send_ref[slot] = jnp.where(fresh, part, before + part)


def send_kernel(tiles, bands, bucket, send_ref, labels_ref, recv_ref, recv_labels_ref,
                data_send, data_recv, label_send, label_recv):
    band, tile = lax.axis_index("band"), lax.axis_index("tile")
    barrier = pltpu.get_barrier_semaphore()
    steps = partners(tiles)
    for step in steps:
        pl.semaphore_signal(barrier, inc=1, device_id=(band, step(tile)), device_id_type=MESH)

    @pl.when(band < bands - 1)
    def _():
        pl.semaphore_signal(barrier, inc=1, device_id=(band + 1, tile), device_id_type=MESH)

    @pl.when(band > 0)
    def _():
        pl.semaphore_signal(barrier, inc=1, device_id=(band - 1, tile), device_id_type=MESH)

    neighbours = jnp.where(band < bands - 1, 1, 0) + jnp.where(band > 0, 1, 0)
    pl.semaphore_wait(barrier, tiles - 1 + neighbours)

    def pair(source, place, device, sem):
        rows = pl.ds(source * bucket, bucket)
        landing = pl.ds(place * bucket, bucket)
        return (
            pltpu.make_async_remote_copy(
                src_ref=labels_ref.at[source], dst_ref=recv_labels_ref.at[place],
                send_sem=label_send.at[sem], recv_sem=label_recv.at[sem],
                device_id=device, device_id_type=MESH),
            pltpu.make_async_remote_copy(
                src_ref=send_ref.at[rows], dst_ref=recv_ref.at[landing],
                send_sem=data_send.at[sem], recv_sem=data_recv.at[sem],
                device_id=device, device_id_type=MESH),
        )

    inside = [pair(step(tile), tile, (band, step(tile)), k) for k, step in enumerate(steps)]
    upward = pair(tiles, tiles, (band + 1, tile), tiles - 1)
    downward = pair(tiles + 1, tiles + 1, (band - 1, tile), tiles)
    for copies in inside[:2]:
        for copy in copies:
            copy.start()

    @pl.when(band < bands - 1)
    def _():
        for copy in upward:
            copy.start()

    @pl.when(band > 0)
    def _():
        for copy in downward:
            copy.start()

    for copies in inside[2:]:
        for copy in copies:
            copy.start()
    for copies in inside:
        for copy in copies:
            copy.wait()

    @pl.when(band < bands - 1)
    def _():
        for up, down in zip(upward, downward):
            up.wait_send()
            down.wait_recv()

    @pl.when(band > 0)
    def _():
        for up, down in zip(upward, downward):
            down.wait_send()
            up.wait_recv()


def add_kernel(tiles, bands, bucket, labels_ref, recv_labels_ref, send_hbm, recv_hbm, out_ref,
               landed, sems):
    band, tile = lax.axis_index("band"), lax.axis_index("tile")
    buckets = tiles + 2

    def copy_of(b, ref):
        rows = pl.ds(b * bucket, bucket)
        return pltpu.make_async_copy(ref.at[rows], landed.at[rows], sems.at[b])

    for b in range(buckets):
        if b < tiles:
            @pl.when(tile == b)
            def _():
                copy_of(b, send_hbm).start()

            @pl.when(tile != b)
            def _():
                copy_of(b, recv_hbm).start()
        else:
            copy_of(b, recv_hbm).start()
    out_ref[...] = jnp.zeros_like(out_ref)
    for b in range(buckets):
        copy_of(b, recv_hbm).wait()
        if b == tiles:
            valid = band > 0
        elif b == tiles + 1:
            valid = band < bands - 1
        else:
            valid = True
        for s in range(bucket):
            label = recv_labels_ref[b, 0, s]
            if b < tiles:
                label = jnp.where(tile == b, labels_ref[b, 0, s], label)

            @pl.when((label >= 0) & valid)
            def _():
                out_ref[label] += landed[b * bucket + s]


def per_device(tiles, bands, patches, pair_patch, pair_atm, numerators, counts):
    pairs, patch_rows, cell_rows = numerators.shape
    flux = patches.shape[1]
    blocks_owned = CELLS_DEV // cell_rows
    bucket = pairs // 8
    buckets = tiles + 2
    chunk = 16
    smem = pl.BlockSpec(memory_space=pltpu.SMEM)
    vmem = pl.BlockSpec(memory_space=pltpu.VMEM)
    anywhere = pl.BlockSpec(memory_space=pl.ANY)
    labels_shape = jax.ShapeDtypeStruct((buckets, 1, LANES), jnp.int32)
    recv_shape = jax.ShapeDtypeStruct((buckets * bucket, cell_rows, flux), jnp.float32)
    send, labels = pl.pallas_call(
        functools.partial(pack_kernel, tiles, bucket, blocks_owned, chunk),
        out_shape=(jax.ShapeDtypeStruct((buckets * bucket + 1, cell_rows, flux), jnp.float32), labels_shape),
        in_specs=[smem, smem, smem, anywhere, anywhere],
        out_specs=(vmem, smem),
        scratch_shapes=[
            pltpu.VMEM(patches.shape, patches.dtype),
            pltpu.VMEM((pairs, cell_rows, patch_rows), jnp.int32),
            pltpu.SMEM((buckets * blocks_owned,), jnp.int32),
            pltpu.SMEM((buckets,), jnp.int32),
            pltpu.SemaphoreType.DMA,
            pltpu.SemaphoreType.DMA((pairs // chunk,)),
        ],
        compiler_params=pltpu.CompilerParams(vmem_limit_bytes=VMEM_LIMIT),
        name="pack",
    )(pair_patch, pair_atm, counts, patches, jnp.transpose(numerators, (0, 2, 1)))
    recv, recv_labels = pl.pallas_call(
        functools.partial(send_kernel, tiles, bands, bucket),
        out_shape=(recv_shape, labels_shape),
        in_specs=[anywhere, anywhere],
        out_specs=(anywhere, anywhere),
        scratch_shapes=[pltpu.SemaphoreType.DMA((tiles + 1,))] * 4,
        compiler_params=pltpu.CompilerParams(collective_id=0, has_side_effects=True, vmem_limit_bytes=VMEM_LIMIT),
        name="exchange",
    )(send, labels)
    out = pl.pallas_call(
        functools.partial(add_kernel, tiles, bands, bucket),
        out_shape=jax.ShapeDtypeStruct((blocks_owned, cell_rows, flux), jnp.float32),
        in_specs=[smem, smem, anywhere, anywhere],
        out_specs=vmem,
        scratch_shapes=[
            pltpu.VMEM(recv_shape.shape, jnp.float32),
            pltpu.SemaphoreType.DMA((buckets,)),
        ],
        compiler_params=pltpu.CompilerParams(vmem_limit_bytes=VMEM_LIMIT),
        name="add",
    )(labels, recv_labels, send, recv)
    return out.reshape(blocks_owned * cell_rows, flux)


def ring_order(tiles):
    wide = tiles // 4
    if wide * 4 != tiles or wide % 2:
        return list(range(tiles))
    order = list(range(wide))
    for step, column in enumerate(reversed(range(wide))):
        rows = range(1, 4) if step % 2 == 0 else range(3, 0, -1)
        order += [row * wide + column for row in rows]
    return order


def chosen(values, index):
    picked = values[0]
    for k in range(1, len(values)):
        picked = jnp.where(index == k, values[k], picked)
    return picked


def ring_tile(tiles, tile, steps):
    order = ring_order(tiles)
    position = chosen([order.index(k) for k in range(tiles)], tile)
    return chosen(order, lax.rem(position + steps + tiles, tiles))


def layout(bucket):
    return dict(up=4 * bucket, down=5 * bucket, own=6 * bucket, end=7 * bucket)


def reaching(tiles, bucket, way, read):
    reach = tiles // 2
    base = 7 * bucket - 1
    far = read(base + reach)
    counts = [read(base + (k if way == 0 else tiles - k)) for k in range(1, reach)]
    counts.append((far + 1) >> 1 if way == 0 else far >> 1)
    beyond = [0]
    for count in reversed(counts):
        beyond.append(beyond[-1] + count)
    return [None] + beyond[::-1]


def list_kernel(tiles, bands, bucket, blocks_owned, chunk,
                patch_ref, atm_ref, counts_ref, patches_hbm, numer_hbm,
                send_ref, labels_ref,
                patches_v, numer_v, table, used, base, spot, code, patch_sem, numer_sems):
    pairs = numer_v.shape[0]
    patch_rows = numer_v.shape[2]
    chunks = pairs // chunk
    reach = tiles // 2
    at = layout(bucket)
    patch_copy = pltpu.make_async_copy(patches_hbm, patches_v, patch_sem)
    patch_copy.start()
    copies = []
    for c in range(chunks):
        part = pl.ds(c * chunk, chunk)
        copy = pltpu.make_async_copy(numer_hbm.at[part], numer_v.at[part], numer_sems.at[c])
        copy.start()
        copies.append(copy)
    band, tile = lax.axis_index("band"), lax.axis_index("tile")
    live = counts_ref[0]
    order = ring_order(tiles)
    for k in range(tiles):
        spot[k] = order.index(k)
    here = spot[tile]

    @pl.loop(0, (tiles + 2) * blocks_owned, step=16)
    def _(i):
        for j in range(16):
            table[i + j] = -1

    for b in range(tiles + 2):
        used[b] = 0
    for s in range(LANES):
        labels_ref[0, s] = -1

    @pl.loop(0, live)
    def _(g):
        atm = atm_ref[g]
        owner = lax.div(atm, blocks_owned)
        block = lax.rem(atm, blocks_owned)
        owner_band = lax.div(owner, tiles)
        owner_tile = lax.rem(owner, tiles)
        ahead = lax.rem(spot[owner_tile] - here + tiles, tiles)
        b = jnp.where(owner_band == band, ahead, jnp.where(owner_band > band, tiles, tiles + 1))
        entry = b * blocks_owned + block
        known = table[entry]
        fresh = known < 0
        new = used[b]
        rank = jnp.where(fresh, new, known)
        table[entry] = rank
        used[b] = jnp.where(fresh, new + 1, new)
        code[g] = (b * pairs + rank) * 2 + jnp.where(fresh, 1, 0)

    half = (used[reach] + 1) >> 1
    start = half
    for k in range(reach - 1, 0, -1):
        base[k] = start
        start = start + used[k]
    total = start
    start = used[reach] - half
    for k in range(reach - 1, 0, -1):
        base[tiles - k] = 2 * bucket + start
        start = start + used[tiles - k]
    overflow = (total > 2 * bucket) | (start > 2 * bucket)
    base[0] = at["own"]
    base[reach] = 0
    base[tiles] = at["up"]
    base[tiles + 1] = at["down"]

    patch_copy.wait()
    for c in range(chunks):
        copies[c].wait()

        @pl.when(c * chunk < live)
        def _():
            for j in range(chunk):
                g = c * chunk + j
                is_live = g < live
                value = jnp.where(is_live, code[g], 0)
                fresh = (value & 1) == 1
                rank = lax.rem(value >> 1, pairs)
                b = lax.div(value >> 1, pairs)
                back = (b == reach) & (rank >= half)
                slot = jnp.where(back, 2 * bucket - half, base[b]) + rank
                slot = jnp.where(is_live, jnp.minimum(slot, at["end"]), at["end"])
                labels_ref[0, slot] = lax.rem(atm_ref[g], blocks_owned)
                rows = pl.multiple_of(patch_ref[g] * patch_rows, patch_rows)
                weight = (numer_v[g].astype(jnp.float32) * SCALE).astype(jnp.bfloat16)
                part = jnp.dot(weight, patches_v[pl.ds(rows, patch_rows), :],
                               preferred_element_type=jnp.float32)
                before = send_ref[slot]
                send_ref[slot] = jnp.where(fresh, part, before + part)

    for k in range(1, tiles):
        labels_ref[0, at["end"] - 1 + k] = used[k]
    labels_ref[0, LANES - 1] = jnp.where(overflow, 1, 0)


def starts(reach, lag, reaches):
    first = [None] * (reach + 1)
    for u in range(reach - 1, -1, -1):
        begin = [0]
        for j in range(1, reach - u):
            after = begin[j - 1] + reaches[u + j - 1][j]
            begin.append(jnp.maximum(after, first[u + 1][j - 1] + lag))
        first[u] = begin
    end = first[0][reach - 1] + reaches[reach - 1][reach]
    return first[0], first[1], end


def stream_kernel(tiles, bands, bucket, plans, send_ref, labels_ref,
                  pool_ref, beside_ref, table_ref, plan_ref,
                  stage, recv, landing, marks, mark,
                  ring_send, ring_recv, beside_send, beside_recv, label_send, label_recv, local_sem):
    band, tile = lax.axis_index("band"), lax.axis_index("tile")
    reach = tiles // 2
    own_rows = 2 * bucket
    at = layout(bucket)
    steps = partners(tiles)
    mine = pltpu.make_async_copy(labels_ref, landing.at[tile], local_sem)
    mine.start()
    barrier = pltpu.get_barrier_semaphore()
    for step in steps:
        pl.semaphore_signal(barrier, inc=1, device_id=(band, step(tile)), device_id_type=MESH)
    for j in range(1, bands):
        pl.semaphore_signal(barrier, inc=1, device_id=(lax.rem(band + j, bands), tile), device_id_type=MESH)
    pl.semaphore_wait(barrier, tiles + bands - 2)

    targets = ((band, ring_tile(tiles, tile, 1)), (band, ring_tile(tiles, tile, -1)))
    is_edge = (band == 0) | (band == bands - 1)
    inside = [
        pltpu.make_async_remote_copy(
            src_ref=labels_ref, dst_ref=landing.at[tile],
            send_sem=label_send.at[k], recv_sem=label_recv.at[k],
            device_id=(band, step(tile)), device_id_type=MESH)
        for k, step in enumerate(steps)
    ]
    across = [
        pltpu.make_async_remote_copy(
            src_ref=mark, dst_ref=marks.at[band],
            send_sem=label_send.at[tiles - 2 + j], recv_sem=label_recv.at[tiles - 2 + j],
            device_id=(lax.rem(band + j, bands), tile), device_id_type=MESH)
        for j in range(1, bands)
    ]
    for copy in inside:
        copy.start()

    def hop(way, r, size, source):
        rows = pl.ds(r * size, size)
        return pltpu.make_async_remote_copy(
            src_ref=source, dst_ref=recv.at[way, rows],
            send_sem=ring_send.at[way, r], recv_sem=ring_recv.at[way, r],
            device_id=targets[way], device_id_type=MESH)

    def own_hop(way, r, size):
        return hop(way, r, size, send_ref.at[pl.ds(way * own_rows + r * size, size)])

    def later_hop(way, r, size):
        return hop(way, r, size, stage.at[way, pl.ds(r * size, size)])

    for edge in (True, False):
        size, rounds, lag = plans[0 if edge else 1]

        @pl.when(is_edge if edge else jnp.logical_not(is_edge))
        def _():
            for r in range(lag):
                for way in range(2):
                    own_hop(way, r, size).start()

    def beside(way, target_band):
        return pltpu.make_async_remote_copy(
            src_ref=send_ref.at[pl.ds(at["up"] + way * bucket, bucket)], dst_ref=beside_ref.at[way],
            send_sem=beside_send.at[way], recv_sem=beside_recv.at[way],
            device_id=(target_band, tile), device_id_type=MESH)

    upward, downward = beside(0, band + 1), beside(1, band - 1)

    @pl.when(band < bands - 1)
    def _():
        upward.start()

    @pl.when(band > 0)
    def _():
        downward.start()

    for way in range(2):
        pool_ref[way, 0:own_rows] = send_ref[way * own_rows:(way + 1) * own_rows]
    mine.wait()
    for copy in inside:
        copy.wait()
    rows_in = pltpu.make_async_copy(landing, table_ref.at[pl.ds(0, tiles)], local_sem)
    rows_in.start()
    rows_in.wait()

    upstream = [[ring_tile(tiles, tile, -u if way == 0 else u) for u in range(tiles)] for way in range(2)]
    reaches = [[reaching(tiles, bucket, way, lambda i, t=t: table_ref[t, 0, i]) for t in upstream[way]]
               for way in range(2)]
    lag_slots = jnp.where(is_edge, plans[0][0] * plans[0][2], plans[1][0] * plans[1][2])
    capacity = jnp.where(is_edge, plans[0][0] * plans[0][1], plans[1][0] * plans[1][1])
    worst = jnp.int32(0)
    flag = jnp.int32(0)
    begins = []
    for way in range(2):
        for v in range(tiles):
            ahead, behind, end = starts(reach, lag_slots, [reaches[way][(v + u) % tiles] for u in range(reach)])
            worst = jnp.maximum(worst, end)
            if v == 0:
                begins.append(ahead)
    arrivals = []
    for way in range(2):
        ahead, _, _ = starts(reach, lag_slots, [reaches[way][(1 + u) % tiles] for u in range(reach)])
        arrivals.append(ahead)
    for t in range(tiles):
        flag = jnp.maximum(flag, table_ref[t, 0, LANES - 1])
    flag = jnp.where(worst > capacity, 1, flag)
    lane = lax.broadcasted_iota(jnp.int32, (1, LANES), 1)
    mark[...] = jnp.where(lane == LANES - 1, flag, landing[tile])
    for way in range(2):
        for j in range(reach):
            plan_ref[0, 1 + way * reach + j] = arrivals[way][j]

    for edge in (True, False):
        size, rounds, lag = plans[0 if edge else 1]
        last_row = own_rows + size * rounds - 1

        @pl.when(is_edge if edge else jnp.logical_not(is_edge))
        def _():
            def keep(way, r):
                later_hop(way, r, size).wait_recv()
                pool_ref[way, pl.ds(own_rows + r * size, size)] = recv[way, pl.ds(r * size, size)]

            def gather(way, r):
                begin, arrived = begins[way], arrivals[way]
                for s in range(size):
                    p = r * size + s
                    row = jnp.minimum(p, own_rows - 1)
                    for j in range(1, reach):
                        row = jnp.where(p >= begin[j], p + (own_rows + arrived[j - 1] - begin[j]), row)
                    row = jnp.clip(row, 0, last_row)
                    stage[way, p] = pool_ref[way, row]

            def one_round(r):
                for way in range(2):
                    keep(way, r - lag)
                for way in range(2):
                    gather(way, r)
                for way in range(2):
                    later_hop(way, r, size).start()

            one_round(lag)
            for copy in across:
                copy.start()

            @pl.loop(lag + 1, rounds)
            def _(r):
                one_round(r)

            @pl.loop(rounds - lag, rounds)
            def _(r):
                for way in range(2):
                    keep(way, r)

            @pl.loop(0, rounds)
            def _(r):
                for way in range(2):
                    later_hop(way, r, size).wait_send()

    for copy in across:
        copy.wait()
    rows_over = pltpu.make_async_copy(marks, table_ref.at[pl.ds(tiles, bands)], local_sem)
    rows_over.start()
    rows_over.wait()
    for j in range(1, bands):
        flag = jnp.maximum(flag, table_ref[tiles + lax.rem(band + j, bands), 0, LANES - 1])
    plan_ref[0, 0] = flag

    @pl.when(band < bands - 1)
    def _():
        upward.wait_send()
        downward.wait_recv()

    @pl.when(band > 0)
    def _():
        downward.wait_send()
        upward.wait_recv()


def take_kernel(tiles, bands, bucket, table_ref, plan_ref, send_ref, pool_ref, beside_ref, out_ref):
    band, tile = lax.axis_index("band"), lax.axis_index("tile")
    reach = tiles // 2
    own_rows = 2 * bucket
    at = layout(bucket)
    out_ref[...] = jnp.zeros_like(out_ref)
    for s in range(bucket):
        label = table_ref[tile, 0, at["own"] + s]

        @pl.when(label >= 0)
        def _():
            out_ref[label] += send_ref[at["own"] + s]

    for way in range(2):
        other = tiles + jnp.clip(band - 1 if way == 0 else band + 1, 0, bands - 1)
        valid = (band > 0) if way == 0 else (band < bands - 1)
        for s in range(bucket):
            label = table_ref[other, 0, at["up"] + way * bucket + s]

            @pl.when((label >= 0) & valid)
            def _():
                out_ref[label] += beside_ref[way, s]

    for way in range(2):
        for distance in range(1, reach + 1):
            source = ring_tile(tiles, tile, -distance if way == 0 else distance)
            reaches = reaching(tiles, bucket, way, lambda i: table_ref[source, 0, i])
            start = own_rows + plan_ref[0, 1 + way * reach + distance - 1]

            @pl.loop(reaches[distance + 1], reaches[distance])
            def _(i):
                out_ref[table_ref[source, 0, way * own_rows + i]] += pool_ref[way, start + i]


def adaptive(tiles, bands, patches, pair_patch, pair_atm, numerators, counts):
    pairs, patch_rows, cell_rows = numerators.shape
    flux = patches.shape[1]
    blocks_owned = CELLS_DEV // cell_rows
    bucket = pairs // 8
    reach = tiles // 2
    chunk = 16
    plans = ((5, 4 * reach, 4), (3, 4 * reach, 4))
    slots = max(size * rounds for size, rounds, _ in plans)
    most = max(rounds for _, rounds, _ in plans)
    smem = pl.BlockSpec(memory_space=pltpu.SMEM)
    vmem = pl.BlockSpec(memory_space=pltpu.VMEM)
    anywhere = pl.BlockSpec(memory_space=pl.ANY)
    block = (cell_rows, flux)
    f32 = jnp.float32
    send, labels = pl.pallas_call(
        functools.partial(list_kernel, tiles, bands, bucket, blocks_owned, chunk),
        out_shape=(jax.ShapeDtypeStruct((7 * bucket + 1,) + block, f32),
                   jax.ShapeDtypeStruct((1, LANES), jnp.int32)),
        in_specs=[smem, smem, smem, anywhere, anywhere],
        out_specs=(vmem, smem),
        scratch_shapes=[
            pltpu.VMEM(patches.shape, patches.dtype),
            pltpu.VMEM((pairs, cell_rows, patch_rows), jnp.int32),
            pltpu.SMEM(((tiles + 2) * blocks_owned,), jnp.int32),
            pltpu.SMEM((tiles + 2,), jnp.int32),
            pltpu.SMEM((tiles + 2,), jnp.int32),
            pltpu.SMEM((tiles,), jnp.int32),
            pltpu.SMEM((pairs,), jnp.int32),
            pltpu.SemaphoreType.DMA,
            pltpu.SemaphoreType.DMA((pairs // chunk,)),
        ],
        compiler_params=pltpu.CompilerParams(vmem_limit_bytes=VMEM_LIMIT),
        name="list",
    )(pair_patch, pair_atm, counts, patches, jnp.transpose(numerators, (0, 2, 1)))
    pool, beside, table, plan = pl.pallas_call(
        functools.partial(stream_kernel, tiles, bands, bucket, plans),
        out_shape=(jax.ShapeDtypeStruct((2, 2 * bucket + slots) + block, f32),
                   jax.ShapeDtypeStruct((2, bucket) + block, f32),
                   jax.ShapeDtypeStruct((tiles + bands, 1, LANES), jnp.int32),
                   jax.ShapeDtypeStruct((1, LANES), jnp.int32)),
        in_specs=[vmem, vmem],
        out_specs=(vmem, vmem, smem, smem),
        scratch_shapes=[
            pltpu.VMEM((2, slots) + block, f32),
            pltpu.VMEM((2, slots) + block, f32),
            pltpu.VMEM((tiles, 1, LANES), jnp.int32),
            pltpu.VMEM((bands, 1, LANES), jnp.int32),
            pltpu.VMEM((1, LANES), jnp.int32),
            pltpu.SemaphoreType.DMA((2, most)),
            pltpu.SemaphoreType.DMA((2, most)),
            pltpu.SemaphoreType.DMA((2,)),
            pltpu.SemaphoreType.DMA((2,)),
            pltpu.SemaphoreType.DMA((tiles + bands - 2,)),
            pltpu.SemaphoreType.DMA((tiles + bands - 2,)),
            pltpu.SemaphoreType.DMA,
        ],
        compiler_params=pltpu.CompilerParams(collective_id=1, has_side_effects=True, vmem_limit_bytes=VMEM_LIMIT),
        name="stream",
    )(send, labels)

    def take(patches, pair_patch, pair_atm, numerators, counts, table, plan, send, pool, beside):
        out = pl.pallas_call(
            functools.partial(take_kernel, tiles, bands, bucket),
            out_shape=jax.ShapeDtypeStruct((blocks_owned,) + block, f32),
            in_specs=[smem, smem, vmem, vmem, vmem],
            out_specs=vmem,
            compiler_params=pltpu.CompilerParams(vmem_limit_bytes=VMEM_LIMIT),
            name="take",
        )(table, plan, send, pool, beside)
        return out.reshape(blocks_owned * cell_rows, flux)

    def padded(patches, pair_patch, pair_atm, numerators, counts, table, plan, send, pool, beside):
        return per_device(tiles, bands, patches, pair_patch, pair_atm, numerators, counts)

    return lax.cond(plan[0, 0] > 0, padded, take, patches, pair_patch, pair_atm, numerators, counts,
                    table, plan, send, pool, beside)


def solution(mesh):
    spec = P(("band", "tile"))
    placed = (
        P(("band", "tile"), None),
        spec,
        spec,
        P(("band", "tile"), None, None),
        spec,
    )
    body = functools.partial(adaptive, mesh.shape["tile"], mesh.shape["band"])
    return jax.shard_map(body, mesh=mesh, in_specs=placed, out_specs=P(("band", "tile"), None), check_vma=False)
```

```python
import functools

import jax
import jax.numpy as jnp
from jax import lax
from jax.experimental import pallas as pl
from jax.experimental.pallas import tpu as pltpu
from jax.sharding import PartitionSpec as P

CELLS_DEV = 4096
SCALE = 2.0 ** (-27)
MESH = pl.DeviceIdType.MESH
LANES = 128
VMEM_LIMIT = 20 * 2 ** 20
STREAM_LIMIT = 24 * 2 ** 20
PADDED_LIMIT = 63 * 2 ** 20


def partners(count):
    if count & (count - 1) == 0:
        return [lambda me, k=k: me ^ k for k in range(count - 1, 0, -1)]
    return [lambda me, k=k: lax.rem(me + k, count) for k in range(1, count)]


def pack_kernel(tiles, bucket, blocks_owned, chunk,
                patch_ref, atm_ref, counts_ref, patches_hbm, numer_hbm,
                send_ref, labels_ref,
                patches_v, numer_v, table, used, patch_sem, numer_sems):
    pairs = numer_v.shape[0]
    patch_rows = numer_v.shape[2]
    chunks = pairs // chunk
    buckets = tiles + 2
    patch_copy = pltpu.make_async_copy(patches_hbm, patches_v, patch_sem)
    patch_copy.start()
    copies = []
    for c in range(chunks):
        part = pl.ds(c * chunk, chunk)
        copy = pltpu.make_async_copy(numer_hbm.at[part], numer_v.at[part], numer_sems.at[c])
        copy.start()
        copies.append(copy)
    band = lax.axis_index("band")
    live = counts_ref[0]

    for b in range(buckets):
        used[b] = 0

        @pl.loop(0, blocks_owned, unroll=16)
        def _(i):
            table[b * blocks_owned + i] = -1

        for s in range(bucket):
            labels_ref[b, 0, s] = -1
    patch_copy.wait()
    for c in range(chunks):
        copies[c].wait()

        @pl.when(c * chunk < live)
        def _():
            for j in range(chunk):
                g = c * chunk + j
                is_live = g < live
                atm = atm_ref[g]
                owner = lax.div(atm, blocks_owned)
                block = lax.rem(atm, blocks_owned)
                owner_band = lax.div(owner, tiles)
                owner_tile = lax.rem(owner, tiles)
                b = jnp.where(owner_band == band, owner_tile,
                              jnp.where(owner_band > band, tiles, tiles + 1))
                entry = b * blocks_owned + block
                known = table[entry]
                fresh = known < 0
                new = used[b]
                rank = jnp.where(fresh, new, known)

                @pl.when(is_live)
                def _():
                    table[entry] = rank
                    used[b] = jnp.where(fresh, new + 1, new)
                    labels_ref[b, 0, rank] = block

                slot = jnp.where(is_live, b * bucket + rank, buckets * bucket)
                rows = pl.multiple_of(patch_ref[g] * patch_rows, patch_rows)
                weight = (numer_v[g].astype(jnp.float32) * SCALE).astype(jnp.bfloat16)
                part = jnp.dot(weight, patches_v[pl.ds(rows, patch_rows), :],
                               preferred_element_type=jnp.float32)
                before = send_ref[slot]
                send_ref[slot] = jnp.where(fresh, part, before + part)


def send_kernel(tiles, bands, bucket, send_ref, labels_ref, recv_ref, recv_labels_ref,
                data_send, data_recv, label_send, label_recv):
    band, tile = lax.axis_index("band"), lax.axis_index("tile")
    barrier = pltpu.get_barrier_semaphore()
    steps = partners(tiles)
    for step in steps:
        pl.semaphore_signal(barrier, inc=1, device_id=(band, step(tile)), device_id_type=MESH)

    @pl.when(band < bands - 1)
    def _():
        pl.semaphore_signal(barrier, inc=1, device_id=(band + 1, tile), device_id_type=MESH)

    @pl.when(band > 0)
    def _():
        pl.semaphore_signal(barrier, inc=1, device_id=(band - 1, tile), device_id_type=MESH)

    neighbours = jnp.where(band < bands - 1, 1, 0) + jnp.where(band > 0, 1, 0)
    pl.semaphore_wait(barrier, tiles - 1 + neighbours)

    def pair(source, place, device, sem):
        rows = pl.ds(source * bucket, bucket)
        landing = pl.ds(place * bucket, bucket)
        return (
            pltpu.make_async_remote_copy(
                src_ref=labels_ref.at[source], dst_ref=recv_labels_ref.at[place],
                send_sem=label_send.at[sem], recv_sem=label_recv.at[sem],
                device_id=device, device_id_type=MESH),
            pltpu.make_async_remote_copy(
                src_ref=send_ref.at[rows], dst_ref=recv_ref.at[landing],
                send_sem=data_send.at[sem], recv_sem=data_recv.at[sem],
                device_id=device, device_id_type=MESH),
        )

    inside = [pair(step(tile), tile, (band, step(tile)), k) for k, step in enumerate(steps)]
    upward = pair(tiles, tiles, (band + 1, tile), tiles - 1)
    downward = pair(tiles + 1, tiles + 1, (band - 1, tile), tiles)
    for copies in inside[:2]:
        for copy in copies:
            copy.start()

    @pl.when(band < bands - 1)
    def _():
        for copy in upward:
            copy.start()

    @pl.when(band > 0)
    def _():
        for copy in downward:
            copy.start()

    for copies in inside[2:]:
        for copy in copies:
            copy.start()
    for copies in inside:
        for copy in copies:
            copy.wait()

    @pl.when(band < bands - 1)
    def _():
        for up, down in zip(upward, downward):
            up.wait_send()
            down.wait_recv()

    @pl.when(band > 0)
    def _():
        for up, down in zip(upward, downward):
            down.wait_send()
            up.wait_recv()


def add_kernel(tiles, bands, bucket, labels_ref, recv_labels_ref, send_hbm, recv_hbm, out_ref,
               landed, sems):
    band, tile = lax.axis_index("band"), lax.axis_index("tile")
    buckets = tiles + 2

    def copy_of(b, ref):
        rows = pl.ds(b * bucket, bucket)
        return pltpu.make_async_copy(ref.at[rows], landed.at[rows], sems.at[b])

    for b in range(buckets):
        if b < tiles:
            @pl.when(tile == b)
            def _():
                copy_of(b, send_hbm).start()

            @pl.when(tile != b)
            def _():
                copy_of(b, recv_hbm).start()
        else:
            copy_of(b, recv_hbm).start()
    out_ref[...] = jnp.zeros_like(out_ref)
    for b in range(buckets):
        copy_of(b, recv_hbm).wait()
        if b == tiles:
            valid = band > 0
        elif b == tiles + 1:
            valid = band < bands - 1
        else:
            valid = True
        for s in range(bucket):
            label = recv_labels_ref[b, 0, s]
            if b < tiles:
                label = jnp.where(tile == b, labels_ref[b, 0, s], label)

            @pl.when((label >= 0) & valid)
            def _():
                out_ref[label] += landed[b * bucket + s]


def per_device(tiles, bands, patches, pair_patch, pair_atm, numerators, counts):
    pairs, cell_rows, patch_rows = numerators.shape
    flux = patches.shape[1]
    blocks_owned = CELLS_DEV // cell_rows
    bucket = pairs // 8
    buckets = tiles + 2
    chunk = 16
    smem = pl.BlockSpec(memory_space=pltpu.SMEM)
    vmem = pl.BlockSpec(memory_space=pltpu.VMEM)
    anywhere = pl.BlockSpec(memory_space=pl.ANY)
    labels_shape = jax.ShapeDtypeStruct((buckets, 1, LANES), jnp.int32)
    recv_shape = jax.ShapeDtypeStruct((buckets * bucket, cell_rows, flux), jnp.float32)
    send, labels = pl.pallas_call(
        functools.partial(pack_kernel, tiles, bucket, blocks_owned, chunk),
        out_shape=(jax.ShapeDtypeStruct((buckets * bucket + 1, cell_rows, flux), jnp.float32), labels_shape),
        in_specs=[smem, smem, smem, anywhere, anywhere],
        out_specs=(vmem, smem),
        scratch_shapes=[
            pltpu.VMEM(patches.shape, patches.dtype),
            pltpu.VMEM((pairs, cell_rows, patch_rows), jnp.int32),
            pltpu.SMEM((buckets * blocks_owned,), jnp.int32),
            pltpu.SMEM((buckets,), jnp.int32),
            pltpu.SemaphoreType.DMA,
            pltpu.SemaphoreType.DMA((pairs // chunk,)),
        ],
        compiler_params=pltpu.CompilerParams(vmem_limit_bytes=PADDED_LIMIT),
        name="pack",
    )(pair_patch, pair_atm, counts, patches, numerators)
    recv, recv_labels = pl.pallas_call(
        functools.partial(send_kernel, tiles, bands, bucket),
        out_shape=(recv_shape, labels_shape),
        in_specs=[anywhere, anywhere],
        out_specs=(anywhere, anywhere),
        scratch_shapes=[pltpu.SemaphoreType.DMA((tiles + 1,))] * 4,
        compiler_params=pltpu.CompilerParams(collective_id=0, has_side_effects=True, vmem_limit_bytes=VMEM_LIMIT),
        name="exchange",
    )(send, labels)
    out = pl.pallas_call(
        functools.partial(add_kernel, tiles, bands, bucket),
        out_shape=jax.ShapeDtypeStruct((blocks_owned, cell_rows, flux), jnp.float32),
        in_specs=[smem, smem, anywhere, anywhere],
        out_specs=vmem,
        scratch_shapes=[
            pltpu.VMEM(recv_shape.shape, jnp.float32),
            pltpu.SemaphoreType.DMA((buckets,)),
        ],
        compiler_params=pltpu.CompilerParams(vmem_limit_bytes=VMEM_LIMIT),
        name="add",
    )(labels, recv_labels, send, recv)
    return out.reshape(blocks_owned * cell_rows, flux)


def ring_order(tiles):
    wide = tiles // 4
    if wide * 4 != tiles or wide % 2:
        return list(range(tiles))
    order = list(range(wide))
    for step, column in enumerate(reversed(range(wide))):
        rows = range(1, 4) if step % 2 == 0 else range(3, 0, -1)
        order += [row * wide + column for row in rows]
    return order


def chosen(values, index):
    picked = values[0]
    for k in range(1, len(values)):
        picked = jnp.where(index == k, values[k], picked)
    return picked


def ring_tile(tiles, tile, steps):
    order = ring_order(tiles)
    position = chosen([order.index(k) for k in range(tiles)], tile)
    return chosen(order, lax.rem(position + steps + tiles, tiles))


def layout(bucket):
    return dict(up=4 * bucket, down=5 * bucket, own=6 * bucket, end=7 * bucket)


def reaching(tiles, bucket, way, read):
    reach = tiles // 2
    base = 7 * bucket - 1
    far = read(base + reach)
    counts = [read(base + (k if way == 0 else tiles - k)) for k in range(1, reach)]
    counts.append((far + 1) >> 1 if way == 0 else far >> 1)
    beyond = [0]
    for count in reversed(counts):
        beyond.append(beyond[-1] + count)
    return [None] + beyond[::-1]


def split(value, size):
    if size & (size - 1) == 0:
        return value >> (size.bit_length() - 1), value & (size - 1)
    return lax.div(value, size), lax.rem(value, size)


def sort_pairs(tiles, bands, bucket, blocks_owned, band, tile, live, atm):
    pairs = atm.shape[1]
    reach = tiles // 2
    order = ring_order(tiles)
    spots = [order.index(k) for k in range(tiles)]
    here = chosen(spots, tile)
    wide = (pairs, pairs)

    def across(value):
        return jnp.broadcast_to(value, wide).T

    def least(value):
        return jnp.min(value, axis=0, keepdims=True)

    def most(value):
        return jnp.max(value, axis=0, keepdims=True)

    def count(mask):
        return jnp.sum(jnp.where(mask, 1, 0), axis=0, keepdims=True)

    def bucket_of(value):
        owner, block = split(value, blocks_owned)
        owner_band, owner_tile = split(owner, tiles)
        ahead = split(chosen(spots, owner_tile) - here + tiles, tiles)[1]
        return jnp.where(owner_band == band, ahead, jnp.where(owner_band > band, tiles, tiles + 1)), block

    row = lax.broadcasted_iota(jnp.int32, wide, 0)
    lane = lax.broadcasted_iota(jnp.int32, wide, 1)
    one_lane = lax.broadcasted_iota(jnp.int32, (1, pairs), 1)
    atm_c = across(atm)
    live_c = row < live
    same = (atm_c == atm) & live_c
    first = least(jnp.where(same, row, pairs))
    before = most(jnp.where(same & (row < lane), row, -1))
    fresh_c = (across(first) == row) & live_c
    b, _ = bucket_of(atm)
    b_c, block_c = bucket_of(atm_c)
    rank = count(fresh_c & (b_c == b) & (row < first))
    back = (b > reach) | ((b == reach) & ((rank & 1) == 1))
    region = jnp.where(b == 0, 4, jnp.where(b >= tiles, b - tiles + 2, jnp.where(back, 1, 0)))
    near = jnp.where(region == 0, reach - b, jnp.where(region == 1, b - reach, 0))
    shift = ((reach + 1) * (pairs + 1)).bit_length()
    key = (region << shift) + near * (pairs + 1) + first
    key_c = across(key)
    place = count(fresh_c & ((key_c >> shift) == region) & (key_c < key))
    ring = region < 2
    room = jnp.where(ring, 2 * bucket, bucket)
    base = jnp.where(ring, 2 * region, region + 2) * bucket
    fits = place < room
    slot = jnp.where((one_lane < live) & fits, base + place, pairs)
    overflow = jnp.max(jnp.where((one_lane < live) & jnp.logical_not(fits), 1, 0), axis=1, keepdims=True)
    hit = across(slot) == lane
    last = most(jnp.where(hit, row, 0))
    label = most(jnp.where(hit, block_c, -1))
    counts = count(fresh_c & (b_c == lane - (7 * bucket - 1)))
    labels = jnp.where(one_lane < 7 * bucket, label, jnp.where(one_lane == pairs - 1, overflow, counts))
    return before, last, labels


def starts(reach, lag, reaches):
    first = [None] * (reach + 1)
    for u in range(reach - 1, -1, -1):
        begin = [0]
        for j in range(1, reach - u):
            after = begin[j - 1] + reaches[u + j - 1][j]
            begin.append(jnp.maximum(after, first[u + 1][j - 1] + lag))
        first[u] = begin
    end = first[0][reach - 1] + reaches[reach - 1][reach]
    return first[0], first[1], end


def stream_kernel(tiles, bands, bucket, blocks_owned, plans, group,
                  patch_ref, counts_ref, atm_ref, patches_hbm, numer_hbm,
                  pool_ref, beside_ref, own_ref, table_ref, plan_ref,
                  patches_ref, numer_ref, labels_ref, work_v, work_ref, load_sems, sums, side, stage, recv, landing, marks, mark,
                  ring_send, ring_recv, beside_send, beside_recv, label_send, label_recv, local_sem):
    band, tile = lax.axis_index("band"), lax.axis_index("tile")
    reach = tiles // 2
    own_rows = 2 * bucket
    at = layout(bucket)
    steps = partners(tiles)
    pairs = numer_ref.shape[0]

    def numer_load(c):
        part = pl.ds(c * group, group)
        return pltpu.make_async_copy(numer_hbm.at[part], numer_ref.at[part], load_sems.at[c])

    patch_load = pltpu.make_async_copy(patches_hbm, patches_ref, load_sems.at[pairs // group])
    patch_load.start()
    for c in range(pairs // group):
        numer_load(c).start()
    barrier = pltpu.get_barrier_semaphore()
    for step in steps:
        pl.semaphore_signal(barrier, inc=1, device_id=(band, step(tile)), device_id_type=MESH)
    for j in range(1, bands):
        pl.semaphore_signal(barrier, inc=1, device_id=(lax.rem(band + j, bands), tile), device_id_type=MESH)
    before, last, labels = sort_pairs(tiles, bands, bucket, blocks_owned, band, tile, counts_ref[0], atm_ref[...])
    labels_ref[...] = labels
    landing[tile] = labels
    work_v[0:1] = before
    work_v[1:2] = last
    work_in = pltpu.make_async_copy(work_v, work_ref, local_sem)
    work_in.start()
    work_in.wait()
    patch_load.wait()

    @pl.loop(0, pairs // group)
    def _(c):
        numer_load(c).wait()
        for j in range(group):
            g = c * group + j
            weight = (numer_ref[g].astype(jnp.float32) * SCALE).astype(jnp.bfloat16)
            part = jnp.dot(weight, patches_ref[patch_ref[g]], preferred_element_type=jnp.float32)
            before = work_ref[0, g]
            earlier = sums[jnp.maximum(before, 0)]
            sums[g] = part + jnp.where(before >= 0, earlier, 0.0)

    def total(slot):
        return sums[work_ref[1, slot]]

    targets = ((band, ring_tile(tiles, tile, 1)), (band, ring_tile(tiles, tile, -1)))
    is_edge = (band == 0) | (band == bands - 1)
    head = max(size * lag for size, _, lag in plans)
    for way in range(2):
        for s in range(head):
            pool_ref[way, s] = total(way * own_rows + s)
    pl.semaphore_wait(barrier, tiles + bands - 2)
    inside = [
        pltpu.make_async_remote_copy(
            src_ref=labels_ref, dst_ref=landing.at[tile],
            send_sem=label_send.at[k], recv_sem=label_recv.at[k],
            device_id=(band, step(tile)), device_id_type=MESH)
        for k, step in enumerate(steps)
    ]
    across = [
        pltpu.make_async_remote_copy(
            src_ref=mark, dst_ref=marks.at[band],
            send_sem=label_send.at[tiles - 2 + j], recv_sem=label_recv.at[tiles - 2 + j],
            device_id=(lax.rem(band + j, bands), tile), device_id_type=MESH)
        for j in range(1, bands)
    ]
    for copy in inside:
        copy.start()

    def hop(way, r, size, source):
        rows = pl.ds(r * size, size)
        return pltpu.make_async_remote_copy(
            src_ref=source, dst_ref=recv.at[way, rows],
            send_sem=ring_send.at[way, r], recv_sem=ring_recv.at[way, r],
            device_id=targets[way], device_id_type=MESH)

    def own_hop(way, r, size):
        return hop(way, r, size, pool_ref.at[way, pl.ds(r * size, size)])

    def later_hop(way, r, size):
        return hop(way, r, size, stage.at[way, pl.ds(r * size, size)])

    for edge in (True, False):
        size, rounds, lag = plans[0 if edge else 1]

        @pl.when(is_edge if edge else jnp.logical_not(is_edge))
        def _():
            for r in range(lag):
                for way in range(2):
                    own_hop(way, r, size).start()

    def beside(way, target_band):
        return pltpu.make_async_remote_copy(
            src_ref=side.at[way], dst_ref=beside_ref.at[way],
            send_sem=beside_send.at[way], recv_sem=beside_recv.at[way],
            device_id=(target_band, tile), device_id_type=MESH)

    upward, downward = beside(0, band + 1), beside(1, band - 1)
    for way in range(2):
        for s in range(bucket):
            side[way, s] = total(at["up"] + way * bucket + s)
    for way in range(2):
        for s in range(head, own_rows):
            pool_ref[way, s] = total(way * own_rows + s)
    for s in range(bucket):
        own_ref[s] = total(at["own"] + s)

    @pl.when(band < bands - 1)
    def _():
        upward.start()

    @pl.when(band > 0)
    def _():
        downward.start()

    for copy in inside:
        copy.wait()
    rows_in = pltpu.make_async_copy(landing, table_ref.at[pl.ds(0, tiles)], local_sem)
    rows_in.start()
    rows_in.wait()

    upstream = [[ring_tile(tiles, tile, -u if way == 0 else u) for u in range(tiles)] for way in range(2)]
    reaches = [[reaching(tiles, bucket, way, lambda i, t=t: table_ref[t, 0, i]) for t in upstream[way]]
               for way in range(2)]
    lag_slots = jnp.where(is_edge, plans[0][0] * plans[0][2], plans[1][0] * plans[1][2])
    capacity = jnp.where(is_edge, plans[0][0] * plans[0][1], plans[1][0] * plans[1][1])
    worst = jnp.int32(0)
    flag = jnp.int32(0)
    begins = []
    for way in range(2):
        for v in range(tiles):
            ahead, behind, end = starts(reach, lag_slots, [reaches[way][(v + u) % tiles] for u in range(reach)])
            worst = jnp.maximum(worst, end)
            if v == 0:
                begins.append(ahead)
    arrivals = []
    for way in range(2):
        ahead, _, _ = starts(reach, lag_slots, [reaches[way][(1 + u) % tiles] for u in range(reach)])
        arrivals.append(ahead)
    for t in range(tiles):
        flag = jnp.maximum(flag, table_ref[t, 0, LANES - 1])
    flag = jnp.where(worst > capacity, 1, flag)
    lane = lax.broadcasted_iota(jnp.int32, (1, LANES), 1)
    mark[...] = jnp.where(lane == LANES - 1, flag, landing[tile])
    for way in range(2):
        for j in range(reach):
            plan_ref[0, 1 + way * reach + j] = arrivals[way][j]

    for edge in (True, False):
        size, rounds, lag = plans[0 if edge else 1]
        last_row = own_rows + size * rounds - 1

        @pl.when(is_edge if edge else jnp.logical_not(is_edge))
        def _():
            def keep(way, r):
                later_hop(way, r, size).wait_recv()
                pool_ref[way, pl.ds(own_rows + r * size, size)] = recv[way, pl.ds(r * size, size)]

            def gather(way, r):
                begin, arrived = begins[way], arrivals[way]
                for s in range(size):
                    p = r * size + s
                    row = jnp.minimum(p, own_rows - 1)
                    for j in range(1, reach):
                        row = jnp.where(p >= begin[j], p + (own_rows + arrived[j - 1] - begin[j]), row)
                    row = jnp.clip(row, 0, last_row)
                    stage[way, p] = pool_ref[way, row]

            def one_round(r):
                for way in range(2):
                    keep(way, r - lag)
                for way in range(2):
                    gather(way, r)
                for way in range(2):
                    later_hop(way, r, size).start()

            one_round(lag)
            for copy in across:
                copy.start()

            @pl.loop(lag + 1, rounds)
            def _(r):
                one_round(r)

            @pl.loop(rounds - lag, rounds)
            def _(r):
                for way in range(2):
                    keep(way, r)

            @pl.loop(0, rounds)
            def _(r):
                for way in range(2):
                    later_hop(way, r, size).wait_send()

    for copy in across:
        copy.wait()
    rows_over = pltpu.make_async_copy(marks, table_ref.at[pl.ds(tiles, bands)], local_sem)
    rows_over.start()
    rows_over.wait()
    for j in range(1, bands):
        flag = jnp.maximum(flag, table_ref[tiles + lax.rem(band + j, bands), 0, LANES - 1])
    plan_ref[0, 0] = flag

    @pl.when(band < bands - 1)
    def _():
        upward.wait_send()
        downward.wait_recv()

    @pl.when(band > 0)
    def _():
        downward.wait_send()
        upward.wait_recv()


def take_kernel(tiles, bands, bucket, table_ref, plan_ref, own_ref, pool_ref, beside_ref, out_ref):
    band, tile = lax.axis_index("band"), lax.axis_index("tile")
    reach = tiles // 2
    own_rows = 2 * bucket
    at = layout(bucket)
    out_ref[...] = jnp.zeros_like(out_ref)
    for s in range(bucket):
        label = table_ref[tile, 0, at["own"] + s]

        @pl.when(label >= 0)
        def _():
            out_ref[label] += own_ref[s]

    for way in range(2):
        other = tiles + jnp.clip(band - 1 if way == 0 else band + 1, 0, bands - 1)
        valid = (band > 0) if way == 0 else (band < bands - 1)
        for s in range(bucket):
            label = table_ref[other, 0, at["up"] + way * bucket + s]

            @pl.when((label >= 0) & valid)
            def _():
                out_ref[label] += beside_ref[way, s]

    for way in range(2):
        for distance in range(1, reach + 1):
            source = ring_tile(tiles, tile, -distance if way == 0 else distance)
            reaches = reaching(tiles, bucket, way, lambda i: table_ref[source, 0, i])
            start = own_rows + plan_ref[0, 1 + way * reach + distance - 1]

            @pl.loop(reaches[distance + 1], reaches[distance])
            def _(i):
                out_ref[table_ref[source, 0, way * own_rows + i]] += pool_ref[way, start + i]


def adaptive(tiles, bands, patches, pair_patch, pair_atm, numerators, counts):
    pairs, patch_rows, cell_rows = numerators.shape
    flux = patches.shape[1]
    blocks_owned = CELLS_DEV // cell_rows
    bucket = pairs // 8
    reach = tiles // 2
    group = 16
    plans = ((3, pl.cdiv(20 * reach, 3), 5), (2, 6 * reach, 5))
    slots = max(size * rounds for size, rounds, _ in plans)
    most = max(rounds for _, rounds, _ in plans)
    smem = pl.BlockSpec(memory_space=pltpu.SMEM)
    vmem = pl.BlockSpec(memory_space=pltpu.VMEM)
    hbm = pl.BlockSpec(memory_space=pltpu.HBM)
    block = (cell_rows, flux)
    f32 = jnp.float32
    numerators = jnp.transpose(numerators, (0, 2, 1))
    pool, beside, own, table, plan = pl.pallas_call(
        functools.partial(stream_kernel, tiles, bands, bucket, blocks_owned, plans, group),
        out_shape=(jax.ShapeDtypeStruct((2, 2 * bucket + slots) + block, f32),
                   jax.ShapeDtypeStruct((2, bucket) + block, f32),
                   jax.ShapeDtypeStruct((bucket,) + block, f32),
                   jax.ShapeDtypeStruct((tiles + bands, 1, LANES), jnp.int32),
                   jax.ShapeDtypeStruct((1, LANES), jnp.int32)),
        in_specs=[smem, smem, vmem, hbm, hbm],
        out_specs=(vmem, vmem, vmem, smem, smem),
        scratch_shapes=[
            pltpu.VMEM((patches.shape[0] // patch_rows, patch_rows, flux), patches.dtype),
            pltpu.VMEM(numerators.shape, numerators.dtype),
            pltpu.VMEM((1, LANES), jnp.int32),
            pltpu.VMEM((2, pairs), jnp.int32),
            pltpu.SMEM((2, pairs), jnp.int32),
            pltpu.SemaphoreType.DMA((pairs // group + 1,)),
            pltpu.VMEM((pairs,) + block, f32),
            pltpu.VMEM((2, bucket) + block, f32),
            pltpu.VMEM((2, slots) + block, f32),
            pltpu.VMEM((2, slots) + block, f32),
            pltpu.VMEM((tiles, 1, LANES), jnp.int32),
            pltpu.VMEM((bands, 1, LANES), jnp.int32),
            pltpu.VMEM((1, LANES), jnp.int32),
            pltpu.SemaphoreType.DMA((2, most)),
            pltpu.SemaphoreType.DMA((2, most)),
            pltpu.SemaphoreType.DMA((2,)),
            pltpu.SemaphoreType.DMA((2,)),
            pltpu.SemaphoreType.DMA((tiles + bands - 2,)),
            pltpu.SemaphoreType.DMA((tiles + bands - 2,)),
            pltpu.SemaphoreType.DMA,
        ],
        compiler_params=pltpu.CompilerParams(collective_id=1, has_side_effects=True, vmem_limit_bytes=STREAM_LIMIT),
        name="stream",
    )(pair_patch, counts, pair_atm.reshape(1, pairs), patches.reshape(-1, patch_rows, flux), numerators)

    def take(patches, pair_patch, pair_atm, numerators, counts, table, plan, own, pool, beside):
        out = pl.pallas_call(
            functools.partial(take_kernel, tiles, bands, bucket),
            out_shape=jax.ShapeDtypeStruct((blocks_owned,) + block, f32),
            in_specs=[smem, smem, vmem, vmem, vmem],
            out_specs=vmem,
            compiler_params=pltpu.CompilerParams(vmem_limit_bytes=VMEM_LIMIT),
            name="take",
        )(table, plan, own, pool, beside)
        return out.reshape(blocks_owned * cell_rows, flux)

    def padded(patches, pair_patch, pair_atm, numerators, counts, table, plan, own, pool, beside):
        return per_device(tiles, bands, patches, pair_patch, pair_atm, numerators, counts)

    return lax.cond(plan[0, 0] > 0, padded, take, patches, pair_patch, pair_atm, numerators, counts,
                    table, plan, own, pool, beside)


def solution(mesh):
    spec = P(("band", "tile"))
    placed = (
        P(("band", "tile"), None),
        spec,
        spec,
        P(("band", "tile"), None, None),
        spec,
    )
    body = functools.partial(adaptive, mesh.shape["tile"], mesh.shape["band"])
    return jax.shard_map(body, mesh=mesh, in_specs=placed, out_specs=P(("band", "tile"), None), check_vma=False)
```

```python
import functools

import jax
import jax.numpy as jnp
from jax import lax
from jax.experimental import pallas as pl
from jax.experimental.pallas import tpu as pltpu
from jax.sharding import PartitionSpec as P

CELLS_DEV = 4096
SCALE = 2.0 ** (-27)
MESH = pl.DeviceIdType.MESH
LANES = 128
VMEM_LIMIT = 20 * 2 ** 20
STREAM_LIMIT = 24 * 2 ** 20
PADDED_LIMIT = 63 * 2 ** 20


def partners(count):
    if count & (count - 1) == 0:
        return [lambda me, k=k: me ^ k for k in range(count - 1, 0, -1)]
    return [lambda me, k=k: lax.rem(me + k, count) for k in range(1, count)]


def pack_kernel(tiles, bucket, blocks_owned, chunk,
                patch_ref, atm_ref, counts_ref, patches_hbm, numer_hbm,
                send_ref, labels_ref,
                patches_v, numer_v, table, used, patch_sem, numer_sems):
    pairs = numer_v.shape[0]
    patch_rows = numer_v.shape[2]
    chunks = pairs // chunk
    buckets = tiles + 2
    patch_copy = pltpu.make_async_copy(patches_hbm, patches_v, patch_sem)
    patch_copy.start()
    copies = []
    for c in range(chunks):
        part = pl.ds(c * chunk, chunk)
        copy = pltpu.make_async_copy(numer_hbm.at[part], numer_v.at[part], numer_sems.at[c])
        copy.start()
        copies.append(copy)
    band = lax.axis_index("band")
    live = counts_ref[0]

    for b in range(buckets):
        used[b] = 0

        @pl.loop(0, blocks_owned, unroll=16)
        def _(i):
            table[b * blocks_owned + i] = -1

        for s in range(bucket):
            labels_ref[b, 0, s] = -1
    patch_copy.wait()
    for c in range(chunks):
        copies[c].wait()

        @pl.when(c * chunk < live)
        def _():
            for j in range(chunk):
                g = c * chunk + j
                is_live = g < live
                atm = atm_ref[g]
                owner = lax.div(atm, blocks_owned)
                block = lax.rem(atm, blocks_owned)
                owner_band = lax.div(owner, tiles)
                owner_tile = lax.rem(owner, tiles)
                b = jnp.where(owner_band == band, owner_tile,
                              jnp.where(owner_band > band, tiles, tiles + 1))
                entry = b * blocks_owned + block
                known = table[entry]
                fresh = known < 0
                new = used[b]
                rank = jnp.where(fresh, new, known)

                @pl.when(is_live)
                def _():
                    table[entry] = rank
                    used[b] = jnp.where(fresh, new + 1, new)
                    labels_ref[b, 0, rank] = block

                slot = jnp.where(is_live, b * bucket + rank, buckets * bucket)
                rows = pl.multiple_of(patch_ref[g] * patch_rows, patch_rows)
                weight = (numer_v[g].astype(jnp.float32) * SCALE).astype(jnp.bfloat16)
                part = jnp.dot(weight, patches_v[pl.ds(rows, patch_rows), :],
                               preferred_element_type=jnp.float32)
                before = send_ref[slot]
                send_ref[slot] = jnp.where(fresh, part, before + part)


def send_kernel(tiles, bands, bucket, send_ref, labels_ref, recv_ref, recv_labels_ref,
                data_send, data_recv, label_send, label_recv):
    band, tile = lax.axis_index("band"), lax.axis_index("tile")
    barrier = pltpu.get_barrier_semaphore()
    steps = partners(tiles)
    for step in steps:
        pl.semaphore_signal(barrier, inc=1, device_id=(band, step(tile)), device_id_type=MESH)

    @pl.when(band < bands - 1)
    def _():
        pl.semaphore_signal(barrier, inc=1, device_id=(band + 1, tile), device_id_type=MESH)

    @pl.when(band > 0)
    def _():
        pl.semaphore_signal(barrier, inc=1, device_id=(band - 1, tile), device_id_type=MESH)

    neighbours = jnp.where(band < bands - 1, 1, 0) + jnp.where(band > 0, 1, 0)
    pl.semaphore_wait(barrier, tiles - 1 + neighbours)

    def pair(source, place, device, sem):
        rows = pl.ds(source * bucket, bucket)
        landing = pl.ds(place * bucket, bucket)
        return (
            pltpu.make_async_remote_copy(
                src_ref=labels_ref.at[source], dst_ref=recv_labels_ref.at[place],
                send_sem=label_send.at[sem], recv_sem=label_recv.at[sem],
                device_id=device, device_id_type=MESH),
            pltpu.make_async_remote_copy(
                src_ref=send_ref.at[rows], dst_ref=recv_ref.at[landing],
                send_sem=data_send.at[sem], recv_sem=data_recv.at[sem],
                device_id=device, device_id_type=MESH),
        )

    inside = [pair(step(tile), tile, (band, step(tile)), k) for k, step in enumerate(steps)]
    upward = pair(tiles, tiles, (band + 1, tile), tiles - 1)
    downward = pair(tiles + 1, tiles + 1, (band - 1, tile), tiles)
    for copies in inside[:2]:
        for copy in copies:
            copy.start()

    @pl.when(band < bands - 1)
    def _():
        for copy in upward:
            copy.start()

    @pl.when(band > 0)
    def _():
        for copy in downward:
            copy.start()

    for copies in inside[2:]:
        for copy in copies:
            copy.start()
    for copies in inside:
        for copy in copies:
            copy.wait()

    @pl.when(band < bands - 1)
    def _():
        for up, down in zip(upward, downward):
            up.wait_send()
            down.wait_recv()

    @pl.when(band > 0)
    def _():
        for up, down in zip(upward, downward):
            down.wait_send()
            up.wait_recv()


def add_kernel(tiles, bands, bucket, labels_ref, recv_labels_ref, send_hbm, recv_hbm, out_ref,
               landed, sems):
    band, tile = lax.axis_index("band"), lax.axis_index("tile")
    buckets = tiles + 2

    def copy_of(b, ref):
        rows = pl.ds(b * bucket, bucket)
        return pltpu.make_async_copy(ref.at[rows], landed.at[rows], sems.at[b])

    for b in range(buckets):
        if b < tiles:
            @pl.when(tile == b)
            def _():
                copy_of(b, send_hbm).start()

            @pl.when(tile != b)
            def _():
                copy_of(b, recv_hbm).start()
        else:
            copy_of(b, recv_hbm).start()
    out_ref[...] = jnp.zeros_like(out_ref)
    for b in range(buckets):
        copy_of(b, recv_hbm).wait()
        if b == tiles:
            valid = band > 0
        elif b == tiles + 1:
            valid = band < bands - 1
        else:
            valid = True
        for s in range(bucket):
            label = recv_labels_ref[b, 0, s]
            if b < tiles:
                label = jnp.where(tile == b, labels_ref[b, 0, s], label)

            @pl.when((label >= 0) & valid)
            def _():
                out_ref[label] += landed[b * bucket + s]


def per_device(tiles, bands, patches, pair_patch, pair_atm, numerators, counts):
    pairs, cell_rows, patch_rows = numerators.shape
    flux = patches.shape[1]
    blocks_owned = CELLS_DEV // cell_rows
    bucket = pairs // 8
    buckets = tiles + 2
    chunk = 16
    smem = pl.BlockSpec(memory_space=pltpu.SMEM)
    vmem = pl.BlockSpec(memory_space=pltpu.VMEM)
    anywhere = pl.BlockSpec(memory_space=pl.ANY)
    labels_shape = jax.ShapeDtypeStruct((buckets, 1, LANES), jnp.int32)
    recv_shape = jax.ShapeDtypeStruct((buckets * bucket, cell_rows, flux), jnp.float32)
    send, labels = pl.pallas_call(
        functools.partial(pack_kernel, tiles, bucket, blocks_owned, chunk),
        out_shape=(jax.ShapeDtypeStruct((buckets * bucket + 1, cell_rows, flux), jnp.float32), labels_shape),
        in_specs=[smem, smem, smem, anywhere, anywhere],
        out_specs=(vmem, smem),
        scratch_shapes=[
            pltpu.VMEM(patches.shape, patches.dtype),
            pltpu.VMEM((pairs, cell_rows, patch_rows), jnp.int32),
            pltpu.SMEM((buckets * blocks_owned,), jnp.int32),
            pltpu.SMEM((buckets,), jnp.int32),
            pltpu.SemaphoreType.DMA,
            pltpu.SemaphoreType.DMA((pairs // chunk,)),
        ],
        compiler_params=pltpu.CompilerParams(vmem_limit_bytes=PADDED_LIMIT),
        name="pack",
    )(pair_patch, pair_atm, counts, patches, numerators)
    recv, recv_labels = pl.pallas_call(
        functools.partial(send_kernel, tiles, bands, bucket),
        out_shape=(recv_shape, labels_shape),
        in_specs=[anywhere, anywhere],
        out_specs=(anywhere, anywhere),
        scratch_shapes=[pltpu.SemaphoreType.DMA((tiles + 1,))] * 4,
        compiler_params=pltpu.CompilerParams(collective_id=0, has_side_effects=True, vmem_limit_bytes=VMEM_LIMIT),
        name="exchange",
    )(send, labels)
    out = pl.pallas_call(
        functools.partial(add_kernel, tiles, bands, bucket),
        out_shape=jax.ShapeDtypeStruct((blocks_owned, cell_rows, flux), jnp.float32),
        in_specs=[smem, smem, anywhere, anywhere],
        out_specs=vmem,
        scratch_shapes=[
            pltpu.VMEM(recv_shape.shape, jnp.float32),
            pltpu.SemaphoreType.DMA((buckets,)),
        ],
        compiler_params=pltpu.CompilerParams(vmem_limit_bytes=VMEM_LIMIT),
        name="add",
    )(labels, recv_labels, send, recv)
    return out.reshape(blocks_owned * cell_rows, flux)


def ring_order(tiles):
    wide = tiles // 4
    if wide * 4 != tiles or wide % 2:
        return list(range(tiles))
    order = list(range(wide))
    for step, column in enumerate(reversed(range(wide))):
        rows = range(1, 4) if step % 2 == 0 else range(3, 0, -1)
        order += [row * wide + column for row in rows]
    return order


def chosen(values, index):
    picked = values[0]
    for k in range(1, len(values)):
        picked = jnp.where(index == k, values[k], picked)
    return picked


def ring_tile(tiles, tile, steps):
    order = ring_order(tiles)
    position = chosen([order.index(k) for k in range(tiles)], tile)
    return chosen(order, lax.rem(position + steps + tiles, tiles))


def layout(bucket):
    return dict(up=4 * bucket, down=5 * bucket, own=6 * bucket, end=7 * bucket)


def reaching(tiles, bucket, way, read):
    reach = tiles // 2
    base = 7 * bucket - 1
    far = read(base + reach)
    counts = [read(base + (k if way == 0 else tiles - k)) for k in range(1, reach)]
    counts.append((far + 1) >> 1 if way == 0 else far >> 1)
    beyond = [0]
    for count in reversed(counts):
        beyond.append(beyond[-1] + count)
    return [None] + beyond[::-1]


def split(value, size):
    if size & (size - 1) == 0:
        return value >> (size.bit_length() - 1), value & (size - 1)
    return lax.div(value, size), lax.rem(value, size)


def sort_pairs(tiles, bands, bucket, blocks_owned, band, tile, live, atm):
    pairs = atm.shape[1]
    reach = tiles // 2
    order = ring_order(tiles)
    spots = [order.index(k) for k in range(tiles)]
    here = chosen(spots, tile)
    wide = (pairs, pairs)

    def across(value):
        return jnp.broadcast_to(value, wide).T

    def least(value):
        return jnp.min(value, axis=0, keepdims=True)

    def most(value):
        return jnp.max(value, axis=0, keepdims=True)

    def count(mask):
        return jnp.sum(jnp.where(mask, 1, 0), axis=0, keepdims=True)

    def bucket_of(value):
        owner, block = split(value, blocks_owned)
        owner_band, owner_tile = split(owner, tiles)
        ahead = split(chosen(spots, owner_tile) - here + tiles, tiles)[1]
        return jnp.where(owner_band == band, ahead, jnp.where(owner_band > band, tiles, tiles + 1)), block

    row = lax.broadcasted_iota(jnp.int32, wide, 0)
    lane = lax.broadcasted_iota(jnp.int32, wide, 1)
    one_lane = lax.broadcasted_iota(jnp.int32, (1, pairs), 1)
    atm_c = across(atm)
    live_c = row < live
    same = (atm_c == atm) & live_c
    first = least(jnp.where(same, row, pairs))
    before = most(jnp.where(same & (row < lane), row, -1))
    fresh_c = (across(first) == row) & live_c
    b, _ = bucket_of(atm)
    b_c, block_c = bucket_of(atm_c)
    rank = count(fresh_c & (b_c == b) & (row < first))
    back = (b > reach) | ((b == reach) & ((rank & 1) == 1))
    region = jnp.where(b == 0, 4, jnp.where(b >= tiles, b - tiles + 2, jnp.where(back, 1, 0)))
    near = jnp.where(region == 0, reach - b, jnp.where(region == 1, b - reach, 0))
    shift = ((reach + 1) * (pairs + 1)).bit_length()
    key = (region << shift) + near * (pairs + 1) + first
    key_c = across(key)
    place = count(fresh_c & ((key_c >> shift) == region) & (key_c < key))
    ring = region < 2
    room = jnp.where(ring, 2 * bucket, bucket)
    base = jnp.where(ring, 2 * region, region + 2) * bucket
    fits = place < room
    slot = jnp.where((one_lane < live) & fits, base + place, pairs)
    overflow = jnp.max(jnp.where((one_lane < live) & jnp.logical_not(fits), 1, 0), axis=1, keepdims=True)
    hit = across(slot) == lane
    last = most(jnp.where(hit, row, 0))
    label = most(jnp.where(hit, block_c, -1))
    counts = count(fresh_c & (b_c == lane - (7 * bucket - 1)))
    kinds = [count(fresh_c & (b_c == k)) for k in (0, tiles, tiles + 1)]
    packed = overflow + sum(kind << (1 + 6 * i) for i, kind in enumerate(kinds))
    labels = jnp.where(one_lane < 7 * bucket, label, jnp.where(one_lane == pairs - 1, packed, counts))
    return before, last, labels


def starts(reach, lag, reaches):
    first = [None] * (reach + 1)
    for u in range(reach - 1, -1, -1):
        begin = [0]
        for j in range(1, reach - u):
            after = begin[j - 1] + reaches[u + j - 1][j]
            begin.append(jnp.maximum(after, first[u + 1][j - 1] + lag))
        first[u] = begin
    end = jnp.int32(0)
    for j in range(reach):
        size = reaches[j][j + 1]
        end = jnp.where(size > 0, first[0][j] + size, end)
    return first[0], first[1], end


def stream_kernel(tiles, bands, bucket, blocks_owned, plans, group,
                  patch_ref, counts_ref, atm_ref, patches_hbm, numer_hbm,
                  pool_ref, beside_ref, own_ref, table_ref, plan_ref,
                  patches_ref, numer_ref, labels_ref, work_v, work_ref, load_sems, sums, side, stage, recv, landing, marks, mark,
                  ring_send, ring_recv, beside_send, beside_recv, label_send, label_recv, local_sem):
    band, tile = lax.axis_index("band"), lax.axis_index("tile")
    reach = tiles // 2
    own_rows = 2 * bucket
    at = layout(bucket)
    steps = partners(tiles)
    pairs = numer_ref.shape[0]

    def numer_load(c):
        part = pl.ds(c * group, group)
        return pltpu.make_async_copy(numer_hbm.at[part], numer_ref.at[part], load_sems.at[c])

    patch_load = pltpu.make_async_copy(patches_hbm, patches_ref, load_sems.at[pairs // group])
    patch_load.start()
    for c in range(pairs // group):
        numer_load(c).start()
    barrier = pltpu.get_barrier_semaphore()
    for step in steps:
        pl.semaphore_signal(barrier, inc=1, device_id=(band, step(tile)), device_id_type=MESH)
    for j in range(1, bands):
        pl.semaphore_signal(barrier, inc=1, device_id=(lax.rem(band + j, bands), tile), device_id_type=MESH)
    before, last, labels = sort_pairs(tiles, bands, bucket, blocks_owned, band, tile, counts_ref[0], atm_ref[...])
    labels_ref[...] = labels
    landing[tile] = labels
    work_v[0:1] = before
    work_v[1:2] = last
    work_in = pltpu.make_async_copy(work_v, work_ref, local_sem)
    work_in.start()
    work_in.wait()
    patch_load.wait()

    @pl.loop(0, pairs // group)
    def _(c):
        numer_load(c).wait()
        for j in range(group):
            g = c * group + j
            weight = (numer_ref[g].astype(jnp.float32) * SCALE).astype(jnp.bfloat16)
            part = jnp.dot(weight, patches_ref[patch_ref[g]], preferred_element_type=jnp.float32)
            before = work_ref[0, g]
            earlier = sums[jnp.maximum(before, 0)]
            sums[g] = part + jnp.where(before >= 0, earlier, 0.0)

    def total(slot):
        return sums[work_ref[1, slot]]

    targets = ((band, ring_tile(tiles, tile, 1)), (band, ring_tile(tiles, tile, -1)))
    is_edge = (band == 0) | (band == bands - 1)
    head = max(size * lag for size, _, lag in plans)
    for way in range(2):
        for s in range(head):
            pool_ref[way, s] = total(way * own_rows + s)
    pl.semaphore_wait(barrier, tiles + bands - 2)
    inside = [
        pltpu.make_async_remote_copy(
            src_ref=labels_ref, dst_ref=landing.at[tile],
            send_sem=label_send.at[k], recv_sem=label_recv.at[k],
            device_id=(band, step(tile)), device_id_type=MESH)
        for k, step in enumerate(steps)
    ]
    across = [
        pltpu.make_async_remote_copy(
            src_ref=mark, dst_ref=marks.at[band],
            send_sem=label_send.at[tiles - 2 + j], recv_sem=label_recv.at[tiles - 2 + j],
            device_id=(lax.rem(band + j, bands), tile), device_id_type=MESH)
        for j in range(1, bands)
    ]
    for copy in inside:
        copy.start()

    def hop(way, r, size, source):
        rows = pl.ds(r * size, size)
        return pltpu.make_async_remote_copy(
            src_ref=source, dst_ref=recv.at[way, rows],
            send_sem=ring_send.at[way, r], recv_sem=ring_recv.at[way, r],
            device_id=targets[way], device_id_type=MESH)

    def own_hop(way, r, size):
        return hop(way, r, size, pool_ref.at[way, pl.ds(r * size, size)])

    def later_hop(way, r, size):
        return hop(way, r, size, stage.at[way, pl.ds(r * size, size)])

    for edge in (True, False):
        size, rounds, lag = plans[0 if edge else 1]

        @pl.when(is_edge if edge else jnp.logical_not(is_edge))
        def _():
            for r in range(lag):
                for way in range(2):
                    own_hop(way, r, size).start()

    def beside(way, target_band):
        return pltpu.make_async_remote_copy(
            src_ref=side.at[way], dst_ref=beside_ref.at[way],
            send_sem=beside_send.at[way], recv_sem=beside_recv.at[way],
            device_id=(target_band, tile), device_id_type=MESH)

    upward, downward = beside(0, band + 1), beside(1, band - 1)
    for way in range(2):
        for s in range(bucket):
            side[way, s] = total(at["up"] + way * bucket + s)
    for way in range(2):
        for s in range(head, own_rows):
            pool_ref[way, s] = total(way * own_rows + s)
    for s in range(bucket):
        own_ref[s] = total(at["own"] + s)

    @pl.when(band < bands - 1)
    def _():
        upward.start()

    @pl.when(band > 0)
    def _():
        downward.start()

    for copy in inside:
        copy.wait()
    rows_in = pltpu.make_async_copy(landing, table_ref.at[pl.ds(0, tiles)], local_sem)
    rows_in.start()
    rows_in.wait()

    upstream = [[ring_tile(tiles, tile, -u if way == 0 else u) for u in range(tiles)] for way in range(2)]
    reaches = [[reaching(tiles, bucket, way, lambda i, t=t: table_ref[t, 0, i]) for t in upstream[way]]
               for way in range(2)]
    lag_slots = jnp.where(is_edge, plans[0][0] * plans[0][2], plans[1][0] * plans[1][2])
    capacity = jnp.where(is_edge, plans[0][0] * plans[0][1], plans[1][0] * plans[1][1])
    worst = jnp.int32(0)
    flag = jnp.int32(0)
    begins = []
    for way in range(2):
        for v in range(tiles):
            ahead, behind, end = starts(reach, lag_slots, [reaches[way][(v + u) % tiles] for u in range(reach)])
            worst = jnp.maximum(worst, end)
            if v == 0:
                begins.append(ahead)
    arrivals = []
    for way in range(2):
        ahead, _, _ = starts(reach, lag_slots, [reaches[way][(1 + u) % tiles] for u in range(reach)])
        arrivals.append(ahead)
    for t in range(tiles):
        flag = jnp.maximum(flag, table_ref[t, 0, LANES - 1] & 1)
    flag = jnp.where(worst > capacity, 1, flag)
    lane = lax.broadcasted_iota(jnp.int32, (1, LANES), 1)
    row = landing[tile]
    mark[...] = jnp.where(lane == LANES - 1, row - (row & 1) + flag, row)
    for way in range(2):
        for j in range(reach):
            plan_ref[0, 1 + way * reach + j] = arrivals[way][j]

    for edge in (True, False):
        size, rounds, lag = plans[0 if edge else 1]
        last_row = own_rows + size * rounds - 1

        @pl.when(is_edge if edge else jnp.logical_not(is_edge))
        def _():
            def keep(way, r):
                later_hop(way, r, size).wait_recv()
                pool_ref[way, pl.ds(own_rows + r * size, size)] = recv[way, pl.ds(r * size, size)]

            def gather(way, r):
                begin, arrived = begins[way], arrivals[way]
                for s in range(size):
                    p = r * size + s
                    row = jnp.minimum(p, own_rows - 1)
                    for j in range(1, reach):
                        row = jnp.where(p >= begin[j], p + (own_rows + arrived[j - 1] - begin[j]), row)
                    row = jnp.clip(row, 0, last_row)
                    stage[way, p] = pool_ref[way, row]

            def one_round(r):
                for way in range(2):
                    keep(way, r - lag)
                    gather(way, r)
                    later_hop(way, r, size).start()

            one_round(lag)
            for copy in across:
                copy.start()

            @pl.loop(lag + 1, rounds)
            def _(r):
                one_round(r)

            @pl.loop(rounds - lag, rounds)
            def _(r):
                for way in range(2):
                    keep(way, r)

            @pl.loop(0, rounds)
            def _(r):
                for way in range(2):
                    later_hop(way, r, size).wait_send()

    for copy in across:
        copy.wait()
    rows_over = pltpu.make_async_copy(marks, table_ref.at[pl.ds(tiles, bands)], local_sem)
    rows_over.start()
    rows_over.wait()
    for j in range(1, bands):
        flag = jnp.maximum(flag, table_ref[tiles + lax.rem(band + j, bands), 0, LANES - 1] & 1)
    plan_ref[0, 0] = flag

    @pl.when(band < bands - 1)
    def _():
        upward.wait_send()
        downward.wait_recv()

    @pl.when(band > 0)
    def _():
        downward.wait_send()
        upward.wait_recv()


def take_kernel(tiles, bands, bucket, table_ref, plan_ref, own_ref, pool_ref, beside_ref, out_ref):
    band, tile = lax.axis_index("band"), lax.axis_index("tile")
    reach = tiles // 2
    own_rows = 2 * bucket
    at = layout(bucket)
    out_ref[...] = jnp.zeros_like(out_ref)

    def how_many(row, kind):
        return (table_ref[row, 0, LANES - 1] >> (1 + 6 * kind)) & 63

    @pl.loop(0, how_many(tile, 0))
    def _(i):
        out_ref[table_ref[tile, 0, at["own"] + i]] += own_ref[i]

    for way in range(2):
        other = tiles + jnp.clip(band - 1 if way == 0 else band + 1, 0, bands - 1)
        valid = (band > 0) if way == 0 else (band < bands - 1)

        @pl.loop(0, jnp.where(valid, how_many(other, 1 + way), 0))
        def _(i):
            out_ref[table_ref[other, 0, at["up"] + way * bucket + i]] += beside_ref[way, i]

    for way in range(2):
        for distance in range(1, reach + 1):
            source = ring_tile(tiles, tile, -distance if way == 0 else distance)
            reaches = reaching(tiles, bucket, way, lambda i: table_ref[source, 0, i])
            start = own_rows + plan_ref[0, 1 + way * reach + distance - 1]

            @pl.loop(reaches[distance + 1], reaches[distance])
            def _(i):
                out_ref[table_ref[source, 0, way * own_rows + i]] += pool_ref[way, start + i]


def adaptive(tiles, bands, patches, pair_patch, pair_atm, numerators, counts):
    pairs, patch_rows, cell_rows = numerators.shape
    flux = patches.shape[1]
    blocks_owned = CELLS_DEV // cell_rows
    bucket = pairs // 8
    reach = tiles // 2
    group = 16
    plans = ((5, 4 * reach, 4), (3, 4 * reach, 3))
    slots = max(size * rounds for size, rounds, _ in plans)
    most = max(rounds for _, rounds, _ in plans)
    smem = pl.BlockSpec(memory_space=pltpu.SMEM)
    vmem = pl.BlockSpec(memory_space=pltpu.VMEM)
    hbm = pl.BlockSpec(memory_space=pltpu.HBM)
    block = (cell_rows, flux)
    f32 = jnp.float32
    numerators = jnp.transpose(numerators, (0, 2, 1))
    pool, beside, own, table, plan = pl.pallas_call(
        functools.partial(stream_kernel, tiles, bands, bucket, blocks_owned, plans, group),
        out_shape=(jax.ShapeDtypeStruct((2, 2 * bucket + slots) + block, f32),
                   jax.ShapeDtypeStruct((2, bucket) + block, f32),
                   jax.ShapeDtypeStruct((bucket,) + block, f32),
                   jax.ShapeDtypeStruct((tiles + bands, 1, LANES), jnp.int32),
                   jax.ShapeDtypeStruct((1, LANES), jnp.int32)),
        in_specs=[smem, smem, vmem, hbm, hbm],
        out_specs=(vmem, vmem, vmem, smem, smem),
        scratch_shapes=[
            pltpu.VMEM((patches.shape[0] // patch_rows, patch_rows, flux), patches.dtype),
            pltpu.VMEM(numerators.shape, numerators.dtype),
            pltpu.VMEM((1, LANES), jnp.int32),
            pltpu.VMEM((2, pairs), jnp.int32),
            pltpu.SMEM((2, pairs), jnp.int32),
            pltpu.SemaphoreType.DMA((pairs // group + 1,)),
            pltpu.VMEM((pairs,) + block, f32),
            pltpu.VMEM((2, bucket) + block, f32),
            pltpu.VMEM((2, slots) + block, f32),
            pltpu.VMEM((2, slots) + block, f32),
            pltpu.VMEM((tiles, 1, LANES), jnp.int32),
            pltpu.VMEM((bands, 1, LANES), jnp.int32),
            pltpu.VMEM((1, LANES), jnp.int32),
            pltpu.SemaphoreType.DMA((2, most)),
            pltpu.SemaphoreType.DMA((2, most)),
            pltpu.SemaphoreType.DMA((2,)),
            pltpu.SemaphoreType.DMA((2,)),
            pltpu.SemaphoreType.DMA((tiles + bands - 2,)),
            pltpu.SemaphoreType.DMA((tiles + bands - 2,)),
            pltpu.SemaphoreType.DMA,
        ],
        compiler_params=pltpu.CompilerParams(collective_id=1, has_side_effects=True, vmem_limit_bytes=STREAM_LIMIT),
        name="stream",
    )(pair_patch, counts, pair_atm.reshape(1, pairs), patches.reshape(-1, patch_rows, flux), numerators)

    def take(patches, pair_patch, pair_atm, numerators, counts, table, plan, own, pool, beside):
        out = pl.pallas_call(
            functools.partial(take_kernel, tiles, bands, bucket),
            out_shape=jax.ShapeDtypeStruct((blocks_owned,) + block, f32),
            in_specs=[smem, smem, vmem, vmem, vmem],
            out_specs=vmem,
            compiler_params=pltpu.CompilerParams(vmem_limit_bytes=VMEM_LIMIT),
            name="take",
        )(table, plan, own, pool, beside)
        return out.reshape(blocks_owned * cell_rows, flux)

    def padded(patches, pair_patch, pair_atm, numerators, counts, table, plan, own, pool, beside):
        return per_device(tiles, bands, patches, pair_patch, pair_atm, numerators, counts)

    return lax.cond(plan[0, 0] > 0, padded, take, patches, pair_patch, pair_atm, numerators, counts,
                    table, plan, own, pool, beside)


def solution(mesh):
    spec = P(("band", "tile"))
    placed = (
        P(("band", "tile"), None),
        spec,
        spec,
        P(("band", "tile"), None, None),
        spec,
    )
    body = functools.partial(adaptive, mesh.shape["tile"], mesh.shape["band"])
    return jax.shard_map(body, mesh=mesh, in_specs=placed, out_specs=P(("band", "tile"), None), check_vma=False)
```

```python
import functools

import jax
import jax.numpy as jnp
from jax import lax
from jax.experimental import pallas as pl
from jax.experimental.pallas import tpu as pltpu
from jax.sharding import PartitionSpec as P

CELLS_DEV = 4096
SCALE = 2.0 ** (-27)
MESH = pl.DeviceIdType.MESH
LANES = 128
VMEM_LIMIT = 20 * 2 ** 20
STREAM_LIMIT = 24 * 2 ** 20
PADDED_LIMIT = 63 * 2 ** 20


def partners(count):
    if count & (count - 1) == 0:
        return [lambda me, k=k: me ^ k for k in range(count - 1, 0, -1)]
    return [lambda me, k=k: lax.rem(me + k, count) for k in range(1, count)]


def pack_kernel(tiles, bucket, blocks_owned, chunk,
                patch_ref, atm_ref, counts_ref, patches_hbm, numer_hbm,
                send_ref, labels_ref,
                patches_v, numer_v, table, used, patch_sem, numer_sems):
    pairs = numer_v.shape[0]
    patch_rows = numer_v.shape[2]
    chunks = pairs // chunk
    buckets = tiles + 2
    patch_copy = pltpu.make_async_copy(patches_hbm, patches_v, patch_sem)
    patch_copy.start()
    copies = []
    for c in range(chunks):
        part = pl.ds(c * chunk, chunk)
        copy = pltpu.make_async_copy(numer_hbm.at[part], numer_v.at[part], numer_sems.at[c])
        copy.start()
        copies.append(copy)
    band = lax.axis_index("band")
    live = counts_ref[0]

    for b in range(buckets):
        used[b] = 0

        @pl.loop(0, blocks_owned, unroll=16)
        def _(i):
            table[b * blocks_owned + i] = -1

        for s in range(bucket):
            labels_ref[b, 0, s] = -1
    patch_copy.wait()
    for c in range(chunks):
        copies[c].wait()

        @pl.when(c * chunk < live)
        def _():
            for j in range(chunk):
                g = c * chunk + j
                is_live = g < live
                atm = atm_ref[g]
                owner = lax.div(atm, blocks_owned)
                block = lax.rem(atm, blocks_owned)
                owner_band = lax.div(owner, tiles)
                owner_tile = lax.rem(owner, tiles)
                b = jnp.where(owner_band == band, owner_tile,
                              jnp.where(owner_band > band, tiles, tiles + 1))
                entry = b * blocks_owned + block
                known = table[entry]
                fresh = known < 0
                new = used[b]
                rank = jnp.where(fresh, new, known)

                @pl.when(is_live)
                def _():
                    table[entry] = rank
                    used[b] = jnp.where(fresh, new + 1, new)
                    labels_ref[b, 0, rank] = block

                slot = jnp.where(is_live, b * bucket + rank, buckets * bucket)
                rows = pl.multiple_of(patch_ref[g] * patch_rows, patch_rows)
                weight = (numer_v[g].astype(jnp.float32) * SCALE).astype(jnp.bfloat16)
                part = jnp.dot(weight, patches_v[pl.ds(rows, patch_rows), :],
                               preferred_element_type=jnp.float32)
                before = send_ref[slot]
                send_ref[slot] = jnp.where(fresh, part, before + part)


def send_kernel(tiles, bands, bucket, send_ref, labels_ref, recv_ref, recv_labels_ref,
                data_send, data_recv, label_send, label_recv):
    band, tile = lax.axis_index("band"), lax.axis_index("tile")
    barrier = pltpu.get_barrier_semaphore()
    steps = partners(tiles)
    for step in steps:
        pl.semaphore_signal(barrier, inc=1, device_id=(band, step(tile)), device_id_type=MESH)

    @pl.when(band < bands - 1)
    def _():
        pl.semaphore_signal(barrier, inc=1, device_id=(band + 1, tile), device_id_type=MESH)

    @pl.when(band > 0)
    def _():
        pl.semaphore_signal(barrier, inc=1, device_id=(band - 1, tile), device_id_type=MESH)

    neighbours = jnp.where(band < bands - 1, 1, 0) + jnp.where(band > 0, 1, 0)
    pl.semaphore_wait(barrier, tiles - 1 + neighbours)

    def pair(source, place, device, sem):
        rows = pl.ds(source * bucket, bucket)
        landing = pl.ds(place * bucket, bucket)
        return (
            pltpu.make_async_remote_copy(
                src_ref=labels_ref.at[source], dst_ref=recv_labels_ref.at[place],
                send_sem=label_send.at[sem], recv_sem=label_recv.at[sem],
                device_id=device, device_id_type=MESH),
            pltpu.make_async_remote_copy(
                src_ref=send_ref.at[rows], dst_ref=recv_ref.at[landing],
                send_sem=data_send.at[sem], recv_sem=data_recv.at[sem],
                device_id=device, device_id_type=MESH),
        )

    inside = [pair(step(tile), tile, (band, step(tile)), k) for k, step in enumerate(steps)]
    upward = pair(tiles, tiles, (band + 1, tile), tiles - 1)
    downward = pair(tiles + 1, tiles + 1, (band - 1, tile), tiles)
    for copies in inside[:2]:
        for copy in copies:
            copy.start()

    @pl.when(band < bands - 1)
    def _():
        for copy in upward:
            copy.start()

    @pl.when(band > 0)
    def _():
        for copy in downward:
            copy.start()

    for copies in inside[2:]:
        for copy in copies:
            copy.start()
    for copies in inside:
        for copy in copies:
            copy.wait()

    @pl.when(band < bands - 1)
    def _():
        for up, down in zip(upward, downward):
            up.wait_send()
            down.wait_recv()

    @pl.when(band > 0)
    def _():
        for up, down in zip(upward, downward):
            down.wait_send()
            up.wait_recv()


def add_kernel(tiles, bands, bucket, labels_ref, recv_labels_ref, send_hbm, recv_hbm, out_ref,
               landed, sems):
    band, tile = lax.axis_index("band"), lax.axis_index("tile")
    buckets = tiles + 2

    def copy_of(b, ref):
        rows = pl.ds(b * bucket, bucket)
        return pltpu.make_async_copy(ref.at[rows], landed.at[rows], sems.at[b])

    for b in range(buckets):
        if b < tiles:
            @pl.when(tile == b)
            def _():
                copy_of(b, send_hbm).start()

            @pl.when(tile != b)
            def _():
                copy_of(b, recv_hbm).start()
        else:
            copy_of(b, recv_hbm).start()
    out_ref[...] = jnp.zeros_like(out_ref)
    for b in range(buckets):
        copy_of(b, recv_hbm).wait()
        if b == tiles:
            valid = band > 0
        elif b == tiles + 1:
            valid = band < bands - 1
        else:
            valid = True
        for s in range(bucket):
            label = recv_labels_ref[b, 0, s]
            if b < tiles:
                label = jnp.where(tile == b, labels_ref[b, 0, s], label)

            @pl.when((label >= 0) & valid)
            def _():
                out_ref[label] += landed[b * bucket + s]


def per_device(tiles, bands, patches, pair_patch, pair_atm, numerators, counts):
    pairs, cell_rows, patch_rows = numerators.shape
    flux = patches.shape[1]
    blocks_owned = CELLS_DEV // cell_rows
    bucket = pairs // 8
    buckets = tiles + 2
    chunk = 16
    smem = pl.BlockSpec(memory_space=pltpu.SMEM)
    vmem = pl.BlockSpec(memory_space=pltpu.VMEM)
    anywhere = pl.BlockSpec(memory_space=pl.ANY)
    labels_shape = jax.ShapeDtypeStruct((buckets, 1, LANES), jnp.int32)
    recv_shape = jax.ShapeDtypeStruct((buckets * bucket, cell_rows, flux), jnp.float32)
    send, labels = pl.pallas_call(
        functools.partial(pack_kernel, tiles, bucket, blocks_owned, chunk),
        out_shape=(jax.ShapeDtypeStruct((buckets * bucket + 1, cell_rows, flux), jnp.float32), labels_shape),
        in_specs=[smem, smem, smem, anywhere, anywhere],
        out_specs=(vmem, smem),
        scratch_shapes=[
            pltpu.VMEM(patches.shape, patches.dtype),
            pltpu.VMEM((pairs, cell_rows, patch_rows), jnp.int32),
            pltpu.SMEM((buckets * blocks_owned,), jnp.int32),
            pltpu.SMEM((buckets,), jnp.int32),
            pltpu.SemaphoreType.DMA,
            pltpu.SemaphoreType.DMA((pairs // chunk,)),
        ],
        compiler_params=pltpu.CompilerParams(vmem_limit_bytes=PADDED_LIMIT),
        name="pack",
    )(pair_patch, pair_atm, counts, patches, numerators)
    recv, recv_labels = pl.pallas_call(
        functools.partial(send_kernel, tiles, bands, bucket),
        out_shape=(recv_shape, labels_shape),
        in_specs=[anywhere, anywhere],
        out_specs=(anywhere, anywhere),
        scratch_shapes=[pltpu.SemaphoreType.DMA((tiles + 1,))] * 4,
        compiler_params=pltpu.CompilerParams(collective_id=0, has_side_effects=True, vmem_limit_bytes=VMEM_LIMIT),
        name="exchange",
    )(send, labels)
    out = pl.pallas_call(
        functools.partial(add_kernel, tiles, bands, bucket),
        out_shape=jax.ShapeDtypeStruct((blocks_owned, cell_rows, flux), jnp.float32),
        in_specs=[smem, smem, anywhere, anywhere],
        out_specs=vmem,
        scratch_shapes=[
            pltpu.VMEM(recv_shape.shape, jnp.float32),
            pltpu.SemaphoreType.DMA((buckets,)),
        ],
        compiler_params=pltpu.CompilerParams(vmem_limit_bytes=VMEM_LIMIT),
        name="add",
    )(labels, recv_labels, send, recv)
    return out.reshape(blocks_owned * cell_rows, flux)


def ring_order(tiles):
    wide = tiles // 4
    if wide * 4 != tiles or wide % 2:
        return list(range(tiles))
    order = list(range(wide))
    for step, column in enumerate(reversed(range(wide))):
        rows = range(1, 4) if step % 2 == 0 else range(3, 0, -1)
        order += [row * wide + column for row in rows]
    return order


def chosen(values, index):
    picked = values[0]
    for k in range(1, len(values)):
        picked = jnp.where(index == k, values[k], picked)
    return picked


def ring_tile(tiles, tile, steps):
    order = ring_order(tiles)
    position = chosen([order.index(k) for k in range(tiles)], tile)
    return chosen(order, lax.rem(position + steps + tiles, tiles))


def layout(bucket):
    return dict(up=4 * bucket, down=5 * bucket, own=6 * bucket, end=7 * bucket)


def reaching(tiles, bucket, way, read):
    reach = tiles // 2
    base = 7 * bucket - 1
    far = read(base + reach)
    counts = [read(base + (k if way == 0 else tiles - k)) for k in range(1, reach)]
    counts.append((far + 1) >> 1 if way == 0 else far >> 1)
    beyond = [0]
    for count in reversed(counts):
        beyond.append(beyond[-1] + count)
    return [None] + beyond[::-1]


def split(value, size):
    if size & (size - 1) == 0:
        return value >> (size.bit_length() - 1), value & (size - 1)
    return lax.div(value, size), lax.rem(value, size)


def sort_pairs(tiles, bands, bucket, blocks_owned, band, tile, live, atm):
    pairs = atm.shape[1]
    reach = tiles // 2
    order = ring_order(tiles)
    spots = [order.index(k) for k in range(tiles)]
    here = chosen(spots, tile)
    wide = (pairs, pairs)

    def across(value):
        return jnp.broadcast_to(value, wide).T

    def least(value):
        return jnp.min(value, axis=0, keepdims=True)

    def most(value):
        return jnp.max(value, axis=0, keepdims=True)

    def count(mask):
        return jnp.sum(jnp.where(mask, 1, 0), axis=0, keepdims=True)

    def bucket_of(value):
        owner, block = split(value, blocks_owned)
        owner_band, owner_tile = split(owner, tiles)
        ahead = split(chosen(spots, owner_tile) - here + tiles, tiles)[1]
        return jnp.where(owner_band == band, ahead, jnp.where(owner_band > band, tiles, tiles + 1)), block

    row = lax.broadcasted_iota(jnp.int32, wide, 0)
    lane = lax.broadcasted_iota(jnp.int32, wide, 1)
    one_lane = lax.broadcasted_iota(jnp.int32, (1, pairs), 1)
    atm_c = across(atm)
    live_c = row < live
    same = (atm_c == atm) & live_c
    first = least(jnp.where(same, row, pairs))
    before = most(jnp.where(same & (row < lane), row, -1))
    fresh_c = (across(first) == row) & live_c
    b, _ = bucket_of(atm)
    b_c, block_c = bucket_of(atm_c)
    rank = count(fresh_c & (b_c == b) & (row < first))
    back = (b > reach) | ((b == reach) & ((rank & 1) == 1))
    region = jnp.where(b == 0, 4, jnp.where(b >= tiles, b - tiles + 2, jnp.where(back, 1, 0)))
    near = jnp.where(region == 0, reach - b, jnp.where(region == 1, b - reach, 0))
    shift = ((reach + 1) * (pairs + 1)).bit_length()
    key = (region << shift) + near * (pairs + 1) + first
    key_c = across(key)
    place = count(fresh_c & ((key_c >> shift) == region) & (key_c < key))
    ring = region < 2
    room = jnp.where(ring, 2 * bucket, bucket)
    base = jnp.where(ring, 2 * region, region + 2) * bucket
    fits = place < room
    slot = jnp.where((one_lane < live) & fits, base + place, pairs)
    overflow = jnp.max(jnp.where((one_lane < live) & jnp.logical_not(fits), 1, 0), axis=1, keepdims=True)
    hit = across(slot) == lane
    last = most(jnp.where(hit, row, 0))
    label = most(jnp.where(hit, block_c, -1))
    counts = count(fresh_c & (b_c == lane - (7 * bucket - 1)))
    kinds = [count(fresh_c & (b_c == k)) for k in (0, tiles, tiles + 1)]
    packed = overflow + sum(kind << (1 + 6 * i) for i, kind in enumerate(kinds))
    labels = jnp.where(one_lane < 7 * bucket, label, jnp.where(one_lane == pairs - 1, packed, counts))
    return before, last, labels


def starts(reach, lag, reaches):
    first = [None] * (reach + 1)
    for u in range(reach - 1, -1, -1):
        begin = [0]
        for j in range(1, reach - u):
            after = begin[j - 1] + reaches[u + j - 1][j]
            begin.append(jnp.maximum(after, first[u + 1][j - 1] + lag))
        first[u] = begin
    end = jnp.int32(0)
    for j in range(reach):
        size = reaches[j][j + 1]
        end = jnp.where(size > 0, first[0][j] + size, end)
    return first[0], first[1], end


def stream_kernel(tiles, bands, bucket, blocks_owned, plans, group,
                  patch_ref, counts_ref, atm_ref, patches_hbm, numer_hbm,
                  pool_ref, beside_ref, own_ref, landing, flag_ref,
                  patches_ref, numer_ref, labels_ref, work_v, work_ref, load_sems, sums, side, stage, recv, table_ref, mark,
                  ring_send, ring_recv, beside_send, beside_recv, label_send, label_recv, local_sem):
    band, tile = lax.axis_index("band"), lax.axis_index("tile")
    reach = tiles // 2
    own_rows = 2 * bucket
    at = layout(bucket)
    steps = partners(tiles)
    pairs = numer_ref.shape[0]

    def numer_load(c):
        part = pl.ds(c * group, group)
        return pltpu.make_async_copy(numer_hbm.at[part], numer_ref.at[part], load_sems.at[c])

    patch_load = pltpu.make_async_copy(patches_hbm, patches_ref, load_sems.at[pairs // group])
    patch_load.start()
    for c in range(pairs // group):
        numer_load(c).start()
    barrier = pltpu.get_barrier_semaphore()
    for step in steps:
        pl.semaphore_signal(barrier, inc=1, device_id=(band, step(tile)), device_id_type=MESH)
    for j in range(1, bands):
        pl.semaphore_signal(barrier, inc=1, device_id=(lax.rem(band + j, bands), tile), device_id_type=MESH)
    before, last, labels = sort_pairs(tiles, bands, bucket, blocks_owned, band, tile, counts_ref[0], atm_ref[...])
    labels_ref[...] = labels
    landing[tile] = labels
    work_v[0:1] = before
    work_v[1:2] = last
    work_in = pltpu.make_async_copy(work_v, work_ref, local_sem)
    work_in.start()
    work_in.wait()
    patch_load.wait()

    @pl.loop(0, pairs // group)
    def _(c):
        numer_load(c).wait()
        for j in range(group):
            g = c * group + j
            weight = (numer_ref[g].astype(jnp.float32) * SCALE).astype(jnp.bfloat16)
            part = jnp.dot(weight, patches_ref[patch_ref[g]], preferred_element_type=jnp.float32)
            before = work_ref[0, g]
            earlier = sums[jnp.maximum(before, 0)]
            sums[g] = part + jnp.where(before >= 0, earlier, 0.0)

    def total(slot):
        return sums[work_ref[1, slot]]

    targets = ((band, ring_tile(tiles, tile, 1)), (band, ring_tile(tiles, tile, -1)))
    is_edge = (band == 0) | (band == bands - 1)
    head = max(size * lag for size, _, lag in plans)
    for way in range(2):
        for s in range(head):
            pool_ref[way, s] = total(way * own_rows + s)
    pl.semaphore_wait(barrier, tiles + bands - 2)
    inside = [
        pltpu.make_async_remote_copy(
            src_ref=labels_ref, dst_ref=landing.at[tile],
            send_sem=label_send.at[k], recv_sem=label_recv.at[k],
            device_id=(band, step(tile)), device_id_type=MESH)
        for k, step in enumerate(steps)
    ]
    across = [
        pltpu.make_async_remote_copy(
            src_ref=mark, dst_ref=landing.at[tiles + band],
            send_sem=label_send.at[tiles - 2 + j], recv_sem=label_recv.at[tiles - 2 + j],
            device_id=(lax.rem(band + j, bands), tile), device_id_type=MESH)
        for j in range(1, bands)
    ]
    for copy in inside:
        copy.start()

    def hop(way, r, size, source):
        rows = pl.ds(r * size, size)
        return pltpu.make_async_remote_copy(
            src_ref=source, dst_ref=recv.at[way, rows],
            send_sem=ring_send.at[way, r], recv_sem=ring_recv.at[way, r],
            device_id=targets[way], device_id_type=MESH)

    def own_hop(way, r, size):
        return hop(way, r, size, pool_ref.at[way, pl.ds(r * size, size)])

    def later_hop(way, r, size):
        return hop(way, r, size, stage.at[way, pl.ds(r * size, size)])

    for edge in (True, False):
        size, rounds, lag = plans[0 if edge else 1]

        @pl.when(is_edge if edge else jnp.logical_not(is_edge))
        def _():
            for r in range(lag):
                for way in range(2):
                    own_hop(way, r, size).start()

    def beside(way, target_band):
        return pltpu.make_async_remote_copy(
            src_ref=side.at[way], dst_ref=beside_ref.at[way],
            send_sem=beside_send.at[way], recv_sem=beside_recv.at[way],
            device_id=(target_band, tile), device_id_type=MESH)

    upward, downward = beside(0, band + 1), beside(1, band - 1)
    for way in range(2):
        for s in range(bucket):
            side[way, s] = total(at["up"] + way * bucket + s)
    for way in range(2):
        for s in range(head, own_rows):
            pool_ref[way, s] = total(way * own_rows + s)
    for s in range(bucket):
        own_ref[s] = total(at["own"] + s)

    @pl.when(band < bands - 1)
    def _():
        upward.start()

    @pl.when(band > 0)
    def _():
        downward.start()

    for copy in inside:
        copy.wait()
    rows_in = pltpu.make_async_copy(landing.at[pl.ds(0, tiles)], table_ref.at[pl.ds(0, tiles)], local_sem)
    rows_in.start()
    rows_in.wait()

    upstream = [[ring_tile(tiles, tile, -u if way == 0 else u) for u in range(tiles)] for way in range(2)]
    reaches = [[reaching(tiles, bucket, way, lambda i, t=t: table_ref[t, 0, i]) for t in upstream[way]]
               for way in range(2)]
    lag_slots = jnp.where(is_edge, plans[0][0] * plans[0][2], plans[1][0] * plans[1][2])
    capacity = jnp.where(is_edge, plans[0][0] * plans[0][1], plans[1][0] * plans[1][1])
    worst = jnp.int32(0)
    flag = jnp.int32(0)
    begins = []
    for way in range(2):
        for v in range(tiles):
            ahead, behind, end = starts(reach, lag_slots, [reaches[way][(v + u) % tiles] for u in range(reach)])
            worst = jnp.maximum(worst, end)
            if v == 0:
                begins.append(ahead)
    arrivals = []
    for way in range(2):
        ahead, _, _ = starts(reach, lag_slots, [reaches[way][(1 + u) % tiles] for u in range(reach)])
        arrivals.append(ahead)
    for t in range(tiles):
        flag = jnp.maximum(flag, table_ref[t, 0, LANES - 1] & 1)
    flag = jnp.where(worst > capacity, 1, flag)
    lane = lax.broadcasted_iota(jnp.int32, (1, LANES), 1)
    row = landing[tile]
    mark[...] = jnp.where(lane == LANES - 1, row - (row & 1) + flag, row)
    plan = jnp.zeros((1, LANES), jnp.int32)
    for way in range(2):
        for j in range(reach):
            plan = jnp.where(lane == way * reach + j, arrivals[way][j], plan)
    landing[tiles + bands] = plan

    for edge in (True, False):
        size, rounds, lag = plans[0 if edge else 1]
        last_row = own_rows + size * rounds - 1

        @pl.when(is_edge if edge else jnp.logical_not(is_edge))
        def _():
            def keep(way, r):
                later_hop(way, r, size).wait_recv()
                pool_ref[way, pl.ds(own_rows + r * size, size)] = recv[way, pl.ds(r * size, size)]

            def gather(way, r):
                begin, arrived = begins[way], arrivals[way]
                for s in range(size):
                    p = r * size + s
                    row = jnp.minimum(p, own_rows - 1)
                    for j in range(1, reach):
                        row = jnp.where(p >= begin[j], p + (own_rows + arrived[j - 1] - begin[j]), row)
                    row = jnp.clip(row, 0, last_row)
                    stage[way, p] = pool_ref[way, row]

            def one_round(r):
                for way in range(2):
                    keep(way, r - lag)
                    gather(way, r)
                    later_hop(way, r, size).start()

            one_round(lag)
            for copy in across:
                copy.start()

            @pl.loop(lag + 1, rounds)
            def _(r):
                one_round(r)

    for copy in across:
        copy.wait()
    rows_over = pltpu.make_async_copy(landing.at[pl.ds(tiles, bands)], table_ref.at[pl.ds(tiles, bands)], local_sem)
    rows_over.start()
    rows_over.wait()
    for j in range(1, bands):
        flag = jnp.maximum(flag, table_ref[tiles + lax.rem(band + j, bands), 0, LANES - 1] & 1)
    flag_ref[0] = flag

    @pl.when(band < bands - 1)
    def _():
        upward.wait_send()
        downward.wait_recv()

    @pl.when(band > 0)
    def _():
        downward.wait_send()
        upward.wait_recv()

    for edge in (True, False):
        size, rounds, lag = plans[0 if edge else 1]

        @pl.when(is_edge if edge else jnp.logical_not(is_edge))
        def _():
            @pl.loop(0, rounds - lag)
            def _(r):
                for way in range(2):
                    later_hop(way, r, size).wait_send()

            @pl.loop(rounds - lag, rounds)
            def _(r):
                for way in range(2):
                    later_hop(way, r, size).wait()
                    pool_ref[way, pl.ds(own_rows + r * size, size)] = recv[way, pl.ds(r * size, size)]


def take_kernel(tiles, bands, bucket, table_ref, own_ref, pool_ref, beside_ref, out_ref):
    band, tile = lax.axis_index("band"), lax.axis_index("tile")
    reach = tiles // 2
    own_rows = 2 * bucket
    at = layout(bucket)
    out_ref[...] = jnp.zeros_like(out_ref)

    def how_many(lane, kind):
        return (lane >> (1 + 6 * kind)) & 63

    def add(low, high, label_of, block_of):
        fours = (high - low) >> 2

        @pl.loop(0, fours)
        def _(k):
            at_once = [low + 4 * k + j for j in range(4)]
            labels = [label_of(i) for i in at_once]
            sums = [out_ref[label] + block_of(i) for label, i in zip(labels, at_once)]
            for label, total in zip(labels, sums):
                out_ref[label] = total

        @pl.loop(low + 4 * fours, high)
        def _(i):
            out_ref[label_of(i)] += block_of(i)

    add(0, how_many(table_ref[tile, 0, LANES - 1], 0),
        lambda i: table_ref[tile, 0, at["own"] + i], lambda i: own_ref[i])
    for way in range(2):
        other = tiles + jnp.clip(band - 1 if way == 0 else band + 1, 0, bands - 1)
        valid = (band > 0) if way == 0 else (band < bands - 1)
        add(0, jnp.where(valid, how_many(table_ref[other, 0, LANES - 1], 1 + way), 0),
            lambda i: table_ref[other, 0, at["up"] + way * bucket + i], lambda i: beside_ref[way, i])

    for way in range(2):
        for distance in range(1, reach + 1):
            source = ring_tile(tiles, tile, -distance if way == 0 else distance)
            reaches = reaching(tiles, bucket, way, lambda i: table_ref[source, 0, i])
            start = own_rows + table_ref[tiles + bands, 0, way * reach + distance - 1]
            add(reaches[distance + 1], reaches[distance],
                lambda i: table_ref[source, 0, way * own_rows + i], lambda i: pool_ref[way, start + i])


def adaptive(tiles, bands, patches, pair_patch, pair_atm, numerators, counts):
    pairs, patch_rows, cell_rows = numerators.shape
    flux = patches.shape[1]
    blocks_owned = CELLS_DEV // cell_rows
    bucket = pairs // 8
    reach = tiles // 2
    group = 16
    plans = ((5, 4 * reach, 4), (3, 4 * reach, 3))
    slots = max(size * rounds for size, rounds, _ in plans)
    most = max(rounds for _, rounds, _ in plans)
    smem = pl.BlockSpec(memory_space=pltpu.SMEM)
    vmem = pl.BlockSpec(memory_space=pltpu.VMEM)
    hbm = pl.BlockSpec(memory_space=pltpu.HBM)
    block = (cell_rows, flux)
    f32 = jnp.float32
    numerators = jnp.transpose(numerators, (0, 2, 1))
    pool, beside, own, table, flag = pl.pallas_call(
        functools.partial(stream_kernel, tiles, bands, bucket, blocks_owned, plans, group),
        out_shape=(jax.ShapeDtypeStruct((2, 2 * bucket + slots) + block, f32),
                   jax.ShapeDtypeStruct((2, bucket) + block, f32),
                   jax.ShapeDtypeStruct((bucket,) + block, f32),
                   jax.ShapeDtypeStruct((tiles + bands + 1, 1, LANES), jnp.int32),
                   jax.ShapeDtypeStruct((1,), jnp.int32)),
        in_specs=[smem, smem, vmem, hbm, hbm],
        out_specs=(vmem, vmem, vmem, vmem, smem),
        scratch_shapes=[
            pltpu.VMEM((patches.shape[0] // patch_rows, patch_rows, flux), patches.dtype),
            pltpu.VMEM(numerators.shape, numerators.dtype),
            pltpu.VMEM((1, LANES), jnp.int32),
            pltpu.VMEM((2, pairs), jnp.int32),
            pltpu.SMEM((2, pairs), jnp.int32),
            pltpu.SemaphoreType.DMA((pairs // group + 1,)),
            pltpu.VMEM((pairs,) + block, f32),
            pltpu.VMEM((2, bucket) + block, f32),
            pltpu.VMEM((2, slots) + block, f32),
            pltpu.VMEM((2, slots) + block, f32),
            pltpu.SMEM((tiles + bands, 1, LANES), jnp.int32),
            pltpu.VMEM((1, LANES), jnp.int32),
            pltpu.SemaphoreType.DMA((2, most)),
            pltpu.SemaphoreType.DMA((2, most)),
            pltpu.SemaphoreType.DMA((2,)),
            pltpu.SemaphoreType.DMA((2,)),
            pltpu.SemaphoreType.DMA((tiles + bands - 2,)),
            pltpu.SemaphoreType.DMA((tiles + bands - 2,)),
            pltpu.SemaphoreType.DMA,
        ],
        compiler_params=pltpu.CompilerParams(collective_id=1, has_side_effects=True, vmem_limit_bytes=STREAM_LIMIT),
        name="stream",
    )(pair_patch, counts, pair_atm.reshape(1, pairs), patches.reshape(-1, patch_rows, flux), numerators)

    def take(patches, pair_patch, pair_atm, numerators, counts, table, own, pool, beside):
        out = pl.pallas_call(
            functools.partial(take_kernel, tiles, bands, bucket),
            out_shape=jax.ShapeDtypeStruct((blocks_owned,) + block, f32),
            in_specs=[smem, vmem, vmem, vmem],
            out_specs=vmem,
            compiler_params=pltpu.CompilerParams(vmem_limit_bytes=VMEM_LIMIT),
            name="take",
        )(table, own, pool, beside)
        return out.reshape(blocks_owned * cell_rows, flux)

    def padded(patches, pair_patch, pair_atm, numerators, counts, table, own, pool, beside):
        return per_device(tiles, bands, patches, pair_patch, pair_atm, numerators, counts)

    return lax.cond(flag[0] > 0, padded, take, patches, pair_patch, pair_atm, numerators, counts,
                    table, own, pool, beside)


def solution(mesh):
    spec = P(("band", "tile"))
    placed = (
        P(("band", "tile"), None),
        spec,
        spec,
        P(("band", "tile"), None, None),
        spec,
    )
    body = functools.partial(adaptive, mesh.shape["tile"], mesh.shape["band"])
    return jax.shard_map(body, mesh=mesh, in_specs=placed, out_specs=P(("band", "tile"), None), check_vma=False)
```

```python
import functools

import jax
import jax.numpy as jnp
from jax import lax
from jax.experimental import pallas as pl
from jax.experimental.pallas import tpu as pltpu
from jax.sharding import PartitionSpec as P

CELLS_DEV = 4096
SCALE = 2.0 ** (-27)
MESH = pl.DeviceIdType.MESH
LANES = 128
VMEM_LIMIT = 20 * 2 ** 20
STREAM_LIMIT = 24 * 2 ** 20
PADDED_LIMIT = 63 * 2 ** 20


def partners(count):
    if count & (count - 1) == 0:
        return [lambda me, k=k: me ^ k for k in range(count - 1, 0, -1)]
    return [lambda me, k=k: lax.rem(me + k, count) for k in range(1, count)]


def pack_kernel(tiles, bucket, blocks_owned, chunk,
                patch_ref, atm_ref, counts_ref, patches_hbm, numer_hbm,
                send_ref, labels_ref,
                patches_v, numer_v, table, used, patch_sem, numer_sems):
    pairs = numer_v.shape[0]
    patch_rows = numer_v.shape[2]
    chunks = pairs // chunk
    buckets = tiles + 2
    patch_copy = pltpu.make_async_copy(patches_hbm, patches_v, patch_sem)
    patch_copy.start()
    copies = []
    for c in range(chunks):
        part = pl.ds(c * chunk, chunk)
        copy = pltpu.make_async_copy(numer_hbm.at[part], numer_v.at[part], numer_sems.at[c])
        copy.start()
        copies.append(copy)
    band = lax.axis_index("band")
    live = counts_ref[0]

    for b in range(buckets):
        used[b] = 0

        @pl.loop(0, blocks_owned, unroll=16)
        def _(i):
            table[b * blocks_owned + i] = -1

        for s in range(bucket):
            labels_ref[b, 0, s] = -1
    patch_copy.wait()
    for c in range(chunks):
        copies[c].wait()

        @pl.when(c * chunk < live)
        def _():
            for j in range(chunk):
                g = c * chunk + j
                is_live = g < live
                atm = atm_ref[g]
                owner = lax.div(atm, blocks_owned)
                block = lax.rem(atm, blocks_owned)
                owner_band = lax.div(owner, tiles)
                owner_tile = lax.rem(owner, tiles)
                b = jnp.where(owner_band == band, owner_tile,
                              jnp.where(owner_band > band, tiles, tiles + 1))
                entry = b * blocks_owned + block
                known = table[entry]
                fresh = known < 0
                new = used[b]
                rank = jnp.where(fresh, new, known)

                @pl.when(is_live)
                def _():
                    table[entry] = rank
                    used[b] = jnp.where(fresh, new + 1, new)
                    labels_ref[b, 0, rank] = block

                slot = jnp.where(is_live, b * bucket + rank, buckets * bucket)
                rows = pl.multiple_of(patch_ref[g] * patch_rows, patch_rows)
                weight = (numer_v[g].astype(jnp.float32) * SCALE).astype(jnp.bfloat16)
                part = jnp.dot(weight, patches_v[pl.ds(rows, patch_rows), :],
                               preferred_element_type=jnp.float32)
                before = send_ref[slot]
                send_ref[slot] = jnp.where(fresh, part, before + part)


def send_kernel(tiles, bands, bucket, send_ref, labels_ref, recv_ref, recv_labels_ref,
                data_send, data_recv, label_send, label_recv):
    band, tile = lax.axis_index("band"), lax.axis_index("tile")
    barrier = pltpu.get_barrier_semaphore()
    steps = partners(tiles)
    for step in steps:
        pl.semaphore_signal(barrier, inc=1, device_id=(band, step(tile)), device_id_type=MESH)

    @pl.when(band < bands - 1)
    def _():
        pl.semaphore_signal(barrier, inc=1, device_id=(band + 1, tile), device_id_type=MESH)

    @pl.when(band > 0)
    def _():
        pl.semaphore_signal(barrier, inc=1, device_id=(band - 1, tile), device_id_type=MESH)

    neighbours = jnp.where(band < bands - 1, 1, 0) + jnp.where(band > 0, 1, 0)
    pl.semaphore_wait(barrier, tiles - 1 + neighbours)

    def pair(source, place, device, sem):
        rows = pl.ds(source * bucket, bucket)
        landing = pl.ds(place * bucket, bucket)
        return (
            pltpu.make_async_remote_copy(
                src_ref=labels_ref.at[source], dst_ref=recv_labels_ref.at[place],
                send_sem=label_send.at[sem], recv_sem=label_recv.at[sem],
                device_id=device, device_id_type=MESH),
            pltpu.make_async_remote_copy(
                src_ref=send_ref.at[rows], dst_ref=recv_ref.at[landing],
                send_sem=data_send.at[sem], recv_sem=data_recv.at[sem],
                device_id=device, device_id_type=MESH),
        )

    inside = [pair(step(tile), tile, (band, step(tile)), k) for k, step in enumerate(steps)]
    upward = pair(tiles, tiles, (band + 1, tile), tiles - 1)
    downward = pair(tiles + 1, tiles + 1, (band - 1, tile), tiles)
    for copies in inside[:2]:
        for copy in copies:
            copy.start()

    @pl.when(band < bands - 1)
    def _():
        for copy in upward:
            copy.start()

    @pl.when(band > 0)
    def _():
        for copy in downward:
            copy.start()

    for copies in inside[2:]:
        for copy in copies:
            copy.start()
    for copies in inside:
        for copy in copies:
            copy.wait()

    @pl.when(band < bands - 1)
    def _():
        for up, down in zip(upward, downward):
            up.wait_send()
            down.wait_recv()

    @pl.when(band > 0)
    def _():
        for up, down in zip(upward, downward):
            down.wait_send()
            up.wait_recv()


def add_kernel(tiles, bands, bucket, labels_ref, recv_labels_ref, send_hbm, recv_hbm, out_ref,
               landed, sems):
    band, tile = lax.axis_index("band"), lax.axis_index("tile")
    buckets = tiles + 2

    def copy_of(b, ref):
        rows = pl.ds(b * bucket, bucket)
        return pltpu.make_async_copy(ref.at[rows], landed.at[rows], sems.at[b])

    for b in range(buckets):
        if b < tiles:
            @pl.when(tile == b)
            def _():
                copy_of(b, send_hbm).start()

            @pl.when(tile != b)
            def _():
                copy_of(b, recv_hbm).start()
        else:
            copy_of(b, recv_hbm).start()
    out_ref[...] = jnp.zeros_like(out_ref)
    for b in range(buckets):
        copy_of(b, recv_hbm).wait()
        if b == tiles:
            valid = band > 0
        elif b == tiles + 1:
            valid = band < bands - 1
        else:
            valid = True
        for s in range(bucket):
            label = recv_labels_ref[b, 0, s]
            if b < tiles:
                label = jnp.where(tile == b, labels_ref[b, 0, s], label)

            @pl.when((label >= 0) & valid)
            def _():
                out_ref[label] += landed[b * bucket + s]


def per_device(tiles, bands, patches, pair_patch, pair_atm, numerators, counts):
    pairs, cell_rows, patch_rows = numerators.shape
    flux = patches.shape[1]
    blocks_owned = CELLS_DEV // cell_rows
    bucket = pairs // 8
    buckets = tiles + 2
    chunk = 16
    smem = pl.BlockSpec(memory_space=pltpu.SMEM)
    vmem = pl.BlockSpec(memory_space=pltpu.VMEM)
    anywhere = pl.BlockSpec(memory_space=pl.ANY)
    labels_shape = jax.ShapeDtypeStruct((buckets, 1, LANES), jnp.int32)
    recv_shape = jax.ShapeDtypeStruct((buckets * bucket, cell_rows, flux), jnp.float32)
    send, labels = pl.pallas_call(
        functools.partial(pack_kernel, tiles, bucket, blocks_owned, chunk),
        out_shape=(jax.ShapeDtypeStruct((buckets * bucket + 1, cell_rows, flux), jnp.float32), labels_shape),
        in_specs=[smem, smem, smem, anywhere, anywhere],
        out_specs=(vmem, smem),
        scratch_shapes=[
            pltpu.VMEM(patches.shape, patches.dtype),
            pltpu.VMEM((pairs, cell_rows, patch_rows), jnp.int32),
            pltpu.SMEM((buckets * blocks_owned,), jnp.int32),
            pltpu.SMEM((buckets,), jnp.int32),
            pltpu.SemaphoreType.DMA,
            pltpu.SemaphoreType.DMA((pairs // chunk,)),
        ],
        compiler_params=pltpu.CompilerParams(vmem_limit_bytes=PADDED_LIMIT),
        name="pack",
    )(pair_patch, pair_atm, counts, patches, numerators)
    recv, recv_labels = pl.pallas_call(
        functools.partial(send_kernel, tiles, bands, bucket),
        out_shape=(recv_shape, labels_shape),
        in_specs=[anywhere, anywhere],
        out_specs=(anywhere, anywhere),
        scratch_shapes=[pltpu.SemaphoreType.DMA((tiles + 1,))] * 4,
        compiler_params=pltpu.CompilerParams(collective_id=0, has_side_effects=True, vmem_limit_bytes=VMEM_LIMIT),
        name="exchange",
    )(send, labels)
    out = pl.pallas_call(
        functools.partial(add_kernel, tiles, bands, bucket),
        out_shape=jax.ShapeDtypeStruct((blocks_owned, cell_rows, flux), jnp.float32),
        in_specs=[smem, smem, anywhere, anywhere],
        out_specs=vmem,
        scratch_shapes=[
            pltpu.VMEM(recv_shape.shape, jnp.float32),
            pltpu.SemaphoreType.DMA((buckets,)),
        ],
        compiler_params=pltpu.CompilerParams(vmem_limit_bytes=VMEM_LIMIT),
        name="add",
    )(labels, recv_labels, send, recv)
    return out.reshape(blocks_owned * cell_rows, flux)


def ring_order(tiles):
    wide = tiles // 4
    if wide * 4 != tiles or wide % 2:
        return list(range(tiles))
    order = list(range(wide))
    for step, column in enumerate(reversed(range(wide))):
        rows = range(1, 4) if step % 2 == 0 else range(3, 0, -1)
        order += [row * wide + column for row in rows]
    return order


def chosen(values, index):
    picked = values[0]
    for k in range(1, len(values)):
        picked = jnp.where(index == k, values[k], picked)
    return picked


def ring_tile(tiles, tile, steps):
    order = ring_order(tiles)
    position = chosen([order.index(k) for k in range(tiles)], tile)
    return chosen(order, lax.rem(position + steps + tiles, tiles))


def layout(bucket):
    return dict(up=4 * bucket, down=5 * bucket, own=6 * bucket, end=7 * bucket)


def reaching(tiles, bucket, way, read):
    reach = tiles // 2
    base = 7 * bucket - 1
    far = read(base + reach)
    counts = [read(base + (k if way == 0 else tiles - k)) for k in range(1, reach)]
    counts.append((far + 1) >> 1 if way == 0 else far >> 1)
    beyond = [0]
    for count in reversed(counts):
        beyond.append(beyond[-1] + count)
    return [None] + beyond[::-1]


def split(value, size):
    if size & (size - 1) == 0:
        return value >> (size.bit_length() - 1), value & (size - 1)
    return lax.div(value, size), lax.rem(value, size)


def sort_pairs(tiles, bands, bucket, blocks_owned, band, tile, live, atm):
    pairs = atm.shape[1]
    reach = tiles // 2
    order = ring_order(tiles)
    spots = [order.index(k) for k in range(tiles)]
    here = chosen(spots, tile)
    wide = (pairs, pairs)

    def across(value):
        return jnp.broadcast_to(value, wide).T

    def least(value):
        return jnp.min(value, axis=0, keepdims=True)

    def most(value):
        return jnp.max(value, axis=0, keepdims=True)

    def count(mask):
        return jnp.sum(jnp.where(mask, 1, 0), axis=0, keepdims=True)

    def bucket_of(value):
        owner, block = split(value, blocks_owned)
        owner_band, owner_tile = split(owner, tiles)
        ahead = split(chosen(spots, owner_tile) - here + tiles, tiles)[1]
        return jnp.where(owner_band == band, ahead, jnp.where(owner_band > band, tiles, tiles + 1)), block

    row = lax.broadcasted_iota(jnp.int32, wide, 0)
    lane = lax.broadcasted_iota(jnp.int32, wide, 1)
    one_lane = lax.broadcasted_iota(jnp.int32, (1, pairs), 1)
    atm_c = across(atm)
    live_c = row < live
    same = (atm_c == atm) & live_c
    first = least(jnp.where(same, row, pairs))
    before = most(jnp.where(same & (row < lane), row, -1))
    fresh_c = (across(first) == row) & live_c
    b, _ = bucket_of(atm)
    b_c, block_c = bucket_of(atm_c)
    rank = count(fresh_c & (b_c == b) & (row < first))
    back = (b > reach) | ((b == reach) & ((rank & 1) == 1))
    region = jnp.where(b == 0, 4, jnp.where(b >= tiles, b - tiles + 2, jnp.where(back, 1, 0)))
    near = jnp.where(region == 0, reach - b, jnp.where(region == 1, b - reach, 0))
    shift = ((reach + 1) * (pairs + 1)).bit_length()
    key = (region << shift) + near * (pairs + 1) + first
    key_c = across(key)
    place = count(fresh_c & ((key_c >> shift) == region) & (key_c < key))
    ring = region < 2
    room = jnp.where(ring, 2 * bucket, bucket)
    base = jnp.where(ring, 2 * region, region + 2) * bucket
    fits = place < room
    slot = jnp.where((one_lane < live) & fits, base + place, pairs)
    overflow = jnp.max(jnp.where((one_lane < live) & jnp.logical_not(fits), 1, 0), axis=1, keepdims=True)
    travels_c = live_c & (b_c > 0) & (b_c < tiles)
    travelling = count(travels_c)
    earlier = count(travels_c & (row < lane))
    rank_of = jnp.where((one_lane < live) & ring, earlier, travelling + one_lane - earlier)
    rank_c = across(rank_of)
    overflow = jnp.maximum(overflow, jnp.where(travelling > pairs // 2, 1, 0))
    here_c = rank_c == lane
    pair_at = most(jnp.where(here_c, row, 0))
    before = most(jnp.where(row == before, rank_c, -1))
    before = most(jnp.where(here_c, across(before), -1))
    hit = across(slot) == lane
    last = most(jnp.where(hit, rank_c, 0))
    label = most(jnp.where(hit, block_c, -1))
    counts = count(fresh_c & (b_c == lane - (7 * bucket - 1)))
    kinds = [count(fresh_c & (b_c == k)) for k in (0, tiles, tiles + 1)]
    packed = overflow + sum(kind << (1 + 6 * i) for i, kind in enumerate(kinds))
    labels = jnp.where(one_lane < 7 * bucket, label, jnp.where(one_lane == pairs - 1, packed, counts))
    return before, last, pair_at, labels


def starts(reach, lag, reaches):
    first = [None] * (reach + 1)
    for u in range(reach - 1, -1, -1):
        begin = [0]
        for j in range(1, reach - u):
            after = begin[j - 1] + reaches[u + j - 1][j]
            begin.append(jnp.maximum(after, first[u + 1][j - 1] + lag))
        first[u] = begin
    end = jnp.int32(0)
    for j in range(reach):
        size = reaches[j][j + 1]
        end = jnp.where(size > 0, first[0][j] + size, end)
    return first[0], first[1], end


def stream_kernel(tiles, bands, bucket, blocks_owned, plans, group,
                  patch_ref, counts_ref, atm_ref, patches_hbm, numer_hbm,
                  pool_ref, beside_ref, own_ref, landing, flag_ref,
                  patches_ref, numer_ref, labels_ref, work_v, work_ref, load_sems, sums, side, stage, recv, table_ref, mark,
                  ring_send, ring_recv, beside_send, beside_recv, label_send, label_recv, local_sem):
    band, tile = lax.axis_index("band"), lax.axis_index("tile")
    reach = tiles // 2
    own_rows = 2 * bucket
    at = layout(bucket)
    steps = partners(tiles)
    pairs = numer_ref.shape[0]

    def numer_load(c):
        part = pl.ds(c * group, group)
        return pltpu.make_async_copy(numer_hbm.at[part], numer_ref.at[part], load_sems.at[c])

    patch_load = pltpu.make_async_copy(patches_hbm, patches_ref, load_sems.at[pairs // group])
    patch_load.start()
    for c in range(pairs // group):
        numer_load(c).start()
    barrier = pltpu.get_barrier_semaphore()
    for step in steps:
        pl.semaphore_signal(barrier, inc=1, device_id=(band, step(tile)), device_id_type=MESH)
    for j in range(1, bands):
        pl.semaphore_signal(barrier, inc=1, device_id=(lax.rem(band + j, bands), tile), device_id_type=MESH)
    before, last, pair_at, labels = sort_pairs(tiles, bands, bucket, blocks_owned, band, tile, counts_ref[0], atm_ref[...])
    labels_ref[...] = labels
    landing[tile] = labels
    work_v[0:1] = before
    work_v[1:2] = last
    work_v[2:3] = pair_at
    work_in = pltpu.make_async_copy(work_v, work_ref, local_sem)
    work_in.start()
    work_in.wait()
    patch_load.wait()
    for c in range(pairs // group):
        numer_load(c).wait()

    def multiply(c):
        for j in range(group):
            k = c * group + j
            g = work_ref[2, k]
            weight = (numer_ref[g].astype(jnp.float32) * SCALE).astype(jnp.bfloat16)
            part = jnp.dot(weight, patches_ref[patch_ref[g]], preferred_element_type=jnp.float32)
            before = work_ref[0, k]
            earlier = sums[jnp.maximum(before, 0)]
            sums[k] = part + jnp.where(before >= 0, earlier, 0.0)

    pl.loop(0, pairs // group // 2)(multiply)

    def total(slot):
        return sums[work_ref[1, slot]]

    targets = ((band, ring_tile(tiles, tile, 1)), (band, ring_tile(tiles, tile, -1)))
    is_edge = (band == 0) | (band == bands - 1)
    head = max(size * lag for size, _, lag in plans)
    for way in range(2):
        for s in range(head):
            pool_ref[way, s] = total(way * own_rows + s)
    pl.semaphore_wait(barrier, tiles + bands - 2)
    inside = [
        pltpu.make_async_remote_copy(
            src_ref=labels_ref, dst_ref=landing.at[tile],
            send_sem=label_send.at[k], recv_sem=label_recv.at[k],
            device_id=(band, step(tile)), device_id_type=MESH)
        for k, step in enumerate(steps)
    ]
    across = [
        pltpu.make_async_remote_copy(
            src_ref=mark, dst_ref=landing.at[tiles + band],
            send_sem=label_send.at[tiles - 2 + j], recv_sem=label_recv.at[tiles - 2 + j],
            device_id=(lax.rem(band + j, bands), tile), device_id_type=MESH)
        for j in range(1, bands)
    ]
    for copy in inside:
        copy.start()

    def hop(way, r, size, source):
        rows = pl.ds(r * size, size)
        return pltpu.make_async_remote_copy(
            src_ref=source, dst_ref=recv.at[way, rows],
            send_sem=ring_send.at[way, r], recv_sem=ring_recv.at[way, r],
            device_id=targets[way], device_id_type=MESH)

    def own_hop(way, r, size):
        return hop(way, r, size, pool_ref.at[way, pl.ds(r * size, size)])

    def later_hop(way, r, size):
        return hop(way, r, size, stage.at[way, pl.ds(r * size, size)])

    for edge in (True, False):
        size, rounds, lag = plans[0 if edge else 1]

        @pl.when(is_edge if edge else jnp.logical_not(is_edge))
        def _():
            for r in range(lag):
                for way in range(2):
                    own_hop(way, r, size).start()

    def beside(way, target_band):
        return pltpu.make_async_remote_copy(
            src_ref=side.at[way], dst_ref=beside_ref.at[way],
            send_sem=beside_send.at[way], recv_sem=beside_recv.at[way],
            device_id=(target_band, tile), device_id_type=MESH)

    upward, downward = beside(0, band + 1), beside(1, band - 1)
    pl.loop(pairs // group // 2, pairs // group)(multiply)
    for way in range(2):
        for s in range(bucket):
            side[way, s] = total(at["up"] + way * bucket + s)
    for way in range(2):
        for s in range(head, own_rows):
            pool_ref[way, s] = total(way * own_rows + s)
    for s in range(bucket):
        own_ref[s] = total(at["own"] + s)

    @pl.when(band < bands - 1)
    def _():
        upward.start()

    @pl.when(band > 0)
    def _():
        downward.start()

    for copy in inside:
        copy.wait()
    rows_in = pltpu.make_async_copy(landing.at[pl.ds(0, tiles)], table_ref.at[pl.ds(0, tiles)], local_sem)
    rows_in.start()
    rows_in.wait()

    upstream = [[ring_tile(tiles, tile, -u if way == 0 else u) for u in range(tiles)] for way in range(2)]
    reaches = [[reaching(tiles, bucket, way, lambda i, t=t: table_ref[t, 0, i]) for t in upstream[way]]
               for way in range(2)]
    lag_slots = jnp.where(is_edge, plans[0][0] * plans[0][2], plans[1][0] * plans[1][2])
    capacity = jnp.where(is_edge, plans[0][0] * plans[0][1], plans[1][0] * plans[1][1])
    worst = jnp.int32(0)
    flag = jnp.int32(0)
    begins = []
    for way in range(2):
        for v in range(tiles):
            ahead, behind, end = starts(reach, lag_slots, [reaches[way][(v + u) % tiles] for u in range(reach)])
            worst = jnp.maximum(worst, end)
            if v == 0:
                begins.append(ahead)
    arrivals = []
    for way in range(2):
        ahead, _, _ = starts(reach, lag_slots, [reaches[way][(1 + u) % tiles] for u in range(reach)])
        arrivals.append(ahead)
    for t in range(tiles):
        flag = jnp.maximum(flag, table_ref[t, 0, LANES - 1] & 1)
    flag = jnp.where(worst > capacity, 1, flag)
    lane = lax.broadcasted_iota(jnp.int32, (1, LANES), 1)
    row = landing[tile]
    mark[...] = jnp.where(lane == LANES - 1, row - (row & 1) + flag, row)
    plan = jnp.zeros((1, LANES), jnp.int32)
    for way in range(2):
        for j in range(reach):
            plan = jnp.where(lane == way * reach + j, arrivals[way][j], plan)
    landing[tiles + bands] = plan

    for edge in (True, False):
        size, rounds, lag = plans[0 if edge else 1]
        last_row = own_rows + size * rounds - 1

        @pl.when(is_edge if edge else jnp.logical_not(is_edge))
        def _():
            def keep(way, r):
                later_hop(way, r, size).wait_recv()
                pool_ref[way, pl.ds(own_rows + r * size, size)] = recv[way, pl.ds(r * size, size)]

            def gather(way, r):
                begin, arrived = begins[way], arrivals[way]
                for s in range(size):
                    p = r * size + s
                    row = jnp.minimum(p, own_rows - 1)
                    for j in range(1, reach):
                        row = jnp.where(p >= begin[j], p + (own_rows + arrived[j - 1] - begin[j]), row)
                    row = jnp.clip(row, 0, last_row)
                    stage[way, p] = pool_ref[way, row]

            def one_round(r):
                for way in range(2):
                    keep(way, r - lag)
                    gather(way, r)
                    later_hop(way, r, size).start()

            one_round(lag)
            for copy in across:
                copy.start()

            @pl.loop(lag + 1, rounds)
            def _(r):
                one_round(r)

    for copy in across:
        copy.wait()
    rows_over = pltpu.make_async_copy(landing.at[pl.ds(tiles, bands)], table_ref.at[pl.ds(tiles, bands)], local_sem)
    rows_over.start()
    rows_over.wait()
    for j in range(1, bands):
        flag = jnp.maximum(flag, table_ref[tiles + lax.rem(band + j, bands), 0, LANES - 1] & 1)
    flag_ref[0, 0] = flag

    @pl.when(band < bands - 1)
    def _():
        upward.wait_send()
        downward.wait_recv()

    @pl.when(band > 0)
    def _():
        downward.wait_send()
        upward.wait_recv()

    for edge in (True, False):
        size, rounds, lag = plans[0 if edge else 1]

        @pl.when(is_edge if edge else jnp.logical_not(is_edge))
        def _():
            @pl.loop(0, rounds - lag)
            def _(r):
                for way in range(2):
                    later_hop(way, r, size).wait_send()

            @pl.loop(rounds - lag, rounds)
            def _(r):
                for way in range(2):
                    later_hop(way, r, size).wait()
                    pool_ref[way, pl.ds(own_rows + r * size, size)] = recv[way, pl.ds(r * size, size)]


def take_kernel(tiles, bands, bucket, table_ref, own_ref, pool_ref, beside_ref, out_ref):
    band, tile = lax.axis_index("band"), lax.axis_index("tile")
    reach = tiles // 2
    own_rows = 2 * bucket
    at = layout(bucket)
    out_ref[...] = jnp.zeros_like(out_ref)

    def how_many(lane, kind):
        return (lane >> (1 + 6 * kind)) & 63

    def add(low, high, label_of, block_of):
        fours = (high - low) >> 2

        @pl.loop(0, fours)
        def _(k):
            at_once = [low + 4 * k + j for j in range(4)]
            labels = [label_of(i) for i in at_once]
            sums = [out_ref[label] + block_of(i) for label, i in zip(labels, at_once)]
            for label, total in zip(labels, sums):
                out_ref[label] = total

        @pl.loop(low + 4 * fours, high)
        def _(i):
            out_ref[label_of(i)] += block_of(i)

    add(0, how_many(table_ref[tile, 0, LANES - 1], 0),
        lambda i: table_ref[tile, 0, at["own"] + i], lambda i: own_ref[i])
    for way in range(2):
        other = tiles + jnp.clip(band - 1 if way == 0 else band + 1, 0, bands - 1)
        valid = (band > 0) if way == 0 else (band < bands - 1)
        add(0, jnp.where(valid, how_many(table_ref[other, 0, LANES - 1], 1 + way), 0),
            lambda i: table_ref[other, 0, at["up"] + way * bucket + i], lambda i: beside_ref[way, i])

    for way in range(2):
        for distance in range(1, reach + 1):
            source = ring_tile(tiles, tile, -distance if way == 0 else distance)
            reaches = reaching(tiles, bucket, way, lambda i: table_ref[source, 0, i])
            start = own_rows + table_ref[tiles + bands, 0, way * reach + distance - 1]
            add(reaches[distance + 1], reaches[distance],
                lambda i: table_ref[source, 0, way * own_rows + i], lambda i: pool_ref[way, start + i])


def adaptive(tiles, bands, patches, pair_patch, pair_atm, numerators, counts):
    pairs, patch_rows, cell_rows = numerators.shape
    flux = patches.shape[1]
    blocks_owned = CELLS_DEV // cell_rows
    bucket = pairs // 8
    reach = tiles // 2
    group = 16
    plans = ((5, 4 * reach, 4), (3, 4 * reach, 3))
    slots = max(size * rounds for size, rounds, _ in plans)
    most = max(rounds for _, rounds, _ in plans)
    smem = pl.BlockSpec(memory_space=pltpu.SMEM)
    vmem = pl.BlockSpec(memory_space=pltpu.VMEM)
    hbm = pl.BlockSpec(memory_space=pltpu.HBM)
    block = (cell_rows, flux)
    f32 = jnp.float32
    numerators = jnp.transpose(numerators, (0, 2, 1))
    pool, beside, own, table, flag = pl.pallas_call(
        functools.partial(stream_kernel, tiles, bands, bucket, blocks_owned, plans, group),
        out_shape=(jax.ShapeDtypeStruct((2, 2 * bucket + slots) + block, f32),
                   jax.ShapeDtypeStruct((2, bucket) + block, f32),
                   jax.ShapeDtypeStruct((bucket,) + block, f32),
                   jax.ShapeDtypeStruct((tiles + bands + 1, 1, LANES), jnp.int32),
                   jax.ShapeDtypeStruct((1, LANES), jnp.int32)),
        in_specs=[smem, smem, vmem, hbm, hbm],
        out_specs=(vmem, vmem, vmem, vmem, smem),
        scratch_shapes=[
            pltpu.VMEM((patches.shape[0] // patch_rows, patch_rows, flux), patches.dtype),
            pltpu.VMEM(numerators.shape, numerators.dtype),
            pltpu.VMEM((1, LANES), jnp.int32),
            pltpu.VMEM((3, pairs), jnp.int32),
            pltpu.SMEM((3, pairs), jnp.int32),
            pltpu.SemaphoreType.DMA((pairs // group + 1,)),
            pltpu.VMEM((pairs,) + block, f32),
            pltpu.VMEM((2, bucket) + block, f32),
            pltpu.VMEM((2, slots) + block, f32),
            pltpu.VMEM((2, slots) + block, f32),
            pltpu.SMEM((tiles + bands, 1, LANES), jnp.int32),
            pltpu.VMEM((1, LANES), jnp.int32),
            pltpu.SemaphoreType.DMA((2, most)),
            pltpu.SemaphoreType.DMA((2, most)),
            pltpu.SemaphoreType.DMA((2,)),
            pltpu.SemaphoreType.DMA((2,)),
            pltpu.SemaphoreType.DMA((tiles + bands - 2,)),
            pltpu.SemaphoreType.DMA((tiles + bands - 2,)),
            pltpu.SemaphoreType.DMA,
        ],
        compiler_params=pltpu.CompilerParams(collective_id=1, has_side_effects=True, vmem_limit_bytes=STREAM_LIMIT),
        name="stream",
    )(pair_patch, counts, pair_atm.reshape(1, pairs), patches.reshape(-1, patch_rows, flux), numerators)

    def take(patches, pair_patch, pair_atm, numerators, counts, table, own, pool, beside):
        out = pl.pallas_call(
            functools.partial(take_kernel, tiles, bands, bucket),
            out_shape=jax.ShapeDtypeStruct((blocks_owned,) + block, f32),
            in_specs=[smem, vmem, vmem, vmem],
            out_specs=vmem,
            compiler_params=pltpu.CompilerParams(vmem_limit_bytes=VMEM_LIMIT),
            name="take",
        )(table, own, pool, beside)
        return out.reshape(blocks_owned * cell_rows, flux)

    def padded(patches, pair_patch, pair_atm, numerators, counts, table, own, pool, beside):
        return per_device(tiles, bands, patches, pair_patch, pair_atm, numerators, counts)

    return lax.cond(flag[0, 0] > 0, padded, take, patches, pair_patch, pair_atm, numerators, counts,
                    table, own, pool, beside)


def solution(mesh):
    spec = P(("band", "tile"))
    placed = (
        P(("band", "tile"), None),
        spec,
        spec,
        P(("band", "tile"), None, None),
        spec,
    )
    body = functools.partial(adaptive, mesh.shape["tile"], mesh.shape["band"])
    return jax.shard_map(body, mesh=mesh, in_specs=placed, out_specs=P(("band", "tile"), None), check_vma=False)
```

```python
import functools

import jax
import jax.numpy as jnp
from jax import lax
from jax.experimental import pallas as pl
from jax.experimental.pallas import tpu as pltpu
from jax.sharding import PartitionSpec as P

CELLS_DEV = 4096
SCALE = 2.0 ** (-27)
MESH = pl.DeviceIdType.MESH
LANES = 128
VMEM_LIMIT = 20 * 2 ** 20
STREAM_LIMIT = 24 * 2 ** 20
PADDED_LIMIT = 63 * 2 ** 20


def partners(count):
    if count & (count - 1) == 0:
        return [lambda me, k=k: me ^ k for k in range(count - 1, 0, -1)]
    return [lambda me, k=k: lax.rem(me + k, count) for k in range(1, count)]


def pack_kernel(tiles, bucket, blocks_owned, chunk,
                patch_ref, atm_ref, counts_ref, patches_hbm, numer_hbm,
                send_ref, labels_ref,
                patches_v, numer_v, table, used, patch_sem, numer_sems):
    pairs = numer_v.shape[0]
    patch_rows = numer_v.shape[2]
    chunks = pairs // chunk
    buckets = tiles + 2
    patch_copy = pltpu.make_async_copy(patches_hbm, patches_v, patch_sem)
    patch_copy.start()
    copies = []
    for c in range(chunks):
        part = pl.ds(c * chunk, chunk)
        copy = pltpu.make_async_copy(numer_hbm.at[part], numer_v.at[part], numer_sems.at[c])
        copy.start()
        copies.append(copy)
    band = lax.axis_index("band")
    live = counts_ref[0]

    for b in range(buckets):
        used[b] = 0

        @pl.loop(0, blocks_owned, unroll=16)
        def _(i):
            table[b * blocks_owned + i] = -1

        for s in range(bucket):
            labels_ref[b, 0, s] = -1
    patch_copy.wait()
    for c in range(chunks):
        copies[c].wait()

        @pl.when(c * chunk < live)
        def _():
            for j in range(chunk):
                g = c * chunk + j
                is_live = g < live
                atm = atm_ref[g]
                owner = lax.div(atm, blocks_owned)
                block = lax.rem(atm, blocks_owned)
                owner_band = lax.div(owner, tiles)
                owner_tile = lax.rem(owner, tiles)
                b = jnp.where(owner_band == band, owner_tile,
                              jnp.where(owner_band > band, tiles, tiles + 1))
                entry = b * blocks_owned + block
                known = table[entry]
                fresh = known < 0
                new = used[b]
                rank = jnp.where(fresh, new, known)

                @pl.when(is_live)
                def _():
                    table[entry] = rank
                    used[b] = jnp.where(fresh, new + 1, new)
                    labels_ref[b, 0, rank] = block

                slot = jnp.where(is_live, b * bucket + rank, buckets * bucket)
                rows = pl.multiple_of(patch_ref[g] * patch_rows, patch_rows)
                weight = (numer_v[g].astype(jnp.float32) * SCALE).astype(jnp.bfloat16)
                part = jnp.dot(weight, patches_v[pl.ds(rows, patch_rows), :],
                               preferred_element_type=jnp.float32)
                before = send_ref[slot]
                send_ref[slot] = jnp.where(fresh, part, before + part)


def send_kernel(tiles, bands, bucket, send_ref, labels_ref, recv_ref, recv_labels_ref,
                data_send, data_recv, label_send, label_recv):
    band, tile = lax.axis_index("band"), lax.axis_index("tile")
    barrier = pltpu.get_barrier_semaphore()
    steps = partners(tiles)
    for step in steps:
        pl.semaphore_signal(barrier, inc=1, device_id=(band, step(tile)), device_id_type=MESH)

    @pl.when(band < bands - 1)
    def _():
        pl.semaphore_signal(barrier, inc=1, device_id=(band + 1, tile), device_id_type=MESH)

    @pl.when(band > 0)
    def _():
        pl.semaphore_signal(barrier, inc=1, device_id=(band - 1, tile), device_id_type=MESH)

    neighbours = jnp.where(band < bands - 1, 1, 0) + jnp.where(band > 0, 1, 0)
    pl.semaphore_wait(barrier, tiles - 1 + neighbours)

    def pair(source, place, device, sem):
        rows = pl.ds(source * bucket, bucket)
        landing = pl.ds(place * bucket, bucket)
        return (
            pltpu.make_async_remote_copy(
                src_ref=labels_ref.at[source], dst_ref=recv_labels_ref.at[place],
                send_sem=label_send.at[sem], recv_sem=label_recv.at[sem],
                device_id=device, device_id_type=MESH),
            pltpu.make_async_remote_copy(
                src_ref=send_ref.at[rows], dst_ref=recv_ref.at[landing],
                send_sem=data_send.at[sem], recv_sem=data_recv.at[sem],
                device_id=device, device_id_type=MESH),
        )

    inside = [pair(step(tile), tile, (band, step(tile)), k) for k, step in enumerate(steps)]
    upward = pair(tiles, tiles, (band + 1, tile), tiles - 1)
    downward = pair(tiles + 1, tiles + 1, (band - 1, tile), tiles)
    for copies in inside[:2]:
        for copy in copies:
            copy.start()

    @pl.when(band < bands - 1)
    def _():
        for copy in upward:
            copy.start()

    @pl.when(band > 0)
    def _():
        for copy in downward:
            copy.start()

    for copies in inside[2:]:
        for copy in copies:
            copy.start()
    for copies in inside:
        for copy in copies:
            copy.wait()

    @pl.when(band < bands - 1)
    def _():
        for up, down in zip(upward, downward):
            up.wait_send()
            down.wait_recv()

    @pl.when(band > 0)
    def _():
        for up, down in zip(upward, downward):
            down.wait_send()
            up.wait_recv()


def add_kernel(tiles, bands, bucket, labels_ref, recv_labels_ref, send_hbm, recv_hbm, out_ref,
               landed, sems):
    band, tile = lax.axis_index("band"), lax.axis_index("tile")
    buckets = tiles + 2

    def copy_of(b, ref):
        rows = pl.ds(b * bucket, bucket)
        return pltpu.make_async_copy(ref.at[rows], landed.at[rows], sems.at[b])

    for b in range(buckets):
        if b < tiles:
            @pl.when(tile == b)
            def _():
                copy_of(b, send_hbm).start()

            @pl.when(tile != b)
            def _():
                copy_of(b, recv_hbm).start()
        else:
            copy_of(b, recv_hbm).start()
    out_ref[...] = jnp.zeros_like(out_ref)
    for b in range(buckets):
        copy_of(b, recv_hbm).wait()
        if b == tiles:
            valid = band > 0
        elif b == tiles + 1:
            valid = band < bands - 1
        else:
            valid = True
        for s in range(bucket):
            label = recv_labels_ref[b, 0, s]
            if b < tiles:
                label = jnp.where(tile == b, labels_ref[b, 0, s], label)

            @pl.when((label >= 0) & valid)
            def _():
                out_ref[label] += landed[b * bucket + s]


def per_device(tiles, bands, patches, pair_patch, pair_atm, numerators, counts):
    pairs, cell_rows, patch_rows = numerators.shape
    flux = patches.shape[1]
    blocks_owned = CELLS_DEV // cell_rows
    bucket = pairs // 8
    buckets = tiles + 2
    chunk = 16
    smem = pl.BlockSpec(memory_space=pltpu.SMEM)
    vmem = pl.BlockSpec(memory_space=pltpu.VMEM)
    anywhere = pl.BlockSpec(memory_space=pl.ANY)
    labels_shape = jax.ShapeDtypeStruct((buckets, 1, LANES), jnp.int32)
    recv_shape = jax.ShapeDtypeStruct((buckets * bucket, cell_rows, flux), jnp.float32)
    send, labels = pl.pallas_call(
        functools.partial(pack_kernel, tiles, bucket, blocks_owned, chunk),
        out_shape=(jax.ShapeDtypeStruct((buckets * bucket + 1, cell_rows, flux), jnp.float32), labels_shape),
        in_specs=[smem, smem, smem, anywhere, anywhere],
        out_specs=(vmem, smem),
        scratch_shapes=[
            pltpu.VMEM(patches.shape, patches.dtype),
            pltpu.VMEM((pairs, cell_rows, patch_rows), jnp.int32),
            pltpu.SMEM((buckets * blocks_owned,), jnp.int32),
            pltpu.SMEM((buckets,), jnp.int32),
            pltpu.SemaphoreType.DMA,
            pltpu.SemaphoreType.DMA((pairs // chunk,)),
        ],
        compiler_params=pltpu.CompilerParams(vmem_limit_bytes=PADDED_LIMIT),
        name="pack",
    )(pair_patch, pair_atm, counts, patches, numerators)
    recv, recv_labels = pl.pallas_call(
        functools.partial(send_kernel, tiles, bands, bucket),
        out_shape=(recv_shape, labels_shape),
        in_specs=[anywhere, anywhere],
        out_specs=(anywhere, anywhere),
        scratch_shapes=[pltpu.SemaphoreType.DMA((tiles + 1,))] * 4,
        compiler_params=pltpu.CompilerParams(collective_id=0, has_side_effects=True, vmem_limit_bytes=VMEM_LIMIT),
        name="exchange",
    )(send, labels)
    out = pl.pallas_call(
        functools.partial(add_kernel, tiles, bands, bucket),
        out_shape=jax.ShapeDtypeStruct((blocks_owned, cell_rows, flux), jnp.float32),
        in_specs=[smem, smem, anywhere, anywhere],
        out_specs=vmem,
        scratch_shapes=[
            pltpu.VMEM(recv_shape.shape, jnp.float32),
            pltpu.SemaphoreType.DMA((buckets,)),
        ],
        compiler_params=pltpu.CompilerParams(vmem_limit_bytes=VMEM_LIMIT),
        name="add",
    )(labels, recv_labels, send, recv)
    return out.reshape(blocks_owned * cell_rows, flux)


def ring_order(tiles):
    wide = tiles // 4
    if wide * 4 != tiles or wide % 2:
        return list(range(tiles))
    order = list(range(wide))
    for step, column in enumerate(reversed(range(wide))):
        rows = range(1, 4) if step % 2 == 0 else range(3, 0, -1)
        order += [row * wide + column for row in rows]
    return order


def chosen(values, index):
    picked = values[0]
    for k in range(1, len(values)):
        picked = jnp.where(index == k, values[k], picked)
    return picked


def ring_tile(tiles, tile, steps):
    order = ring_order(tiles)
    position = chosen([order.index(k) for k in range(tiles)], tile)
    return chosen(order, lax.rem(position + steps + tiles, tiles))


def layout(bucket):
    return dict(up=4 * bucket, down=5 * bucket, own=6 * bucket, end=7 * bucket)


def reaching(tiles, bucket, way, read):
    reach = tiles // 2
    base = 7 * bucket - 1
    far = read(base + reach)
    counts = [read(base + (k if way == 0 else tiles - k)) for k in range(1, reach)]
    counts.append((far + 1) >> 1 if way == 0 else far >> 1)
    beyond = [0]
    for count in reversed(counts):
        beyond.append(beyond[-1] + count)
    return [None] + beyond[::-1]


def split(value, size):
    if size & (size - 1) == 0:
        return value >> (size.bit_length() - 1), value & (size - 1)
    return lax.div(value, size), lax.rem(value, size)


def sort_pairs(tiles, bands, bucket, blocks_owned, band, tile, live, atm):
    pairs = atm.shape[1]
    reach = tiles // 2
    order = ring_order(tiles)
    spots = [order.index(k) for k in range(tiles)]
    here = chosen(spots, tile)
    wide = (pairs, pairs)

    def across(value):
        return jnp.broadcast_to(value, wide).T

    def least(value):
        return jnp.min(value, axis=0, keepdims=True)

    def most(value):
        return jnp.max(value, axis=0, keepdims=True)

    def count(mask):
        return jnp.sum(jnp.where(mask, 1, 0), axis=0, keepdims=True)

    def bucket_of(value):
        owner, block = split(value, blocks_owned)
        owner_band, owner_tile = split(owner, tiles)
        ahead = split(chosen(spots, owner_tile) - here + tiles, tiles)[1]
        return jnp.where(owner_band == band, ahead, jnp.where(owner_band > band, tiles, tiles + 1)), block

    row = lax.broadcasted_iota(jnp.int32, wide, 0)
    lane = lax.broadcasted_iota(jnp.int32, wide, 1)
    one_lane = lax.broadcasted_iota(jnp.int32, (1, pairs), 1)
    atm_c = across(atm)
    live_c = row < live
    same = (atm_c == atm) & live_c
    first = least(jnp.where(same, row, pairs))
    before = most(jnp.where(same & (row < lane), row, -1))
    fresh_c = (across(first) == row) & live_c
    b, _ = bucket_of(atm)
    b_c, block_c = bucket_of(atm_c)
    rank = count(fresh_c & (b_c == b) & (row < first))
    back = (b > reach) | ((b == reach) & ((rank & 1) == 1))
    region = jnp.where(b == 0, 4, jnp.where(b >= tiles, b - tiles + 2, jnp.where(back, 1, 0)))
    near = jnp.where(region == 0, reach - b, jnp.where(region == 1, b - reach, 0))
    shift = ((reach + 1) * (pairs + 1)).bit_length()
    key = (region << shift) + near * (pairs + 1) + first
    key_c = across(key)
    place = count(fresh_c & ((key_c >> shift) == region) & (key_c < key))
    ring = region < 2
    room = jnp.where(ring, 2 * bucket, bucket)
    base = jnp.where(ring, 2 * region, region + 2) * bucket
    fits = place < room
    slot = jnp.where((one_lane < live) & fits, base + place, pairs)
    overflow = jnp.max(jnp.where((one_lane < live) & jnp.logical_not(fits), 1, 0), axis=1, keepdims=True)
    travels_c = live_c & (b_c > 0) & (b_c < tiles)
    travelling = count(travels_c)
    earlier = count(travels_c & (row < lane))
    rank_of = jnp.where((one_lane < live) & ring, earlier, travelling + one_lane - earlier)
    rank_c = across(rank_of)
    overflow = jnp.maximum(overflow, jnp.where(travelling > pairs // 2, 1, 0))
    here_c = rank_c == lane
    pair_at = most(jnp.where(here_c, row, 0))
    before = most(jnp.where(row == before, rank_c, -1))
    before = most(jnp.where(here_c, across(before), -1))
    hit = across(slot) == lane
    last = most(jnp.where(hit, rank_c, 0))
    label = most(jnp.where(hit, block_c, -1))
    counts = count(fresh_c & (b_c == lane - (7 * bucket - 1)))
    kinds = [count(fresh_c & (b_c == k)) for k in (0, tiles, tiles + 1)]
    packed = overflow + sum(kind << (1 + 6 * i) for i, kind in enumerate(kinds))
    labels = jnp.where(one_lane < 7 * bucket, label, jnp.where(one_lane == pairs - 1, packed, counts))
    return before, last, pair_at, labels


def starts(reach, lag, reaches):
    first = [None] * (reach + 1)
    for u in range(reach - 1, -1, -1):
        begin = [0]
        for j in range(1, reach - u):
            after = begin[j - 1] + reaches[u + j - 1][j]
            begin.append(jnp.maximum(after, first[u + 1][j - 1] + lag))
        first[u] = begin
    end = jnp.int32(0)
    for j in range(reach):
        size = reaches[j][j + 1]
        end = jnp.where(size > 0, first[0][j] + size, end)
    return first[0], first[1], end


def stream_kernel(tiles, bands, bucket, blocks_owned, plans, group,
                  patch_ref, counts_ref, atm_ref, patches_hbm, numer_hbm,
                  pool_ref, beside_ref, own_ref, landing, flag_ref,
                  patches_ref, numer_ref, labels_ref, work_v, work_ref, load_sems, sums, side, stage, recv, table_ref, mark,
                  ring_send, ring_recv, beside_send, beside_recv, label_send, label_recv, local_sem):
    band, tile = lax.axis_index("band"), lax.axis_index("tile")
    reach = tiles // 2
    own_rows = 2 * bucket
    at = layout(bucket)
    steps = partners(tiles)
    pairs = numer_ref.shape[0]

    def numer_load(c):
        part = pl.ds(c * group, group)
        return pltpu.make_async_copy(numer_hbm.at[part], numer_ref.at[part], load_sems.at[c])

    patch_load = pltpu.make_async_copy(patches_hbm, patches_ref, load_sems.at[pairs // group])
    patch_load.start()
    for c in range(pairs // group):
        numer_load(c).start()
    barrier = pltpu.get_barrier_semaphore()
    for step in steps:
        pl.semaphore_signal(barrier, inc=1, device_id=(band, step(tile)), device_id_type=MESH)
    for j in range(1, bands):
        pl.semaphore_signal(barrier, inc=1, device_id=(lax.rem(band + j, bands), tile), device_id_type=MESH)
    before, last, pair_at, labels = sort_pairs(tiles, bands, bucket, blocks_owned, band, tile, counts_ref[0], atm_ref[...])
    labels_ref[...] = labels
    landing[tile] = labels
    work_v[0:1] = before
    work_v[1:2] = last
    work_v[2:3] = pair_at
    work_in = pltpu.make_async_copy(work_v, work_ref, local_sem)
    work_in.start()
    work_in.wait()
    patch_load.wait()
    for c in range(pairs // group):
        numer_load(c).wait()

    def multiply(c):
        for j in range(group):
            k = c * group + j
            g = work_ref[2, k]
            weight = (numer_ref[g].astype(jnp.float32) * SCALE).astype(jnp.bfloat16)
            part = jnp.dot(weight, patches_ref[patch_ref[g]], preferred_element_type=jnp.float32)
            before = work_ref[0, k]
            earlier = sums[jnp.maximum(before, 0)]
            sums[k] = part + jnp.where(before >= 0, earlier, 0.0)

    pl.loop(0, pairs // group // 2)(multiply)

    def total(slot):
        return sums[work_ref[1, slot]]

    targets = ((band, ring_tile(tiles, tile, 1)), (band, ring_tile(tiles, tile, -1)))
    is_edge = (band == 0) | (band == bands - 1)
    head = max(size * lag for size, _, lag in plans)
    for way in range(2):
        for s in range(head):
            pool_ref[way, s] = total(way * own_rows + s)
    pl.semaphore_wait(barrier, tiles + bands - 2)
    inside = [
        pltpu.make_async_remote_copy(
            src_ref=labels_ref, dst_ref=landing.at[tile],
            send_sem=label_send.at[k], recv_sem=label_recv.at[k],
            device_id=(band, step(tile)), device_id_type=MESH)
        for k, step in enumerate(steps)
    ]
    across = [
        pltpu.make_async_remote_copy(
            src_ref=mark, dst_ref=landing.at[tiles + band],
            send_sem=label_send.at[tiles - 2 + j], recv_sem=label_recv.at[tiles - 2 + j],
            device_id=(lax.rem(band + j, bands), tile), device_id_type=MESH)
        for j in range(1, bands)
    ]
    for copy in inside:
        copy.start()

    def hop(way, r, size, source):
        rows = pl.ds(r * size, size)
        return pltpu.make_async_remote_copy(
            src_ref=source, dst_ref=recv.at[way, rows],
            send_sem=ring_send.at[way, r], recv_sem=ring_recv.at[way, r],
            device_id=targets[way], device_id_type=MESH)

    def own_hop(way, r, size):
        return hop(way, r, size, pool_ref.at[way, pl.ds(r * size, size)])

    def later_hop(way, r, size):
        return hop(way, r, size, stage.at[way, pl.ds(r * size, size)])

    for edge in (True, False):
        size, rounds, lag = plans[0 if edge else 1]

        @pl.when(is_edge if edge else jnp.logical_not(is_edge))
        def _():
            for r in range(lag):
                for way in range(2):
                    own_hop(way, r, size).start()

    def beside(way, target_band):
        return pltpu.make_async_remote_copy(
            src_ref=side.at[way], dst_ref=beside_ref.at[way],
            send_sem=beside_send.at[way], recv_sem=beside_recv.at[way],
            device_id=(target_band, tile), device_id_type=MESH)

    upward, downward = beside(0, band + 1), beside(1, band - 1)
    pl.loop(pairs // group // 2, pairs // group)(multiply)
    for way in range(2):
        for s in range(bucket):
            side[way, s] = total(at["up"] + way * bucket + s)
    for way in range(2):
        for s in range(head, own_rows):
            pool_ref[way, s] = total(way * own_rows + s)
    for s in range(bucket):
        own_ref[s] = total(at["own"] + s)

    @pl.when(band < bands - 1)
    def _():
        upward.start()

    @pl.when(band > 0)
    def _():
        downward.start()

    for copy in inside:
        copy.wait()
    rows_in = pltpu.make_async_copy(landing.at[pl.ds(0, tiles)], table_ref.at[pl.ds(0, tiles)], local_sem)
    rows_in.start()
    rows_in.wait()

    upstream = [[ring_tile(tiles, tile, -u if way == 0 else u) for u in range(tiles)] for way in range(2)]
    reaches = [[reaching(tiles, bucket, way, lambda i, t=t: table_ref[t, 0, i]) for t in upstream[way]]
               for way in range(2)]
    lag_slots = jnp.where(is_edge, plans[0][0] * plans[0][2], plans[1][0] * plans[1][2])
    capacity = jnp.where(is_edge, plans[0][0] * plans[0][1], plans[1][0] * plans[1][1])
    worst = jnp.int32(0)
    flag = jnp.int32(0)
    begins = []
    for way in range(2):
        for v in range(tiles):
            ahead, behind, end = starts(reach, lag_slots, [reaches[way][(v + u) % tiles] for u in range(reach)])
            worst = jnp.maximum(worst, end)
            if v == 0:
                begins.append(ahead)
    arrivals = []
    for way in range(2):
        ahead, _, _ = starts(reach, lag_slots, [reaches[way][(1 + u) % tiles] for u in range(reach)])
        arrivals.append(ahead)
    for t in range(tiles):
        flag = jnp.maximum(flag, table_ref[t, 0, LANES - 1] & 1)
    flag = jnp.where(worst > capacity, 1, flag)
    lane = lax.broadcasted_iota(jnp.int32, (1, LANES), 1)
    row = landing[tile]
    mark[...] = jnp.where(lane == LANES - 1, row - (row & 1) + flag, row)
    plan = jnp.zeros((1, LANES), jnp.int32)
    for way in range(2):
        for j in range(reach):
            plan = jnp.where(lane == way * reach + j, arrivals[way][j], plan)
    landing[tiles + bands] = plan

    for edge in (True, False):
        size, rounds, lag = plans[0 if edge else 1]
        last_row = own_rows + size * rounds - 1

        @pl.when(is_edge if edge else jnp.logical_not(is_edge))
        def _():
            def keep(way, r):
                later_hop(way, r, size).wait_recv()
                pool_ref[way, pl.ds(own_rows + r * size, size)] = recv[way, pl.ds(r * size, size)]

            def gather(way, r):
                begin, arrived = begins[way], arrivals[way]
                for s in range(size):
                    p = r * size + s
                    row = jnp.minimum(p, own_rows - 1)
                    for j in range(1, reach):
                        row = jnp.where(p >= begin[j], p + (own_rows + arrived[j - 1] - begin[j]), row)
                    row = jnp.clip(row, 0, last_row)
                    stage[way, p] = pool_ref[way, row]

            def one_round(r):
                for way in range(2):
                    keep(way, r - lag)
                    gather(way, r)
                    later_hop(way, r, size).start()

            one_round(lag)
            for copy in across:
                copy.start()

            @pl.loop(lag + 1, rounds)
            def _(r):
                one_round(r)

    for copy in across:
        copy.wait()
    rows_over = pltpu.make_async_copy(landing.at[pl.ds(tiles, bands)], table_ref.at[pl.ds(tiles, bands)], local_sem)
    rows_over.start()
    rows_over.wait()
    for j in range(1, bands):
        flag = jnp.maximum(flag, table_ref[tiles + lax.rem(band + j, bands), 0, LANES - 1] & 1)
    flag_ref[0, 0] = flag

    @pl.when(band < bands - 1)
    def _():
        upward.wait_send()
        downward.wait_recv()

    @pl.when(band > 0)
    def _():
        downward.wait_send()
        upward.wait_recv()

    for edge in (True, False):
        size, rounds, lag = plans[0 if edge else 1]

        @pl.when(is_edge if edge else jnp.logical_not(is_edge))
        def _():
            @pl.loop(0, rounds - lag)
            def _(r):
                for way in range(2):
                    later_hop(way, r, size).wait_send()

            @pl.loop(rounds - lag, rounds)
            def _(r):
                for way in range(2):
                    later_hop(way, r, size).wait()
                    pool_ref[way, pl.ds(own_rows + r * size, size)] = recv[way, pl.ds(r * size, size)]


def take_kernel(tiles, bands, bucket, table_ref, own_ref, pool_ref, beside_ref, out_ref):
    band, tile = lax.axis_index("band"), lax.axis_index("tile")
    reach = tiles // 2
    own_rows = 2 * bucket
    at = layout(bucket)
    out_ref[...] = jnp.zeros_like(out_ref)

    def how_many(lane, kind):
        return (lane >> (1 + 6 * kind)) & 63

    def add(low, high, label_of, block_of):
        fours = (high - low) >> 2

        @pl.loop(0, fours)
        def _(k):
            at_once = [low + 4 * k + j for j in range(4)]
            labels = [label_of(i) for i in at_once]
            sums = [out_ref[label] + block_of(i) for label, i in zip(labels, at_once)]
            for label, total in zip(labels, sums):
                out_ref[label] = total

        @pl.loop(low + 4 * fours, high)
        def _(i):
            out_ref[label_of(i)] += block_of(i)

    add(0, how_many(table_ref[tile, 0, LANES - 1], 0),
        lambda i: table_ref[tile, 0, at["own"] + i], lambda i: own_ref[i])
    for way in range(2):
        other = tiles + jnp.clip(band - 1 if way == 0 else band + 1, 0, bands - 1)
        valid = (band > 0) if way == 0 else (band < bands - 1)
        add(0, jnp.where(valid, how_many(table_ref[other, 0, LANES - 1], 1 + way), 0),
            lambda i: table_ref[other, 0, at["up"] + way * bucket + i], lambda i: beside_ref[way, i])

    for way in range(2):
        for distance in range(1, reach + 1):
            source = ring_tile(tiles, tile, -distance if way == 0 else distance)
            reaches = reaching(tiles, bucket, way, lambda i: table_ref[source, 0, i])
            start = own_rows + table_ref[tiles + bands, 0, way * reach + distance - 1]
            add(reaches[distance + 1], reaches[distance],
                lambda i: table_ref[source, 0, way * own_rows + i], lambda i: pool_ref[way, start + i])


def adaptive(tiles, bands, patches, pair_patch, pair_atm, numerators, counts):
    pairs, patch_rows, cell_rows = numerators.shape
    flux = patches.shape[1]
    blocks_owned = CELLS_DEV // cell_rows
    bucket = pairs // 8
    reach = tiles // 2
    group = 16
    plans = ((5, 4 * reach + 1, 4), (3, 4 * reach + 1, 3))
    slots = max(size * rounds for size, rounds, _ in plans)
    most = max(rounds for _, rounds, _ in plans)
    smem = pl.BlockSpec(memory_space=pltpu.SMEM)
    vmem = pl.BlockSpec(memory_space=pltpu.VMEM)
    hbm = pl.BlockSpec(memory_space=pltpu.HBM)
    block = (cell_rows, flux)
    f32 = jnp.float32
    numerators = jnp.transpose(numerators, (0, 2, 1))
    pool, beside, own, table, flag = pl.pallas_call(
        functools.partial(stream_kernel, tiles, bands, bucket, blocks_owned, plans, group),
        out_shape=(jax.ShapeDtypeStruct((2, 2 * bucket + slots) + block, f32),
                   jax.ShapeDtypeStruct((2, bucket) + block, f32),
                   jax.ShapeDtypeStruct((bucket,) + block, f32),
                   jax.ShapeDtypeStruct((tiles + bands + 1, 1, LANES), jnp.int32),
                   jax.ShapeDtypeStruct((1, LANES), jnp.int32)),
        in_specs=[smem, smem, vmem, hbm, hbm],
        out_specs=(vmem, vmem, vmem, vmem, smem),
        scratch_shapes=[
            pltpu.VMEM((patches.shape[0] // patch_rows, patch_rows, flux), patches.dtype),
            pltpu.VMEM(numerators.shape, numerators.dtype),
            pltpu.VMEM((1, LANES), jnp.int32),
            pltpu.VMEM((3, pairs), jnp.int32),
            pltpu.SMEM((3, pairs), jnp.int32),
            pltpu.SemaphoreType.DMA((pairs // group + 1,)),
            pltpu.VMEM((pairs,) + block, f32),
            pltpu.VMEM((2, bucket) + block, f32),
            pltpu.VMEM((2, slots) + block, f32),
            pltpu.VMEM((2, slots) + block, f32),
            pltpu.SMEM((tiles + bands, 1, LANES), jnp.int32),
            pltpu.VMEM((1, LANES), jnp.int32),
            pltpu.SemaphoreType.DMA((2, most)),
            pltpu.SemaphoreType.DMA((2, most)),
            pltpu.SemaphoreType.DMA((2,)),
            pltpu.SemaphoreType.DMA((2,)),
            pltpu.SemaphoreType.DMA((tiles + bands - 2,)),
            pltpu.SemaphoreType.DMA((tiles + bands - 2,)),
            pltpu.SemaphoreType.DMA,
        ],
        compiler_params=pltpu.CompilerParams(collective_id=1, has_side_effects=True, vmem_limit_bytes=STREAM_LIMIT),
        name="stream",
    )(pair_patch, counts, pair_atm.reshape(1, pairs), patches.reshape(-1, patch_rows, flux), numerators)

    def take(patches, pair_patch, pair_atm, numerators, counts, table, own, pool, beside):
        out = pl.pallas_call(
            functools.partial(take_kernel, tiles, bands, bucket),
            out_shape=jax.ShapeDtypeStruct((blocks_owned,) + block, f32),
            in_specs=[smem, vmem, vmem, vmem],
            out_specs=vmem,
            compiler_params=pltpu.CompilerParams(vmem_limit_bytes=VMEM_LIMIT),
            name="take",
        )(table, own, pool, beside)
        return out.reshape(blocks_owned * cell_rows, flux)

    def padded(patches, pair_patch, pair_atm, numerators, counts, table, own, pool, beside):
        return per_device(tiles, bands, patches, pair_patch, pair_atm, numerators, counts)

    return lax.cond(flag[0, 0] > 0, padded, take, patches, pair_patch, pair_atm, numerators, counts,
                    table, own, pool, beside)


def solution(mesh):
    spec = P(("band", "tile"))
    placed = (
        P(("band", "tile"), None),
        spec,
        spec,
        P(("band", "tile"), None, None),
        spec,
    )
    body = functools.partial(adaptive, mesh.shape["tile"], mesh.shape["band"])
    return jax.shard_map(body, mesh=mesh, in_specs=placed, out_specs=P(("band", "tile"), None), check_vma=False)
```

```python
import functools

import jax
import jax.numpy as jnp
from jax import lax
from jax.experimental import pallas as pl
from jax.experimental.pallas import tpu as pltpu
from jax.sharding import PartitionSpec as P

CELLS_DEV = 4096
SCALE = 2.0 ** (-27)
MESH = pl.DeviceIdType.MESH
LANES = 128
VMEM_LIMIT = 20 * 2 ** 20
STREAM_LIMIT = 24 * 2 ** 20
PADDED_LIMIT = 63 * 2 ** 20


def partners(count):
    if count & (count - 1) == 0:
        return [lambda me, k=k: me ^ k for k in range(count - 1, 0, -1)]
    return [lambda me, k=k: lax.rem(me + k, count) for k in range(1, count)]


def pack_kernel(tiles, bucket, blocks_owned, chunk,
                patch_ref, atm_ref, counts_ref, patches_hbm, numer_hbm,
                send_ref, labels_ref,
                patches_v, numer_v, table, used, patch_sem, numer_sems):
    pairs = numer_v.shape[0]
    patch_rows = numer_v.shape[2]
    chunks = pairs // chunk
    buckets = tiles + 2
    patch_copy = pltpu.make_async_copy(patches_hbm, patches_v, patch_sem)
    patch_copy.start()
    copies = []
    for c in range(chunks):
        part = pl.ds(c * chunk, chunk)
        copy = pltpu.make_async_copy(numer_hbm.at[part], numer_v.at[part], numer_sems.at[c])
        copy.start()
        copies.append(copy)
    band = lax.axis_index("band")
    live = counts_ref[0]

    for b in range(buckets):
        used[b] = 0

        @pl.loop(0, blocks_owned, unroll=16)
        def _(i):
            table[b * blocks_owned + i] = -1

        for s in range(bucket):
            labels_ref[b, 0, s] = -1
    patch_copy.wait()
    for c in range(chunks):
        copies[c].wait()

        @pl.when(c * chunk < live)
        def _():
            for j in range(chunk):
                g = c * chunk + j
                is_live = g < live
                atm = atm_ref[g]
                owner = lax.div(atm, blocks_owned)
                block = lax.rem(atm, blocks_owned)
                owner_band = lax.div(owner, tiles)
                owner_tile = lax.rem(owner, tiles)
                b = jnp.where(owner_band == band, owner_tile,
                              jnp.where(owner_band > band, tiles, tiles + 1))
                entry = b * blocks_owned + block
                known = table[entry]
                fresh = known < 0
                new = used[b]
                rank = jnp.where(fresh, new, known)

                @pl.when(is_live)
                def _():
                    table[entry] = rank
                    used[b] = jnp.where(fresh, new + 1, new)
                    labels_ref[b, 0, rank] = block

                slot = jnp.where(is_live, b * bucket + rank, buckets * bucket)
                rows = pl.multiple_of(patch_ref[g] * patch_rows, patch_rows)
                weight = (numer_v[g].astype(jnp.float32) * SCALE).astype(jnp.bfloat16)
                part = jnp.dot(weight, patches_v[pl.ds(rows, patch_rows), :],
                               preferred_element_type=jnp.float32)
                before = send_ref[slot]
                send_ref[slot] = jnp.where(fresh, part, before + part)


def send_kernel(tiles, bands, bucket, send_ref, labels_ref, recv_ref, recv_labels_ref,
                data_send, data_recv, label_send, label_recv):
    band, tile = lax.axis_index("band"), lax.axis_index("tile")
    barrier = pltpu.get_barrier_semaphore()
    steps = partners(tiles)
    for step in steps:
        pl.semaphore_signal(barrier, inc=1, device_id=(band, step(tile)), device_id_type=MESH)

    @pl.when(band < bands - 1)
    def _():
        pl.semaphore_signal(barrier, inc=1, device_id=(band + 1, tile), device_id_type=MESH)

    @pl.when(band > 0)
    def _():
        pl.semaphore_signal(barrier, inc=1, device_id=(band - 1, tile), device_id_type=MESH)

    neighbours = jnp.where(band < bands - 1, 1, 0) + jnp.where(band > 0, 1, 0)
    pl.semaphore_wait(barrier, tiles - 1 + neighbours)

    def pair(source, place, device, sem):
        rows = pl.ds(source * bucket, bucket)
        landing = pl.ds(place * bucket, bucket)
        return (
            pltpu.make_async_remote_copy(
                src_ref=labels_ref.at[source], dst_ref=recv_labels_ref.at[place],
                send_sem=label_send.at[sem], recv_sem=label_recv.at[sem],
                device_id=device, device_id_type=MESH),
            pltpu.make_async_remote_copy(
                src_ref=send_ref.at[rows], dst_ref=recv_ref.at[landing],
                send_sem=data_send.at[sem], recv_sem=data_recv.at[sem],
                device_id=device, device_id_type=MESH),
        )

    inside = [pair(step(tile), tile, (band, step(tile)), k) for k, step in enumerate(steps)]
    upward = pair(tiles, tiles, (band + 1, tile), tiles - 1)
    downward = pair(tiles + 1, tiles + 1, (band - 1, tile), tiles)
    for copies in inside[:2]:
        for copy in copies:
            copy.start()

    @pl.when(band < bands - 1)
    def _():
        for copy in upward:
            copy.start()

    @pl.when(band > 0)
    def _():
        for copy in downward:
            copy.start()

    for copies in inside[2:]:
        for copy in copies:
            copy.start()
    for copies in inside:
        for copy in copies:
            copy.wait()

    @pl.when(band < bands - 1)
    def _():
        for up, down in zip(upward, downward):
            up.wait_send()
            down.wait_recv()

    @pl.when(band > 0)
    def _():
        for up, down in zip(upward, downward):
            down.wait_send()
            up.wait_recv()


def add_kernel(tiles, bands, bucket, labels_ref, recv_labels_ref, send_hbm, recv_hbm, out_ref,
               landed, sems):
    band, tile = lax.axis_index("band"), lax.axis_index("tile")
    buckets = tiles + 2

    def copy_of(b, ref):
        rows = pl.ds(b * bucket, bucket)
        return pltpu.make_async_copy(ref.at[rows], landed.at[rows], sems.at[b])

    for b in range(buckets):
        if b < tiles:
            @pl.when(tile == b)
            def _():
                copy_of(b, send_hbm).start()

            @pl.when(tile != b)
            def _():
                copy_of(b, recv_hbm).start()
        else:
            copy_of(b, recv_hbm).start()
    out_ref[...] = jnp.zeros_like(out_ref)
    for b in range(buckets):
        copy_of(b, recv_hbm).wait()
        if b == tiles:
            valid = band > 0
        elif b == tiles + 1:
            valid = band < bands - 1
        else:
            valid = True
        for s in range(bucket):
            label = recv_labels_ref[b, 0, s]
            if b < tiles:
                label = jnp.where(tile == b, labels_ref[b, 0, s], label)

            @pl.when((label >= 0) & valid)
            def _():
                out_ref[label] += landed[b * bucket + s]


def per_device(tiles, bands, patches, pair_patch, pair_atm, numerators, counts):
    pairs, cell_rows, patch_rows = numerators.shape
    flux = patches.shape[1]
    blocks_owned = CELLS_DEV // cell_rows
    bucket = pairs // 8
    buckets = tiles + 2
    chunk = 16
    smem = pl.BlockSpec(memory_space=pltpu.SMEM)
    vmem = pl.BlockSpec(memory_space=pltpu.VMEM)
    anywhere = pl.BlockSpec(memory_space=pl.ANY)
    labels_shape = jax.ShapeDtypeStruct((buckets, 1, LANES), jnp.int32)
    recv_shape = jax.ShapeDtypeStruct((buckets * bucket, cell_rows, flux), jnp.float32)
    send, labels = pl.pallas_call(
        functools.partial(pack_kernel, tiles, bucket, blocks_owned, chunk),
        out_shape=(jax.ShapeDtypeStruct((buckets * bucket + 1, cell_rows, flux), jnp.float32), labels_shape),
        in_specs=[smem, smem, smem, anywhere, anywhere],
        out_specs=(vmem, smem),
        scratch_shapes=[
            pltpu.VMEM(patches.shape, patches.dtype),
            pltpu.VMEM((pairs, cell_rows, patch_rows), jnp.int32),
            pltpu.SMEM((buckets * blocks_owned,), jnp.int32),
            pltpu.SMEM((buckets,), jnp.int32),
            pltpu.SemaphoreType.DMA,
            pltpu.SemaphoreType.DMA((pairs // chunk,)),
        ],
        compiler_params=pltpu.CompilerParams(vmem_limit_bytes=PADDED_LIMIT),
        name="pack",
    )(pair_patch, pair_atm, counts, patches, numerators)
    recv, recv_labels = pl.pallas_call(
        functools.partial(send_kernel, tiles, bands, bucket),
        out_shape=(recv_shape, labels_shape),
        in_specs=[anywhere, anywhere],
        out_specs=(anywhere, anywhere),
        scratch_shapes=[pltpu.SemaphoreType.DMA((tiles + 1,))] * 4,
        compiler_params=pltpu.CompilerParams(collective_id=0, has_side_effects=True, vmem_limit_bytes=VMEM_LIMIT),
        name="exchange",
    )(send, labels)
    out = pl.pallas_call(
        functools.partial(add_kernel, tiles, bands, bucket),
        out_shape=jax.ShapeDtypeStruct((blocks_owned, cell_rows, flux), jnp.float32),
        in_specs=[smem, smem, anywhere, anywhere],
        out_specs=vmem,
        scratch_shapes=[
            pltpu.VMEM(recv_shape.shape, jnp.float32),
            pltpu.SemaphoreType.DMA((buckets,)),
        ],
        compiler_params=pltpu.CompilerParams(vmem_limit_bytes=VMEM_LIMIT),
        name="add",
    )(labels, recv_labels, send, recv)
    return out.reshape(blocks_owned * cell_rows, flux)


def ring_order(tiles):
    wide = tiles // 4
    if wide * 4 != tiles or wide % 2:
        return list(range(tiles))
    order = list(range(wide))
    for step, column in enumerate(reversed(range(wide))):
        rows = range(1, 4) if step % 2 == 0 else range(3, 0, -1)
        order += [row * wide + column for row in rows]
    return order


def chosen(values, index):
    picked = values[0]
    for k in range(1, len(values)):
        picked = jnp.where(index == k, values[k], picked)
    return picked


def ring_tile(tiles, tile, steps):
    order = ring_order(tiles)
    position = chosen([order.index(k) for k in range(tiles)], tile)
    return chosen(order, lax.rem(position + steps + tiles, tiles))


def layout(bucket):
    return dict(up=4 * bucket, down=5 * bucket, own=6 * bucket, end=7 * bucket)


def reaching(tiles, bucket, way, read):
    reach = tiles // 2
    base = 7 * bucket - 1
    far = read(base + reach)
    counts = [read(base + (k if way == 0 else tiles - k)) for k in range(1, reach)]
    counts.append((far + 1) >> 1 if way == 0 else far >> 1)
    beyond = [0]
    for count in reversed(counts):
        beyond.append(beyond[-1] + count)
    return [None] + beyond[::-1]


def split(value, size):
    if size & (size - 1) == 0:
        return value >> (size.bit_length() - 1), value & (size - 1)
    return lax.div(value, size), lax.rem(value, size)


def sort_pairs(tiles, bands, bucket, blocks_owned, band, tile, live, atm):
    pairs = atm.shape[1]
    reach = tiles // 2
    order = ring_order(tiles)
    spots = [order.index(k) for k in range(tiles)]
    here = chosen(spots, tile)
    wide = (pairs, pairs)

    def across(value):
        return jnp.broadcast_to(value, wide).T

    def least(value):
        return jnp.min(value, axis=0, keepdims=True)

    def most(value):
        return jnp.max(value, axis=0, keepdims=True)

    def count(mask):
        return jnp.sum(jnp.where(mask, 1, 0), axis=0, keepdims=True)

    def bucket_of(value):
        owner, block = split(value, blocks_owned)
        owner_band, owner_tile = split(owner, tiles)
        ahead = split(chosen(spots, owner_tile) - here + tiles, tiles)[1]
        return jnp.where(owner_band == band, ahead, jnp.where(owner_band > band, tiles, tiles + 1)), block

    row = lax.broadcasted_iota(jnp.int32, wide, 0)
    lane = lax.broadcasted_iota(jnp.int32, wide, 1)
    one_lane = lax.broadcasted_iota(jnp.int32, (1, pairs), 1)
    atm_c = across(atm)
    live_c = row < live
    same = (atm_c == atm) & live_c
    first = least(jnp.where(same, row, pairs))
    before = most(jnp.where(same & (row < lane), row, -1))
    fresh_c = (across(first) == row) & live_c
    b, _ = bucket_of(atm)
    b_c, block_c = bucket_of(atm_c)
    rank = count(fresh_c & (b_c == b) & (row < first))
    back = (b > reach) | ((b == reach) & ((rank & 1) == 1))
    region = jnp.where(b == 0, 4, jnp.where(b >= tiles, b - tiles + 2, jnp.where(back, 1, 0)))
    near = jnp.where(region == 0, reach - b, jnp.where(region == 1, b - reach, 0))
    shift = ((reach + 1) * (pairs + 1)).bit_length()
    key = (region << shift) + near * (pairs + 1) + first
    key_c = across(key)
    place = count(fresh_c & ((key_c >> shift) == region) & (key_c < key))
    ring = region < 2
    room = jnp.where(ring, 2 * bucket, bucket)
    base = jnp.where(ring, 2 * region, region + 2) * bucket
    fits = place < room
    slot = jnp.where((one_lane < live) & fits, base + place, pairs)
    overflow = jnp.max(jnp.where((one_lane < live) & jnp.logical_not(fits), 1, 0), axis=1, keepdims=True)
    travels_c = live_c & (b_c > 0) & (b_c < tiles)
    travelling = count(travels_c)
    earlier = count(travels_c & (row < lane))
    rank_of = jnp.where((one_lane < live) & ring, earlier, travelling + one_lane - earlier)
    rank_c = across(rank_of)
    overflow = jnp.maximum(overflow, jnp.where(travelling > pairs // 2, 1, 0))
    here_c = rank_c == lane
    pair_at = most(jnp.where(here_c, row, 0))
    before = most(jnp.where(row == before, rank_c, -1))
    before = most(jnp.where(here_c, across(before), -1))
    hit = across(slot) == lane
    last = most(jnp.where(hit, rank_c, 0))
    label = most(jnp.where(hit, block_c, -1))
    counts = count(fresh_c & (b_c == lane - (7 * bucket - 1)))
    kinds = [count(fresh_c & (b_c == k)) for k in (0, tiles, tiles + 1)]
    packed = overflow + sum(kind << (1 + 6 * i) for i, kind in enumerate(kinds))
    labels = jnp.where(one_lane < 7 * bucket, label, jnp.where(one_lane == pairs - 1, packed, counts))
    return before, last, pair_at, labels


def starts(reach, lag, reaches):
    first = [None] * (reach + 1)
    for u in range(reach - 1, -1, -1):
        begin = [0]
        for j in range(1, reach - u):
            after = begin[j - 1] + reaches[u + j - 1][j]
            begin.append(jnp.maximum(after, first[u + 1][j - 1] + lag))
        first[u] = begin
    end = jnp.int32(0)
    for j in range(reach):
        size = reaches[j][j + 1]
        end = jnp.where(size > 0, first[0][j] + size, end)
    return first[0], first[1], end


def stream_kernel(tiles, bands, bucket, blocks_owned, plans, group,
                  patch_ref, counts_ref, atm_ref, patches_hbm, numer_hbm,
                  pool_ref, beside_ref, own_ref, landing, flag_ref,
                  patches_ref, numer_ref, labels_ref, work_v, work_ref, load_sems, sums, side, stage, recv, table_ref, mark,
                  ring_send, ring_recv, beside_send, beside_recv, label_send, label_recv, local_sem):
    band, tile = lax.axis_index("band"), lax.axis_index("tile")
    reach = tiles // 2
    own_rows = 2 * bucket
    at = layout(bucket)
    steps = partners(tiles)
    pairs = numer_ref.shape[0]

    def numer_load(c):
        part = pl.ds(c * group, group)
        return pltpu.make_async_copy(numer_hbm.at[part], numer_ref.at[part], load_sems.at[c])

    patch_load = pltpu.make_async_copy(patches_hbm, patches_ref, load_sems.at[pairs // group])
    patch_load.start()
    for c in range(pairs // group):
        numer_load(c).start()
    barrier = pltpu.get_barrier_semaphore()
    for step in steps:
        pl.semaphore_signal(barrier, inc=1, device_id=(band, step(tile)), device_id_type=MESH)
    for j in range(1, bands):
        pl.semaphore_signal(barrier, inc=1, device_id=(lax.rem(band + j, bands), tile), device_id_type=MESH)
    before, last, pair_at, labels = sort_pairs(tiles, bands, bucket, blocks_owned, band, tile, counts_ref[0], atm_ref[...])
    labels_ref[...] = labels
    landing[tile] = labels
    work_v[0:1] = before
    work_v[1:2] = last
    work_v[2:3] = pair_at
    work_in = pltpu.make_async_copy(work_v, work_ref, local_sem)
    work_in.start()
    work_in.wait()
    patch_load.wait()
    for c in range(pairs // group):
        numer_load(c).wait()

    def multiply(c):
        for j in range(group):
            k = c * group + j
            g = work_ref[2, k]
            weight = (numer_ref[g].astype(jnp.float32) * SCALE).astype(jnp.bfloat16)
            part = jnp.dot(weight, patches_ref[patch_ref[g]], preferred_element_type=jnp.float32)
            before = work_ref[0, k]
            earlier = sums[jnp.maximum(before, 0)]
            sums[k] = part + jnp.where(before >= 0, earlier, 0.0)

    pl.loop(0, pairs // group // 2)(multiply)

    def total(slot):
        return sums[work_ref[1, slot]]

    targets = ((band, ring_tile(tiles, tile, 1)), (band, ring_tile(tiles, tile, -1)))
    is_edge = (band == 0) | (band == bands - 1)
    head = max(size * lag for size, _, lag in plans)
    for way in range(2):
        for s in range(head):
            pool_ref[way, s] = total(way * own_rows + s)
    pl.semaphore_wait(barrier, tiles + bands - 2)
    inside = [
        pltpu.make_async_remote_copy(
            src_ref=labels_ref, dst_ref=landing.at[tile],
            send_sem=label_send.at[k], recv_sem=label_recv.at[k],
            device_id=(band, step(tile)), device_id_type=MESH)
        for k, step in enumerate(steps)
    ]
    across = [
        pltpu.make_async_remote_copy(
            src_ref=mark, dst_ref=landing.at[tiles + band],
            send_sem=label_send.at[tiles - 2 + j], recv_sem=label_recv.at[tiles - 2 + j],
            device_id=(lax.rem(band + j, bands), tile), device_id_type=MESH)
        for j in range(1, bands)
    ]
    for copy in inside:
        copy.start()

    def hop(way, r, size, source):
        rows = pl.ds(r * size, size)
        return pltpu.make_async_remote_copy(
            src_ref=source, dst_ref=recv.at[way, rows],
            send_sem=ring_send.at[way, r], recv_sem=ring_recv.at[way, r],
            device_id=targets[way], device_id_type=MESH)

    def own_hop(way, r, size):
        return hop(way, r, size, pool_ref.at[way, pl.ds(r * size, size)])

    def later_hop(way, r, size):
        return hop(way, r, size, stage.at[way, pl.ds(r * size, size)])

    for edge in (True, False):
        size, rounds, lag = plans[0 if edge else 1]

        @pl.when(is_edge if edge else jnp.logical_not(is_edge))
        def _():
            for r in range(lag):
                for way in range(2):
                    own_hop(way, r, size).start()

    def beside(way, target_band):
        return pltpu.make_async_remote_copy(
            src_ref=side.at[way], dst_ref=beside_ref.at[way],
            send_sem=beside_send.at[way], recv_sem=beside_recv.at[way],
            device_id=(target_band, tile), device_id_type=MESH)

    upward, downward = beside(0, band + 1), beside(1, band - 1)
    pl.loop(pairs // group // 2, pairs // group)(multiply)
    for way in range(2):
        for s in range(bucket):
            side[way, s] = total(at["up"] + way * bucket + s)
    for way in range(2):
        for s in range(head, own_rows):
            pool_ref[way, s] = total(way * own_rows + s)
    for s in range(bucket):
        own_ref[s] = total(at["own"] + s)

    @pl.when(band < bands - 1)
    def _():
        upward.start()

    @pl.when(band > 0)
    def _():
        downward.start()

    for copy in inside:
        copy.wait()
    rows_in = pltpu.make_async_copy(landing.at[pl.ds(0, tiles)], table_ref.at[pl.ds(0, tiles)], local_sem)
    rows_in.start()
    rows_in.wait()

    upstream = [[ring_tile(tiles, tile, -u if way == 0 else u) for u in range(tiles)] for way in range(2)]
    reaches = [[reaching(tiles, bucket, way, lambda i, t=t: table_ref[t, 0, i]) for t in upstream[way]]
               for way in range(2)]
    lag_slots = jnp.where(is_edge, plans[0][0] * plans[0][2], plans[1][0] * plans[1][2])
    capacity = jnp.where(is_edge, plans[0][0] * plans[0][1], plans[1][0] * plans[1][1])
    worst = jnp.int32(0)
    flag = jnp.int32(0)
    begins = []
    for way in range(2):
        for v in range(tiles):
            ahead, behind, end = starts(reach, lag_slots, [reaches[way][(v + u) % tiles] for u in range(reach)])
            worst = jnp.maximum(worst, end)
            if v == 0:
                begins.append(ahead)
    arrivals = []
    for way in range(2):
        ahead, _, _ = starts(reach, lag_slots, [reaches[way][(1 + u) % tiles] for u in range(reach)])
        arrivals.append(ahead)
    for t in range(tiles):
        flag = jnp.maximum(flag, table_ref[t, 0, LANES - 1] & 1)
    flag = jnp.where(worst > capacity, 1, flag)
    lane = lax.broadcasted_iota(jnp.int32, (1, LANES), 1)
    row = landing[tile]
    mark[...] = jnp.where(lane == LANES - 1, row - (row & 1) + flag, row)
    plan = jnp.zeros((1, LANES), jnp.int32)
    for way in range(2):
        for j in range(reach):
            plan = jnp.where(lane == way * reach + j, arrivals[way][j], plan)
    landing[tiles + bands] = plan

    for edge in (True, False):
        size, rounds, lag = plans[0 if edge else 1]
        last_row = own_rows + size * rounds - 1

        @pl.when(is_edge if edge else jnp.logical_not(is_edge))
        def _():
            def keep(way, r):
                later_hop(way, r, size).wait_recv()
                pool_ref[way, pl.ds(own_rows + r * size, size)] = recv[way, pl.ds(r * size, size)]

            def gather(way, r):
                begin, arrived = begins[way], arrivals[way]
                for s in range(size):
                    p = r * size + s
                    row = jnp.minimum(p, own_rows - 1)
                    for j in range(1, reach):
                        row = jnp.where(p >= begin[j], p + (own_rows + arrived[j - 1] - begin[j]), row)
                    row = jnp.clip(row, 0, last_row)
                    stage[way, p] = pool_ref[way, row]

            def one_round(r):
                for way in range(2):
                    keep(way, r - lag)
                    gather(way, r)
                    later_hop(way, r, size).start()

            one_round(lag)
            for copy in across:
                copy.start()

            @pl.loop(lag + 1, rounds)
            def _(r):
                one_round(r)

    for copy in across:
        copy.wait()
    rows_over = pltpu.make_async_copy(landing.at[pl.ds(tiles, bands)], table_ref.at[pl.ds(tiles, bands)], local_sem)
    rows_over.start()
    rows_over.wait()
    for j in range(1, bands):
        flag = jnp.maximum(flag, table_ref[tiles + lax.rem(band + j, bands), 0, LANES - 1] & 1)
    flag_ref[0, 0] = flag

    @pl.when(band < bands - 1)
    def _():
        upward.wait_send()
        downward.wait_recv()

    @pl.when(band > 0)
    def _():
        downward.wait_send()
        upward.wait_recv()

    for edge in (True, False):
        size, rounds, lag = plans[0 if edge else 1]

        @pl.when(is_edge if edge else jnp.logical_not(is_edge))
        def _():
            @pl.loop(0, rounds - lag)
            def _(r):
                for way in range(2):
                    later_hop(way, r, size).wait_send()

            @pl.loop(rounds - lag, rounds)
            def _(r):
                for way in range(2):
                    later_hop(way, r, size).wait()
                    pool_ref[way, pl.ds(own_rows + r * size, size)] = recv[way, pl.ds(r * size, size)]


def take_kernel(tiles, bands, bucket, table_ref, own_ref, pool_ref, beside_ref, out_ref):
    band, tile = lax.axis_index("band"), lax.axis_index("tile")
    reach = tiles // 2
    own_rows = 2 * bucket
    at = layout(bucket)
    out_ref[...] = jnp.zeros_like(out_ref)

    def how_many(lane, kind):
        return (lane >> (1 + 6 * kind)) & 63

    def add(low, high, label_of, block_of):
        fours = (high - low) >> 2

        @pl.loop(0, fours)
        def _(k):
            at_once = [low + 4 * k + j for j in range(4)]
            labels = [label_of(i) for i in at_once]
            sums = [out_ref[label] + block_of(i) for label, i in zip(labels, at_once)]
            for label, total in zip(labels, sums):
                out_ref[label] = total

        @pl.loop(low + 4 * fours, high)
        def _(i):
            out_ref[label_of(i)] += block_of(i)

    add(0, how_many(table_ref[tile, 0, LANES - 1], 0),
        lambda i: table_ref[tile, 0, at["own"] + i], lambda i: own_ref[i])
    for way in range(2):
        other = tiles + jnp.clip(band - 1 if way == 0 else band + 1, 0, bands - 1)
        valid = (band > 0) if way == 0 else (band < bands - 1)
        add(0, jnp.where(valid, how_many(table_ref[other, 0, LANES - 1], 1 + way), 0),
            lambda i: table_ref[other, 0, at["up"] + way * bucket + i], lambda i: beside_ref[way, i])

    for way in range(2):
        for distance in range(1, reach + 1):
            source = ring_tile(tiles, tile, -distance if way == 0 else distance)
            reaches = reaching(tiles, bucket, way, lambda i: table_ref[source, 0, i])
            start = own_rows + table_ref[tiles + bands, 0, way * reach + distance - 1]
            add(reaches[distance + 1], reaches[distance],
                lambda i: table_ref[source, 0, way * own_rows + i], lambda i: pool_ref[way, start + i])


def adaptive(tiles, bands, patches, pair_patch, pair_atm, numerators, counts):
    pairs, patch_rows, cell_rows = numerators.shape
    flux = patches.shape[1]
    blocks_owned = CELLS_DEV // cell_rows
    bucket = pairs // 8
    reach = tiles // 2
    group = 32
    plans = ((4, 5 * reach, 5), (3, 4 * reach, 3))
    slots = max(size * rounds for size, rounds, _ in plans)
    most = max(rounds for _, rounds, _ in plans)
    smem = pl.BlockSpec(memory_space=pltpu.SMEM)
    vmem = pl.BlockSpec(memory_space=pltpu.VMEM)
    hbm = pl.BlockSpec(memory_space=pltpu.HBM)
    block = (cell_rows, flux)
    f32 = jnp.float32
    numerators = jnp.transpose(numerators, (0, 2, 1))
    pool, beside, own, table, flag = pl.pallas_call(
        functools.partial(stream_kernel, tiles, bands, bucket, blocks_owned, plans, group),
        out_shape=(jax.ShapeDtypeStruct((2, 2 * bucket + slots) + block, f32),
                   jax.ShapeDtypeStruct((2, bucket) + block, f32),
                   jax.ShapeDtypeStruct((bucket,) + block, f32),
                   jax.ShapeDtypeStruct((tiles + bands + 1, 1, LANES), jnp.int32),
                   jax.ShapeDtypeStruct((1, LANES), jnp.int32)),
        in_specs=[smem, smem, vmem, hbm, hbm],
        out_specs=(vmem, vmem, vmem, vmem, smem),
        scratch_shapes=[
            pltpu.VMEM((patches.shape[0] // patch_rows, patch_rows, flux), patches.dtype),
            pltpu.VMEM(numerators.shape, numerators.dtype),
            pltpu.VMEM((1, LANES), jnp.int32),
            pltpu.VMEM((3, pairs), jnp.int32),
            pltpu.SMEM((3, pairs), jnp.int32),
            pltpu.SemaphoreType.DMA((pairs // group + 1,)),
            pltpu.VMEM((pairs,) + block, f32),
            pltpu.VMEM((2, bucket) + block, f32),
            pltpu.VMEM((2, slots) + block, f32),
            pltpu.VMEM((2, slots) + block, f32),
            pltpu.SMEM((tiles + bands, 1, LANES), jnp.int32),
            pltpu.VMEM((1, LANES), jnp.int32),
            pltpu.SemaphoreType.DMA((2, most)),
            pltpu.SemaphoreType.DMA((2, most)),
            pltpu.SemaphoreType.DMA((2,)),
            pltpu.SemaphoreType.DMA((2,)),
            pltpu.SemaphoreType.DMA((tiles + bands - 2,)),
            pltpu.SemaphoreType.DMA((tiles + bands - 2,)),
            pltpu.SemaphoreType.DMA,
        ],
        compiler_params=pltpu.CompilerParams(collective_id=1, has_side_effects=True, vmem_limit_bytes=STREAM_LIMIT),
        name="stream",
    )(pair_patch, counts, pair_atm.reshape(1, pairs), patches.reshape(-1, patch_rows, flux), numerators)

    def take(patches, pair_patch, pair_atm, numerators, counts, table, own, pool, beside):
        out = pl.pallas_call(
            functools.partial(take_kernel, tiles, bands, bucket),
            out_shape=jax.ShapeDtypeStruct((blocks_owned,) + block, f32),
            in_specs=[smem, vmem, vmem, vmem],
            out_specs=vmem,
            compiler_params=pltpu.CompilerParams(vmem_limit_bytes=VMEM_LIMIT),
            name="take",
        )(table, own, pool, beside)
        return out.reshape(blocks_owned * cell_rows, flux)

    def padded(patches, pair_patch, pair_atm, numerators, counts, table, own, pool, beside):
        return per_device(tiles, bands, patches, pair_patch, pair_atm, numerators, counts)

    return lax.cond(flag[0, 0] > 0, padded, take, patches, pair_patch, pair_atm, numerators, counts,
                    table, own, pool, beside)


def solution(mesh):
    spec = P(("band", "tile"))
    placed = (
        P(("band", "tile"), None),
        spec,
        spec,
        P(("band", "tile"), None, None),
        spec,
    )
    body = functools.partial(adaptive, mesh.shape["tile"], mesh.shape["band"])
    return jax.shard_map(body, mesh=mesh, in_specs=placed, out_specs=P(("band", "tile"), None), check_vma=False)
```
